32 devices in a mesh: fsdp: 32 (over z, y, x, core).
Axes of the slice: x: 2, y: 2, z: 4, core: 2. Of those that a mesh axis runs over, the one named last changes fastest.
Arguments:
- tokens: int32 [32, 512], P('fsdp')
- positions: int32 [32, 512], P('fsdp')
- embed_table: bfloat16 [152064, 896], P('fsdp')
- attn_norm: bfloat16 [896], P('fsdp')
- w_query: bfloat16 [896, 896], P('fsdp')
- w_key: bfloat16 [896, 128], P('fsdp')
- w_value: bfloat16 [896, 128], P('fsdp')
- q_norm: bfloat16 [64], replicated
- k_norm: bfloat16 [64], replicated
- w_out: bfloat16 [896, 896], P('fsdp')
- mlp_norm: bfloat16 [896], P('fsdp')
- w_gate: bfloat16 [896, 4864], P('fsdp')
- w_up: bfloat16 [896, 4864], P('fsdp')
- w_down: bfloat16 [4864, 896], P('fsdp')
- dy_out: bfloat16 [32, 512, 896], P('fsdp')
Outputs:
- output 1: bfloat16 [32, 512, 896], P('fsdp')
- output 2: float32 [152064, 896], P('fsdp')
- output 3: float32 [896], P('fsdp')
- output 4: float32 [896, 896], P('fsdp')
- output 5: float32 [896, 128], P('fsdp')
- output 6: float32 [896, 128], P('fsdp')
- output 7: float32 [64], replicated
- output 8: float32 [64], replicated
- output 9: float32 [896, 896], P('fsdp')
- output 10: float32 [896], P('fsdp')
- output 11: float32 [896, 4864], P('fsdp')
- output 12: float32 [896, 4864], P('fsdp')
- output 13: float32 [4864, 896], P('fsdp')
All inputs are finite; a program needn't handle non-finite values.
Results may differ from the reference program's by a relative error of at most 0.0199887.
Values are sent between devices in bfloat16 or wider.
A program may use at most 1 GiB of HBM per device.

```python
import math
import jax
import jax.numpy as jnp
from jax import lax

D = 896
HEADS = 14
KV_HEADS = 2
HEAD = 64
FF = 4864
VOCAB = 151936
VOCAB_P = 152064
GROUP = 32
BATCH_DEV = 1
SEQ = 512

BATCH = GROUP * BATCH_DEV
Q_PER_KV = HEADS // KV_HEADS
ROWS_SHARD = VOCAB_P // GROUP
DOC_SPAN = max(SEQ // 4, 2)
NORM_EPS = 1e-6
ROPE_THETA = 1.0e6


def draw_tokens(rng_key):
    key_list = jax.random.split(rng_key, 4)
    id_top = jax.random.randint(key_list[0], (BATCH, SEQ), 1, VOCAB + 1)
    id_mid = jax.random.randint(key_list[1], (BATCH, SEQ), 0, id_top)
    token_ids = jax.random.randint(key_list[2], (BATCH, SEQ), 0, id_mid + 1)
    shard_lo = (jnp.arange(BATCH) % GROUP) * ROWS_SHARD
    shard_hi = jnp.minimum(shard_lo + ROWS_SHARD, VOCAB)
    cover_ids = jax.random.randint(key_list[3], (BATCH,), shard_lo, shard_hi)
    token_ids = token_ids.at[:, 0].set(cover_ids)
    return token_ids.at[BATCH - 1, SEQ - 1].set(VOCAB - 1).astype(jnp.int32)


def draw_positions(rng_key):
    seq_idx = jnp.arange(SEQ, dtype=jnp.int32)[None, :]
    starts = (jax.random.randint(rng_key, (BATCH, SEQ), 0, DOC_SPAN) == 0) | (seq_idx == 0)
    last_start = lax.cummax(jnp.where(starts, seq_idx, 0), axis=1)
    return (seq_idx - last_start).astype(jnp.int32)


def setup_inputs(seed: int = 0) -> dict:
    key_list = jax.random.split(jax.random.key(seed), 16)

    def weight(key_idx, arr_shape, fan_in):
        return (jax.random.normal(key_list[key_idx], arr_shape, jnp.float32) * fan_in ** -0.5).astype(jnp.bfloat16)

    def gain_vec(key_idx, vec_len):
        return (1.0 + 0.25 * jax.random.normal(key_list[key_idx], (vec_len,), jnp.float32)).astype(jnp.bfloat16)

    table_f = jax.random.normal(key_list[2], (VOCAB_P, D), jnp.float32)
    table_f = jnp.where(jnp.arange(VOCAB_P)[:, None] < VOCAB, table_f, 0.0)
    return {
        'tokens': draw_tokens(key_list[0]),
        'positions': draw_positions(key_list[1]),
        'embed_table': table_f.astype(jnp.bfloat16),
        'attn_norm': gain_vec(3, D),
        'w_query': weight(4, (D, HEADS * HEAD), D),
        'w_key': weight(5, (D, KV_HEADS * HEAD), D),
        'w_value': weight(6, (D, KV_HEADS * HEAD), D),
        'q_norm': gain_vec(7, HEAD),
        'k_norm': gain_vec(8, HEAD),
        'w_out': weight(9, (HEADS * HEAD, D), HEADS * HEAD),
        'mlp_norm': gain_vec(10, D),
        'w_gate': weight(11, (D, FF), D),
        'w_up': weight(12, (D, FF), D),
        'w_down': weight(13, (FF, D), FF),
        'dy_out': jax.random.normal(key_list[14], (BATCH, SEQ, D), jnp.float32).astype(jnp.bfloat16),
    }


def to_bf16(values):
    return values + lax.stop_gradient(values.astype(jnp.bfloat16).astype(jnp.float32) - values)


def rms_scale(values, norm_gain):
    inv_rms = lax.rsqrt(jnp.mean(values * values, axis=-1, keepdims=True) + NORM_EPS)
    return values * inv_rms * norm_gain


def rope_tables(positions):
    half_dim = HEAD // 2
    inv_freq = jnp.exp(jnp.arange(half_dim, dtype=jnp.float32) * (-2.0 * math.log(ROPE_THETA) / HEAD))
    angles = positions.astype(jnp.float32)[:, :, None] * inv_freq
    return jnp.cos(angles), jnp.sin(angles)


def rotate(values, cos_t, sin_t):
    half_dim = values.shape[-1] // 2
    lead_half = values[..., :half_dim]
    tail_half = values[..., half_dim:]
    return jnp.concatenate([lead_half * cos_t - tail_half * sin_t, tail_half * cos_t + lead_half * sin_t], axis=-1)


def seq_attend(operands):
    q_seq, k_seq, v_seq = operands
    scores = jnp.einsum('qgrh,kgh->grqk', q_seq, k_seq) * (HEAD ** -0.5)
    causal = jnp.arange(SEQ)[:, None] >= jnp.arange(SEQ)[None, :]
    scores = jnp.where(causal, scores, -1e30)
    attn_probs = to_bf16(jax.nn.softmax(scores, axis=-1))
    return to_bf16(jnp.einsum('grqk,kgh->qgrh', attn_probs, v_seq))


def reference(tokens, positions, embed_table, attn_norm, w_query, w_key, w_value, q_norm, k_norm, w_out, mlp_norm, w_gate, w_up, w_down, dy_out):
    cos_t, sin_t = rope_tables(positions)
    cos_q = cos_t[:, :, None, None, :]
    sin_q = sin_t[:, :, None, None, :]
    cos_k = cos_t[:, :, None, :]
    sin_k = sin_t[:, :, None, :]

    def layer_fwd(x_emb, g_attn, wt_query, wt_key, wt_value, g_query, g_key, wt_out, g_mlp, wt_gate, wt_up, wt_down):
        normed = to_bf16(rms_scale(x_emb, g_attn)).reshape(BATCH * SEQ, D)
        q_proj = to_bf16(jnp.dot(normed, wt_query, preferred_element_type=jnp.float32)).reshape(BATCH, SEQ, KV_HEADS, Q_PER_KV, HEAD)
        k_proj = to_bf16(jnp.dot(normed, wt_key, preferred_element_type=jnp.float32)).reshape(BATCH, SEQ, KV_HEADS, HEAD)
        v_proj = to_bf16(jnp.dot(normed, wt_value, preferred_element_type=jnp.float32)).reshape(BATCH, SEQ, KV_HEADS, HEAD)
        q_rot = to_bf16(rotate(rms_scale(q_proj, g_query), cos_q, sin_q))
        k_rot = to_bf16(rotate(rms_scale(k_proj, g_key), cos_k, sin_k))
        attn_heads = lax.map(jax.checkpoint(seq_attend), (q_rot, k_rot, v_proj))
        attn_proj = jnp.dot(attn_heads.reshape(BATCH * SEQ, HEADS * HEAD), wt_out, preferred_element_type=jnp.float32)
        hidden = to_bf16(x_emb + attn_proj.reshape(BATCH, SEQ, D))
        mlp_in = to_bf16(rms_scale(hidden, g_mlp)).reshape(BATCH * SEQ, D)
        gate_pre = jnp.dot(mlp_in, wt_gate, preferred_element_type=jnp.float32)
        up_proj = jnp.dot(mlp_in, wt_up, preferred_element_type=jnp.float32)
        mlp_act = to_bf16(jax.nn.silu(gate_pre) * up_proj)
        mlp_proj = jnp.dot(mlp_act, wt_down, preferred_element_type=jnp.float32)
        return to_bf16(hidden + mlp_proj.reshape(BATCH, SEQ, D))

    x_emb = jnp.take(embed_table, tokens, axis=0).astype(jnp.float32)
    params = [weight_arr.astype(jnp.float32) for weight_arr in (attn_norm, w_query, w_key, w_value, q_norm, k_norm, w_out, mlp_norm, w_gate, w_up, w_down)]
    layer_out, pullback = jax.vjp(layer_fwd, x_emb, *params)
    grad_list = pullback(dy_out.astype(jnp.float32))
    d_table = jax.ops.segment_sum(grad_list[0].reshape(BATCH * SEQ, D), tokens.reshape(BATCH * SEQ), num_segments=VOCAB_P)
    return (layer_out.astype(jnp.bfloat16), d_table, grad_list[1], grad_list[2], grad_list[3], grad_list[4], grad_list[5], grad_list[6], grad_list[7], grad_list[8], grad_list[9], grad_list[10], grad_list[11])
```

```python
import math
import jax
import jax.numpy as jnp
from jax import lax
from jax.sharding import PartitionSpec as P

NORM_EPS = 1e-6
ROPE_THETA = 1.0e6
AXIS_NAME = 'fsdp'
F32 = jnp.float32
BF16 = jnp.bfloat16


def rope_tables(positions, head_dim):
    half_dim = head_dim // 2
    inv_freq = jnp.exp(jnp.arange(half_dim, dtype=jnp.float32) * (-2.0 * math.log(ROPE_THETA) / head_dim))
    angles = positions.astype(jnp.float32)[:, :, None] * inv_freq
    return jnp.cos(angles), jnp.sin(angles)


def rotate(values, cos_t, sin_t):
    half_dim = values.shape[-1] // 2
    lead_half = values[..., :half_dim]
    tail_half = values[..., half_dim:]
    return jnp.concatenate([lead_half * cos_t - tail_half * sin_t, tail_half * cos_t + lead_half * sin_t], axis=-1)


def norm_fwd(values):
    values_f = values.astype(jnp.float32)
    inv_rms = lax.rsqrt(jnp.mean(values_f * values_f, axis=-1, keepdims=True) + NORM_EPS)
    return values_f * inv_rms, inv_rms


def norm_bwd(grad_out, normed, inv_rms, norm_gain):
    grad_normed = grad_out * norm_gain.astype(jnp.float32)
    mean_term = jnp.mean(grad_normed * normed, axis=-1, keepdims=True)
    return inv_rms * (grad_normed - normed * mean_term)


def attn_fwd(q_rot, k_rot, v_raw):
    seq_len = q_rot.shape[1]
    attn_scale = q_rot.shape[-1] ** -0.5
    scores = jnp.einsum('bqgrh,bkgh->bgrqk', q_rot, k_rot, preferred_element_type=jnp.float32) * attn_scale
    causal = lax.broadcasted_iota(jnp.int32, (seq_len, seq_len), 0) >= lax.broadcasted_iota(jnp.int32, (seq_len, seq_len), 1)
    attn_probs = jax.nn.softmax(jnp.where(causal, scores, -1e30), axis=-1)
    attn_heads = jnp.einsum('bgrqk,bkgh->bqgrh', attn_probs.astype(jnp.bfloat16), v_raw, preferred_element_type=jnp.float32)
    return attn_heads.astype(jnp.bfloat16), attn_probs


def attn_bwd(grad_out, q_rot, k_rot, v_raw, attn_probs):
    attn_scale = q_rot.shape[-1] ** -0.5
    grad_b = grad_out.astype(jnp.bfloat16)
    probs_b = attn_probs.astype(jnp.bfloat16)
    grad_probs = jnp.einsum('bqgrh,bkgh->bgrqk', grad_b, v_raw, preferred_element_type=jnp.float32)
    grad_v = jnp.einsum('bgrqk,bqgrh->bkgh', probs_b, grad_b, preferred_element_type=jnp.float32)
    grad_scores = attn_probs * (grad_probs - jnp.sum(grad_probs * attn_probs, axis=-1, keepdims=True)) * attn_scale
    scores_b = grad_scores.astype(jnp.bfloat16)
    grad_q = jnp.einsum('bgrqk,bkgh->bqgrh', scores_b, k_rot, preferred_element_type=jnp.float32)
    grad_k = jnp.einsum('bgrqk,bqgrh->bkgh', scores_b, q_rot, preferred_element_type=jnp.float32)
    return grad_q, grad_k, grad_v


def dot(a, b, ca, cb):
    return lax.dot_general(a, b, (((ca,), (cb,)), ((), ())), preferred_element_type=F32)


def solution(mesh):
    n_dev = mesh.shape[AXIS_NAME]
    n_chip = n_dev // 2
    pair = [(i, i ^ 1) for i in range(n_dev)]
    groups = [[2 * k + c for k in range(n_chip)] for c in range(2)]
    to_use = [(d, 2 * (d % n_chip) + d // n_chip) for d in range(n_dev)]
    to_store = [(b, a) for a, b in to_use]

    row_spec = P(AXIS_NAME, None)
    vec_spec = P(AXIS_NAME)
    full_spec = P(None)
    batch_spec = P(AXIS_NAME, None, None)
    weight_specs = (vec_spec, row_spec, row_spec, row_spec, full_spec, full_spec, row_spec, vec_spec, row_spec, row_spec, row_spec)

    def swap(v):
        return lax.ppermute(v, AXIS_NAME, pair)

    def gather_group(v):
        return lax.all_gather(v, AXIS_NAME, axis_index_groups=groups, tiled=True)

    def scatter_group(v):
        return lax.psum_scatter(v, AXIS_NAME, scatter_dimension=0, axis_index_groups=groups, tiled=True)

    def device_step(tokens, positions, table_shard, attn_norm, w_query, w_key, w_value, q_norm, k_norm, w_out, mlp_norm, w_gate, w_up, w_down, dy_out):
        me = lax.axis_index(AXIS_NAME)
        core = lax.rem(me, 2)
        seq_len = tokens.shape[1]
        rows_local, model_dim = table_shard.shape
        rows_w, ff = w_gate.shape
        half = ff // 2
        nq, nk = w_query.shape[1], w_key.shape[1]
        head_dim = q_norm.shape[0]
        kv_heads = nk // head_dim
        q_per_kv = nq // nk

        gains = jnp.pad(jnp.stack([attn_norm, mlp_norm], axis=1), ((0, 0), (0, 126)))
        attn_pack = jnp.concatenate([w_query, w_out, w_key, w_value, gains], axis=1)
        attn_full = lax.all_gather(attn_pack, AXIS_NAME, tiled=True)
        mine_gu = jnp.concatenate([lax.dynamic_slice(w_gate, (0, core * half), (rows_w, half)), lax.dynamic_slice(w_up, (0, core * half), (rows_w, half))], axis=1)
        other_gu = jnp.concatenate([lax.dynamic_slice(w_gate, (0, (1 - core) * half), (rows_w, half)), lax.dynamic_slice(w_up, (0, (1 - core) * half), (rows_w, half))], axis=1)
        recv_gu = swap(other_gu)
        block_gu = jnp.where(core == 0, jnp.concatenate([mine_gu, recv_gu], axis=0), jnp.concatenate([recv_gu, mine_gu], axis=0))
        wgu = gather_group(block_gu)
        wd = gather_group(lax.ppermute(w_down, AXIS_NAME, to_use))
        w_g, w_u = wgu[:, :half], wgu[:, half:]

        all_ids = lax.all_gather(tokens.reshape(-1), AXIS_NAME, tiled=True)
        local_ids = all_ids - me * rows_local
        is_owner = (local_ids >= 0) & (local_ids < rows_local)
        picked = jnp.take(table_shard, jnp.clip(local_ids, 0, rows_local - 1), axis=0)
        picked = jnp.where(is_owner[:, None], picked, jnp.zeros((), picked.dtype)).reshape(n_chip, 2, seq_len, model_dim)
        keep = lax.dynamic_slice(picked, (0, core, 0, 0), (n_chip, 1, seq_len, model_dim)).reshape(-1, model_dim)
        give = lax.dynamic_slice(picked, (0, 1 - core, 0, 0), (n_chip, 1, seq_len, model_dim)).reshape(-1, model_dim)
        x_emb = scatter_group(keep + swap(give))

        dy = dy_out.reshape(seq_len, model_dim)
        dy2 = jnp.concatenate([dy, swap(dy)], axis=0)

        wq = attn_full[:, :nq]
        wo = attn_full[:, nq:2 * nq]
        wk = attn_full[:, 2 * nq:2 * nq + nk]
        wv = attn_full[:, 2 * nq + nk:2 * nq + 2 * nk]
        g_attn = attn_full[:, 2 * nq + 2 * nk]
        g_mlp = attn_full[:, 2 * nq + 2 * nk + 1]

        cos_t, sin_t = rope_tables(positions, head_dim)
        cos_q, sin_q = cos_t[:, :, None, None, :], sin_t[:, :, None, None, :]
        cos_k, sin_k = cos_t[:, :, None, :], sin_t[:, :, None, :]
        normed1, norm1_inv = norm_fwd(x_emb)
        attn_in = (normed1 * g_attn.astype(F32)).astype(BF16)
        q_raw = dot(attn_in, wq, 1, 0).astype(BF16).reshape(1, seq_len, kv_heads, q_per_kv, head_dim)
        k_raw = dot(attn_in, wk, 1, 0).astype(BF16).reshape(1, seq_len, kv_heads, head_dim)
        v_raw = dot(attn_in, wv, 1, 0).astype(BF16).reshape(1, seq_len, kv_heads, head_dim)
        q_normed, q_inv = norm_fwd(q_raw)
        k_normed, k_inv = norm_fwd(k_raw)
        q_rot = rotate(q_normed * q_norm.astype(F32), cos_q, sin_q).astype(BF16)
        k_rot = rotate(k_normed * k_norm.astype(F32), cos_k, sin_k).astype(BF16)
        attn_heads, attn_probs = attn_fwd(q_rot, k_rot, v_raw)
        attn_flat = attn_heads.reshape(seq_len, nq)
        hidden = (x_emb.astype(F32) + dot(attn_flat, wo, 1, 0)).astype(BF16)
        normed2, norm2_inv = norm_fwd(hidden)
        mlp_in = (normed2 * g_mlp.astype(F32)).astype(BF16)

        mlp2 = jnp.concatenate([mlp_in, swap(mlp_in)], axis=0)
        gate_pre = dot(mlp2, w_g, 1, 0)
        up_proj = dot(mlp2, w_u, 1, 0)
        gate_sig = jax.nn.sigmoid(gate_pre)
        mlp_act = (gate_pre * gate_sig * up_proj).astype(BF16)
        grad_w_down = dot(mlp_act, dy2, 0, 0)
        down_shard = lax.ppermute(scatter_group(grad_w_down), AXIS_NAME, to_store)
        grad_act = dot(dy2, wd, 1, 1)
        grad_gate = (grad_act * up_proj * gate_sig * (1.0 + gate_pre * (1.0 - gate_sig))).astype(BF16)
        grad_up = (grad_act * gate_pre * gate_sig).astype(BF16)
        part_in = dot(grad_gate, w_g, 1, 1) + dot(grad_up, w_u, 1, 1)
        grad_mlp_in = part_in[:seq_len] + swap(part_in[seq_len:])
        gate_shard = scatter_group(dot(mlp2, grad_gate, 0, 0))
        up_shard = scatter_group(dot(mlp2, grad_up, 0, 0))
        part_y = dot(mlp_act, wd, 1, 0)
        layer_out = (hidden.astype(F32) + (part_y[:seq_len] + swap(part_y[seq_len:]))).astype(BF16)

        grad_mlp_norm = jnp.sum(grad_mlp_in * normed2, axis=0)
        grad_hidden = dy.astype(F32) + norm_bwd(grad_mlp_in, normed2, norm2_inv, g_mlp)
        hidden_b = grad_hidden.astype(BF16)
        grad_w_out = dot(attn_flat, hidden_b, 0, 0)
        grad_heads = dot(hidden_b, wo, 1, 1).reshape(q_rot.shape)
        grad_q, grad_k, grad_v = attn_bwd(grad_heads, q_rot, k_rot, v_raw, attn_probs)
        grad_qt = rotate(grad_q, cos_q, -sin_q)
        grad_kt = rotate(grad_k, cos_k, -sin_k)
        grad_q_norm = jnp.sum(grad_qt * q_normed, axis=(0, 1, 2, 3))
        grad_k_norm = jnp.sum(grad_kt * k_normed, axis=(0, 1, 2))
        grad_q_raw = norm_bwd(grad_qt, q_normed, q_inv, q_norm).astype(BF16).reshape(seq_len, nq)
        grad_k_raw = norm_bwd(grad_kt, k_normed, k_inv, k_norm).astype(BF16).reshape(seq_len, nk)
        grad_v_raw = grad_v.astype(BF16).reshape(seq_len, nk)
        grad_attn_in = dot(grad_q_raw, wq, 1, 1) + dot(grad_k_raw, wk, 1, 1) + dot(grad_v_raw, wv, 1, 1)
        grad_attn_norm = jnp.sum(grad_attn_in * normed1, axis=0)
        grad_x_emb = grad_hidden + norm_bwd(grad_attn_in, normed1, norm1_inv, g_attn)

        my_rows = gather_group(grad_x_emb)
        other_rows = swap(my_rows)
        seg = jnp.where(is_owner, local_ids, rows_local).reshape(n_chip, 2, seq_len)
        seg_mine = lax.dynamic_slice(seg, (0, core, 0), (n_chip, 1, seq_len)).reshape(-1)
        seg_other = lax.dynamic_slice(seg, (0, 1 - core, 0), (n_chip, 1, seq_len)).reshape(-1)
        d_table = jax.ops.segment_sum(jnp.concatenate([my_rows, other_rows], axis=0), jnp.concatenate([seg_mine, seg_other]), num_segments=rows_local)

        grad_w_query = dot(attn_in, grad_q_raw, 0, 0)
        grad_w_key = dot(attn_in, grad_k_raw, 0, 0)
        grad_w_value = dot(attn_in, grad_v_raw, 0, 0)
        vecs = jnp.pad(jnp.stack([grad_attn_norm, grad_mlp_norm], axis=1), ((0, 0), (0, 126)))
        zeros = jnp.zeros_like(vecs)
        pack0 = jnp.concatenate([grad_w_query, grad_w_key, vecs], axis=1)
        pack1 = jnp.concatenate([grad_w_out, grad_w_value, zeros], axis=1)
        keep_pack = jnp.where(core == 0, pack0, pack1)
        give_pack = jnp.where(core == 0, pack1, pack0)
        attn_shard = scatter_group(keep_pack + swap(give_pack))

        chip_rows = jnp.concatenate([gate_shard, up_shard, attn_shard], axis=1)
        mine = lax.dynamic_slice(chip_rows, (core * rows_w, 0), (rows_w, chip_rows.shape[1]))
        recv = swap(lax.dynamic_slice(chip_rows, ((1 - core) * rows_w, 0), (rows_w, chip_rows.shape[1])))
        low = jnp.where(core == 0, mine, recv)
        high = jnp.where(core == 0, recv, mine)
        d_gate = jnp.concatenate([low[:, :half], high[:, :half]], axis=1)
        d_up = jnp.concatenate([low[:, half:ff], high[:, half:ff]], axis=1)
        d_query, d_key = low[:, ff:ff + nq], low[:, ff + nq:ff + nq + nk]
        d_attn_norm, d_mlp_norm = low[:, ff + nq + nk], low[:, ff + nq + nk + 1]
        d_out, d_value = high[:, ff:ff + nq], high[:, ff + nq:ff + nq + nk]
        qk = lax.psum(jnp.concatenate([grad_q_norm, grad_k_norm]), AXIS_NAME)
        return (layer_out.reshape(1, seq_len, model_dim), d_table, d_attn_norm, d_query, d_key, d_value, qk[:head_dim], qk[head_dim:], d_out, d_mlp_norm, d_gate, d_up, down_shard)

    return jax.shard_map(device_step, mesh=mesh, in_specs=(row_spec, row_spec, row_spec) + weight_specs + (batch_spec,), out_specs=(batch_spec, row_spec) + weight_specs, check_vma=False)
```

```python
import functools
import math
import jax
import jax.numpy as jnp
from jax import lax
from jax.experimental import pallas as pl
from jax.experimental.pallas import tpu as pltpu
from jax.sharding import PartitionSpec as P

NORM_EPS = 1e-6
ROPE_THETA = 1.0e6
AXIS_NAME = 'fsdp'
F32 = jnp.float32
BF16 = jnp.bfloat16
MESH = pl.DeviceIdType.MESH


def rope_tables(positions, head_dim):
    half_dim = head_dim // 2
    inv_freq = jnp.exp(jnp.arange(half_dim, dtype=jnp.float32) * (-2.0 * math.log(ROPE_THETA) / head_dim))
    angles = positions.astype(jnp.float32)[:, :, None] * inv_freq
    return jnp.cos(angles), jnp.sin(angles)


def rotate(values, cos_t, sin_t):
    half_dim = values.shape[-1] // 2
    lead_half = values[..., :half_dim]
    tail_half = values[..., half_dim:]
    return jnp.concatenate([lead_half * cos_t - tail_half * sin_t, tail_half * cos_t + lead_half * sin_t], axis=-1)


def norm_fwd(values):
    values_f = values.astype(jnp.float32)
    inv_rms = lax.rsqrt(jnp.mean(values_f * values_f, axis=-1, keepdims=True) + NORM_EPS)
    return values_f * inv_rms, inv_rms


def norm_bwd(grad_out, normed, inv_rms, norm_gain):
    grad_normed = grad_out * norm_gain.astype(jnp.float32)
    mean_term = jnp.mean(grad_normed * normed, axis=-1, keepdims=True)
    return inv_rms * (grad_normed - normed * mean_term)


def attn_fwd(q_rot, k_rot, v_raw):
    seq_len = q_rot.shape[1]
    attn_scale = q_rot.shape[-1] ** -0.5
    scores = jnp.einsum('bqgrh,bkgh->bgrqk', q_rot, k_rot, preferred_element_type=jnp.float32) * attn_scale
    causal = lax.broadcasted_iota(jnp.int32, (seq_len, seq_len), 0) >= lax.broadcasted_iota(jnp.int32, (seq_len, seq_len), 1)
    attn_probs = jax.nn.softmax(jnp.where(causal, scores, -1e30), axis=-1)
    attn_heads = jnp.einsum('bgrqk,bkgh->bqgrh', attn_probs.astype(jnp.bfloat16), v_raw, preferred_element_type=jnp.float32)
    return attn_heads.astype(jnp.bfloat16), attn_probs


def attn_bwd(grad_out, q_rot, k_rot, v_raw, attn_probs):
    attn_scale = q_rot.shape[-1] ** -0.5
    grad_b = grad_out.astype(jnp.bfloat16)
    probs_b = attn_probs.astype(jnp.bfloat16)
    grad_probs = jnp.einsum('bqgrh,bkgh->bgrqk', grad_b, v_raw, preferred_element_type=jnp.float32)
    grad_v = jnp.einsum('bgrqk,bqgrh->bkgh', probs_b, grad_b, preferred_element_type=jnp.float32)
    grad_scores = attn_probs * (grad_probs - jnp.sum(grad_probs * attn_probs, axis=-1, keepdims=True)) * attn_scale
    scores_b = grad_scores.astype(jnp.bfloat16)
    grad_q = jnp.einsum('bgrqk,bkgh->bqgrh', scores_b, k_rot, preferred_element_type=jnp.float32)
    grad_k = jnp.einsum('bgrqk,bqgrh->bkgh', scores_b, q_rot, preferred_element_type=jnp.float32)
    return grad_q, grad_k, grad_v


def dot(a, b, ca, cb):
    return lax.dot_general(a, b, (((ca,), (cb,)), ((), ())), preferred_element_type=F32)


def _coords(me):
    core = me % 2
    x = (me // 2) % 2
    y = (me // 4) % 2
    z = me // 8
    a = y * (1 - core) + x * core
    b = x * (1 - core) + y * core
    return core, a, b, z, 4 - 2 * core, 2 + 2 * core


def _barrier(peers):
    sem = pltpu.get_barrier_semaphore()
    for peer in peers:
        pl.semaphore_signal(sem, inc=1, device_id=(peer,), device_id_type=MESH)
    pl.semaphore_wait(sem, len(peers))


def _remote(src, dst, send_sem, recv_sem, dev):
    return pltpu.make_async_remote_copy(src_ref=src, dst_ref=dst, send_sem=send_sem, recv_sem=recv_sem, device_id=(dev,), device_id_type=MESH)


def _all_rows_kernel(n_dev, in_ref, out_ref, send_sem, recv_sem):
    me = lax.axis_index(AXIS_NAME)
    peers = [(me + d) % n_dev for d in range(1, n_dev)]
    _barrier(peers)
    copies = []
    for i, peer in enumerate(peers):
        copy = _remote(in_ref, out_ref.at[me], send_sem.at[i], recv_sem.at[i], peer)
        copy.start()
        copies.append(copy)
    out_ref[me] = in_ref[...]
    for copy in copies:
        copy.wait()


def all_rows(block, n_dev, collective_id):
    return pl.pallas_call(
        functools.partial(_all_rows_kernel, n_dev),
        out_shape=jax.ShapeDtypeStruct((n_dev,) + block.shape, block.dtype),
        in_specs=[pl.BlockSpec(memory_space=pltpu.VMEM)],
        out_specs=pl.BlockSpec(memory_space=pltpu.VMEM),
        scratch_shapes=[pltpu.SemaphoreType.DMA((n_dev - 1,)), pltpu.SemaphoreType.DMA((n_dev - 1,))],
        compiler_params=pltpu.CompilerParams(collective_id=collective_id, has_side_effects=True),
        cost_estimate=pl.CostEstimate(flops=10_000_000, bytes_accessed=1 << 18, transcendentals=0),
        name='all_rows',
    )(block)


def _gather_kernel(cuts, *refs):
    n_arr = len(cuts)
    (own_sem, z_send, z_recv, b_send, b_recv, a_send, a_recv, p_send, p_recv) = refs[2 * n_arr:]
    ins, outs = [], []
    for arr, (rows, n_cut) in enumerate(cuts):
        for i in range(n_cut):
            at = pl.ds(i * (rows // n_cut), rows // n_cut)
            ins.append(refs[arr] if n_cut == 1 else refs[arr].at[at])
            outs.append(functools.partial(lambda ref, at, slot: ref.at[slot] if at is None else ref.at[slot, at], refs[n_arr + arr], None if n_cut == 1 else at))
    n_pieces = len(ins)
    me = lax.axis_index(AXIS_NAME)
    core, a, b, z, a_str, b_str = _coords(me)
    a_nbr = me + (1 - 2 * a) * a_str
    b_nbr = me + (1 - 2 * b) * b_str
    partner = me + 1 - 2 * core
    z_base = me - 8 * z
    z_peer = [z_base + 8 * ((z + 1 + i) % 4) for i in range(3)]
    z_src = [z_base + 8 * ((z + 3 - i) % 4) for i in range(3)]
    b_shift = (1 - 2 * b) * b_str
    a_shift = (1 - 2 * a) * a_str
    _barrier([a_nbr, b_nbr, partner] + z_peer)
    z_blocks = [me] + z_src
    b_blocks = [d + b_shift for d in z_blocks]
    order = [('z', 0), ('z', 1), ('b', 0), ('z', 2), ('b', 1), ('z', 3), ('b', 2), ('b', 3)]
    a_out = [z_blocks[i] if kind == 'z' else b_blocks[i] for kind, i in order]
    a_in = [d + a_shift for d in a_out]
    started = []
    n_partner = [0]

    def send(p, src, dev_slot, s_sem, r_sem, dev):
        copy = _remote(src, outs[p](dev_slot), s_sem, r_sem, dev)
        copy.start()
        started.append(copy)

    def arrived(p, slot, sem):
        pltpu.make_async_copy(outs[p](slot), outs[p](slot), sem).wait()

    def to_partner(p, src, slot, j):
        send(p, src, slot, p_send.at[p, j], p_recv.at[p, j], partner)

    own = []
    for p in range(n_pieces):
        for i in range(3):
            send(p, ins[p], me, z_send.at[p, i], z_recv.at[p, i], z_peer[i])
        send(p, ins[p], me, b_send.at[p, 0], b_recv.at[p, 0], b_nbr)
        send(p, ins[p], me, a_send.at[p, 0], a_recv.at[p, 0], a_nbr)
        to_partner(p, ins[p], me, 0)
        copy = pltpu.make_async_copy(ins[p], outs[p](me), own_sem.at[p])
        copy.start()
        own.append(copy)
    j = 1
    for m, (kind, i) in enumerate(order):
        if m == 0:
            continue
        for p in range(n_pieces):
            slot = a_out[m]
            if kind == 'z':
                arrived(p, slot, z_recv.at[p, i - 1])
                send(p, outs[p](slot), slot, b_send.at[p, i], b_recv.at[p, i], b_nbr)
            else:
                arrived(p, slot, b_recv.at[p, i])
            send(p, outs[p](slot), slot, a_send.at[p, m], a_recv.at[p, m], a_nbr)
            to_partner(p, outs[p](slot), slot, j)
        j += 1
    for m in range(8):
        for p in range(n_pieces):
            arrived(p, a_in[m], a_recv.at[p, m])
            to_partner(p, outs[p](a_in[m]), a_in[m], j)
        j += 1
    p_shift = 1 - 2 * core
    pa_shift, pb_shift = b_shift, a_shift
    pz = [partner] + [s + p_shift for s in z_src]
    pb = [d + pb_shift for d in pz]
    p_first = [pz[i] if kind == 'z' else pb[i] for kind, i in order]
    p_in = p_first + [d + pa_shift for d in p_first]
    for j in range(16):
        for p in range(n_pieces):
            arrived(p, p_in[j], p_recv.at[p, j])
    for copy in own:
        copy.wait()
    for copy in started:
        copy.wait_send()


def gather_all(blocks, cuts, n_dev, collective_id):
    n_arr = len(blocks)
    n = sum(cuts)
    dma = pltpu.SemaphoreType.DMA
    nbytes = sum(v.size * v.dtype.itemsize for v in blocks)
    return pl.pallas_call(
        functools.partial(_gather_kernel, tuple((v.shape[0], c) for v, c in zip(blocks, cuts))),
        out_shape=[jax.ShapeDtypeStruct((n_dev,) + v.shape, v.dtype) for v in blocks],
        in_specs=[pl.BlockSpec(memory_space=pltpu.VMEM)] * n_arr,
        out_specs=[pl.BlockSpec(memory_space=pl.ANY)] * n_arr,
        scratch_shapes=[dma((n,)), dma((n, 3)), dma((n, 3)), dma((n, 4)), dma((n, 4)), dma((n, 8)), dma((n, 8)), dma((n, 16)), dma((n, 16))],
        compiler_params=pltpu.CompilerParams(collective_id=collective_id, has_side_effects=True, vmem_limit_bytes=nbytes + (8 << 20)),
        cost_estimate=pl.CostEstimate(flops=200_000_000, bytes_accessed=nbytes * 64, transcendentals=0),
        name='gather_all',
    )(*blocks)


def _scatter_kernel(specs, *refs):
    n = len(specs)
    n_pair = sum(1 for s in specs if s[3])
    ins = refs[:n]
    outs = refs[n:2 * n]
    k = 2 * n
    ra = refs[k:k + n]
    rb = refs[k + n:k + 2 * n]
    rz = refs[k + 2 * n:k + 3 * n]
    k += 3 * n
    rd = list(refs[k:k + n_pair])
    k += n_pair
    stage = refs[k:k + n]
    sent = refs[k + n:k + 2 * n]
    k += 2 * n
    (load_sem, d_send, d_recv, a_send, a_recv, b_send, b_recv, z_send, z_recv) = refs[k:]
    d_of = []
    for s in specs:
        d_of.append(rd.pop(0) if s[3] else None)
    me = lax.axis_index(AXIS_NAME)
    core, a, b, z, a_str, b_str = _coords(me)
    a_nbr = me + (1 - 2 * a) * a_str
    b_nbr = me + (1 - 2 * b) * b_str
    partner = me + 1 - 2 * core
    z_base = me - 8 * z
    z_peer = [z_base + 8 * ((z + 1 + i) % 4) for i in range(3)]
    _barrier([a_nbr, b_nbr, partner] + z_peer)

    def chip(ka, kb, kz):
        return (8 * kz + ka * a_str + kb * b_str) // 2

    def s1_chip(s, a, b, a_str, b_str):
        far = 1 - s // 4
        kb = b + far * (1 - 2 * b)
        return (8 * (s % 4) + (1 - a) * a_str + kb * b_str) // 2

    def s2_chip(s):
        return chip(a, 1 - b, s)

    def d_order(s, a, b, a_str, b_str):
        in1 = (s < 8).astype(jnp.int32) if not isinstance(s, int) else int(s < 8)
        t = s - 8
        k1 = s1_chip(s % 8, a, b, a_str, b_str)
        kb = b + (1 - (t // 4) % 2) * (1 - 2 * b)
        k2 = (8 * (s % 4) + a * a_str + kb * b_str) // 2
        return in1 * k1 + (1 - in1) * k2

    started = []
    for p, (rows, cols, dtype, paired) in enumerate(specs):
        if not paired:
            continue
    for s in range(16):
        for p, (rows, cols, dtype, paired) in enumerate(specs):
            if paired:
                kc = d_order(s, b, a, b_str, a_str)
                copy = _remote(ins[p].at[2 * kc + 1 - core], d_of[p].at[kc], d_send.at[p, s], d_recv.at[p, kc], partner)
                copy.start()
                started.append(copy)

    def term(p, kc):
        return ins[p].at[2 * kc + core] if specs[p][3] else ins[p].at[kc]

    def landed(ref, sem):
        pltpu.make_async_copy(ref, ref, sem).wait()

    def add_up(p, operands, dst):
        rows, cols, dtype, _ = specs[p]
        loads = []
        for o, (ref, sem) in enumerate(operands):
            if sem is not None:
                landed(ref, sem)
            load = pltpu.make_async_copy(ref, stage[p].at[o], load_sem.at[p, o])
            load.start()
            loads.append(load)
        for load in loads:
            load.wait()
        step = 8 if dtype == F32 else 16

        def body(r, _):
            at = pl.ds(pl.multiple_of(r * step, step), step)
            total = stage[p][0, at, :].astype(F32)
            for o in range(1, len(operands)):
                total = total + stage[p][o, at, :].astype(F32)
            dst[at, :] = total.astype(dtype)
            return 0

        lax.fori_loop(0, rows // step, body, 0)

    def base(p, kc):
        ops = [(term(p, kc), None)]
        if specs[p][3]:
            ops.append((d_of[p].at[kc], d_recv.at[p, kc]))
        return ops

    def s1(s, carry):
        kc = s1_chip(s, a, b, a_str, b_str)
        for p in range(n):
            add_up(p, base(p, kc), sent[p].at[s])
            _remote(sent[p].at[s], ra[p].at[s], a_send.at[p, s], a_recv.at[p, s], a_nbr).start()
        return carry

    lax.fori_loop(0, 8, s1, 0)

    def s2(s, carry):
        kc = s2_chip(s)
        for p in range(n):
            add_up(p, base(p, kc) + [(ra[p].at[s], a_recv.at[p, s])], sent[p].at[8 + s])
            _remote(sent[p].at[8 + s], rb[p].at[s], b_send.at[p, s], b_recv.at[p, s], b_nbr).start()
        return carry

    lax.fori_loop(0, 4, s2, 0)

    def last(p, kz):
        return base(p, chip(a, b, kz)) + [(ra[p].at[4 + kz], a_recv.at[p, 4 + kz]), (rb[p].at[kz], b_recv.at[p, kz])]

    def s3(i, carry):
        kz = (z + 1 + i) % 4
        for p in range(n):
            add_up(p, last(p, kz), sent[p].at[12 + i])
            _remote(sent[p].at[12 + i], rz[p].at[i], z_send.at[p, i], z_recv.at[p, i], z_base + 8 * kz).start()
        return carry

    lax.fori_loop(0, 3, s3, 0)
    for p in range(n):
        add_up(p, last(p, z) + [(rz[p].at[i], z_recv.at[p, i]) for i in range(3)], outs[p])
    for copy in started:
        copy.wait_send()

    def drain(sem, count, lo):
        def body(s, carry):
            for p in range(n):
                _remote(sent[p].at[lo + s], sent[p].at[lo + s], sem.at[p, s], sem.at[p, s], me).wait_send()
            return carry
        lax.fori_loop(0, count, body, 0)

    drain(a_send, 8, 0)
    drain(b_send, 4, 8)
    drain(z_send, 3, 12)


def scatter_sum(pieces, paired, collective_id):
    specs = tuple((v.shape[1], v.shape[2], jnp.dtype(v.dtype), pr) for v, pr in zip(pieces, paired))
    n = len(specs)
    dma = pltpu.SemaphoreType.DMA
    hbm = pl.BlockSpec(memory_space=pl.ANY)
    sds = jax.ShapeDtypeStruct
    outs = [sds((r, c), d) for r, c, d, _ in specs]
    lands = [sds((m, r, c), d) for m in (8, 4, 3) for r, c, d, _ in specs]
    lands += [sds((16, r, c), d) for r, c, d, pr in specs if pr]
    scratch = [pltpu.VMEM((7 if pr else 6, r, c), d) for r, c, d, pr in specs]
    scratch += [pltpu.VMEM((15, r, c), d) for r, c, d, _ in specs]
    scratch += [dma((n, 7)), dma((n, 16)), dma((n, 16)), dma((n, 8)), dma((n, 8)), dma((n, 4)), dma((n, 4)), dma((n, 3)), dma((n, 3))]
    nbytes = sum(r * c * d.itemsize * (16 + 7) for r, c, d, _ in specs)
    res = pl.pallas_call(
        functools.partial(_scatter_kernel, specs),
        out_shape=outs + lands,
        in_specs=[hbm] * n,
        out_specs=[pl.BlockSpec(memory_space=pltpu.VMEM)] * n + [hbm] * len(lands),
        scratch_shapes=scratch,
        compiler_params=pltpu.CompilerParams(collective_id=collective_id, has_side_effects=True, vmem_limit_bytes=nbytes + (6 << 20)),
        cost_estimate=pl.CostEstimate(flops=200_000_000, bytes_accessed=nbytes * 4, transcendentals=0),
        name='scatter_sum',
    )(*pieces)
    return res[:n]


def solution(mesh):
    n_dev = mesh.shape[AXIS_NAME]
    n_chip = n_dev // 2
    pair = [(i, i ^ 1) for i in range(n_dev)]
    groups = [[2 * k + c for k in range(n_chip)] for c in range(2)]
    to_use = [(d, 2 * (d % n_chip) + d // n_chip) for d in range(n_dev)]
    to_store = [(b, a) for a, b in to_use]

    row_spec = P(AXIS_NAME, None)
    vec_spec = P(AXIS_NAME)
    full_spec = P(None)
    batch_spec = P(AXIS_NAME, None, None)
    weight_specs = (vec_spec, row_spec, row_spec, row_spec, full_spec, full_spec, row_spec, vec_spec, row_spec, row_spec, row_spec)

    def swap(v):
        return lax.ppermute(v, AXIS_NAME, pair)

    def gather_group(v):
        return lax.all_gather(v, AXIS_NAME, axis_index_groups=groups, tiled=True)

    def device_step(tokens, positions, table_shard, attn_norm, w_query, w_key, w_value, q_norm, k_norm, w_out, mlp_norm, w_gate, w_up, w_down, dy_out):
        me = lax.axis_index(AXIS_NAME)
        core = lax.rem(me, 2)
        seq_len = tokens.shape[1]
        rows_local, model_dim = table_shard.shape
        rows_w, ff = w_gate.shape
        half = ff // 2
        nq, nk = w_query.shape[1], w_key.shape[1]
        head_dim = q_norm.shape[0]
        kv_heads = nk // head_dim
        q_per_kv = nq // nk

        gains = jnp.pad(jnp.stack([attn_norm, mlp_norm], axis=1), ((0, 0), (0, 126)))
        attn_pack = jnp.concatenate([w_query, w_out, w_key, w_value, gains], axis=1)
        attn_full = gather_all([attn_pack], [1], n_dev, 1)[0].reshape(-1, attn_pack.shape[1])
        mine_gu = jnp.concatenate([lax.dynamic_slice(w_gate, (0, core * half), (rows_w, half)), lax.dynamic_slice(w_up, (0, core * half), (rows_w, half))], axis=1)
        other_gu = jnp.concatenate([lax.dynamic_slice(w_gate, (0, (1 - core) * half), (rows_w, half)), lax.dynamic_slice(w_up, (0, (1 - core) * half), (rows_w, half))], axis=1)
        recv_gu = swap(other_gu)
        block_gu = jnp.where(core == 0, jnp.concatenate([mine_gu, recv_gu], axis=0), jnp.concatenate([recv_gu, mine_gu], axis=0))
        wgu = gather_group(block_gu)
        wd = gather_group(lax.ppermute(w_down, AXIS_NAME, to_use))
        w_g, w_u = wgu[:, :half], wgu[:, half:]

        all_ids = all_rows(jnp.pad(tokens.reshape(-1, 128), ((0, 4), (0, 0))), n_dev, 0)[:, :seq_len // 128].reshape(-1)
        local_ids = all_ids - me * rows_local
        is_owner = (local_ids >= 0) & (local_ids < rows_local)
        picked = jnp.take(table_shard, jnp.clip(local_ids, 0, rows_local - 1), axis=0)
        picked = jnp.where(is_owner[:, None], picked, jnp.zeros((), picked.dtype)).reshape(n_dev, seq_len, model_dim)
        x_emb = scatter_sum([picked], [True], 2)[0]

        dy = dy_out.reshape(seq_len, model_dim)
        dy2 = jnp.concatenate([dy, swap(dy)], axis=0)

        wq = attn_full[:, :nq]
        wo = attn_full[:, nq:2 * nq]
        wk = attn_full[:, 2 * nq:2 * nq + nk]
        wv = attn_full[:, 2 * nq + nk:2 * nq + 2 * nk]
        g_attn = attn_full[:, 2 * nq + 2 * nk]
        g_mlp = attn_full[:, 2 * nq + 2 * nk + 1]

        cos_t, sin_t = rope_tables(positions, head_dim)
        cos_q, sin_q = cos_t[:, :, None, None, :], sin_t[:, :, None, None, :]
        cos_k, sin_k = cos_t[:, :, None, :], sin_t[:, :, None, :]
        normed1, norm1_inv = norm_fwd(x_emb)
        attn_in = (normed1 * g_attn.astype(F32)).astype(BF16)
        q_raw = dot(attn_in, wq, 1, 0).astype(BF16).reshape(1, seq_len, kv_heads, q_per_kv, head_dim)
        k_raw = dot(attn_in, wk, 1, 0).astype(BF16).reshape(1, seq_len, kv_heads, head_dim)
        v_raw = dot(attn_in, wv, 1, 0).astype(BF16).reshape(1, seq_len, kv_heads, head_dim)
        q_normed, q_inv = norm_fwd(q_raw)
        k_normed, k_inv = norm_fwd(k_raw)
        q_rot = rotate(q_normed * q_norm.astype(F32), cos_q, sin_q).astype(BF16)
        k_rot = rotate(k_normed * k_norm.astype(F32), cos_k, sin_k).astype(BF16)
        attn_heads, attn_probs = attn_fwd(q_rot, k_rot, v_raw)
        attn_flat = attn_heads.reshape(seq_len, nq)
        hidden = (x_emb.astype(F32) + dot(attn_flat, wo, 1, 0)).astype(BF16)
        normed2, norm2_inv = norm_fwd(hidden)
        mlp_in = (normed2 * g_mlp.astype(F32)).astype(BF16)

        mlp2 = jnp.concatenate([mlp_in, swap(mlp_in)], axis=0)
        gate_pre = dot(mlp2, w_g, 1, 0)
        up_proj = dot(mlp2, w_u, 1, 0)
        gate_sig = jax.nn.sigmoid(gate_pre)
        mlp_act = (gate_pre * gate_sig * up_proj).astype(BF16)
        grad_w_down = dot(mlp_act, dy2, 0, 0)
        grad_act = dot(dy2, wd, 1, 1)
        grad_gate = (grad_act * up_proj * gate_sig * (1.0 + gate_pre * (1.0 - gate_sig))).astype(BF16)
        grad_up = (grad_act * gate_pre * gate_sig).astype(BF16)
        part_in = dot(grad_gate, w_g, 1, 1) + dot(grad_up, w_u, 1, 1)
        grad_mlp_in = part_in[:seq_len] + swap(part_in[seq_len:])
        grad_w_gate = dot(mlp2, grad_gate, 0, 0)
        grad_w_up = dot(mlp2, grad_up, 0, 0)
        part_y = dot(mlp_act, wd, 1, 0)
        layer_out = (hidden.astype(F32) + (part_y[:seq_len] + swap(part_y[seq_len:]))).astype(BF16)

        grad_mlp_norm = jnp.sum(grad_mlp_in * normed2, axis=0)
        grad_hidden = dy.astype(F32) + norm_bwd(grad_mlp_in, normed2, norm2_inv, g_mlp)
        hidden_b = grad_hidden.astype(BF16)
        grad_w_out = dot(attn_flat, hidden_b, 0, 0)
        grad_heads = dot(hidden_b, wo, 1, 1).reshape(q_rot.shape)
        grad_q, grad_k, grad_v = attn_bwd(grad_heads, q_rot, k_rot, v_raw, attn_probs)
        grad_qt = rotate(grad_q, cos_q, -sin_q)
        grad_kt = rotate(grad_k, cos_k, -sin_k)
        grad_q_norm = jnp.sum(grad_qt * q_normed, axis=(0, 1, 2, 3))
        grad_k_norm = jnp.sum(grad_kt * k_normed, axis=(0, 1, 2))
        grad_q_raw = norm_bwd(grad_qt, q_normed, q_inv, q_norm).astype(BF16).reshape(seq_len, nq)
        grad_k_raw = norm_bwd(grad_kt, k_normed, k_inv, k_norm).astype(BF16).reshape(seq_len, nk)
        grad_v_raw = grad_v.astype(BF16).reshape(seq_len, nk)
        grad_attn_in = dot(grad_q_raw, wq, 1, 1) + dot(grad_k_raw, wk, 1, 1) + dot(grad_v_raw, wv, 1, 1)
        grad_attn_norm = jnp.sum(grad_attn_in * normed1, axis=0)
        grad_x_emb = grad_hidden + norm_bwd(grad_attn_in, normed1, norm1_inv, g_attn)

        qk = jnp.pad(jnp.concatenate([grad_q_norm, grad_k_norm])[None], ((0, 7), (0, 0)))
        all_dx, all_qk = gather_all([grad_x_emb, qk], [2, 1], n_dev, 4)
        d_table = jax.ops.segment_sum(all_dx.reshape(-1, model_dim), jnp.where(is_owner, local_ids, rows_local), num_segments=rows_local)
        qk = jnp.sum(all_qk[:, 0], axis=0)

        grad_w_query = dot(attn_in, grad_q_raw, 0, 0)
        grad_w_key = dot(attn_in, grad_k_raw, 0, 0)
        grad_w_value = dot(attn_in, grad_v_raw, 0, 0)
        vecs = jnp.pad(jnp.stack([grad_attn_norm, grad_mlp_norm], axis=1), ((0, 0), (0, 126)))
        zeros = jnp.zeros_like(vecs)
        pack0 = jnp.concatenate([grad_w_query, grad_w_key, vecs], axis=1)
        pack1 = jnp.concatenate([grad_w_out, grad_w_value, zeros], axis=1)
        packs = jnp.stack([pack0.reshape(n_chip, 2 * rows_w, -1), pack1.reshape(n_chip, 2 * rows_w, -1)], axis=1).reshape(n_dev, 2 * rows_w, -1)
        by_chip = [v.reshape(n_chip, -1, v.shape[1]) for v in (grad_w_down, grad_w_gate, grad_w_up)]
        down_rows, gate_shard, up_shard, attn_shard = scatter_sum(by_chip + [packs], [False, False, False, True], 3)
        down_shard = lax.ppermute(down_rows, AXIS_NAME, to_store)

        chip_rows = jnp.concatenate([gate_shard, up_shard, attn_shard], axis=1)
        mine = lax.dynamic_slice(chip_rows, (core * rows_w, 0), (rows_w, chip_rows.shape[1]))
        recv = swap(lax.dynamic_slice(chip_rows, ((1 - core) * rows_w, 0), (rows_w, chip_rows.shape[1])))
        low = jnp.where(core == 0, mine, recv)
        high = jnp.where(core == 0, recv, mine)
        d_gate = jnp.concatenate([low[:, :half], high[:, :half]], axis=1)
        d_up = jnp.concatenate([low[:, half:ff], high[:, half:ff]], axis=1)
        d_query, d_key = low[:, ff:ff + nq], low[:, ff + nq:ff + nq + nk]
        d_attn_norm, d_mlp_norm = low[:, ff + nq + nk], low[:, ff + nq + nk + 1]
        d_out, d_value = high[:, ff:ff + nq], high[:, ff + nq:ff + nq + nk]
        return (layer_out.reshape(1, seq_len, model_dim), d_table, d_attn_norm, d_query, d_key, d_value, qk[:head_dim], qk[head_dim:], d_out, d_mlp_norm, d_gate, d_up, down_shard)

    return jax.shard_map(device_step, mesh=mesh, in_specs=(row_spec, row_spec, row_spec) + weight_specs + (batch_spec,), out_specs=(batch_spec, row_spec) + weight_specs, check_vma=False)
```

```python
import functools
import math
import jax
import jax.numpy as jnp
from jax import lax
from jax.experimental import pallas as pl
from jax.experimental.pallas import tpu as pltpu
from jax.sharding import PartitionSpec as P

NORM_EPS = 1e-6
ROPE_THETA = 1.0e6
AXIS_NAME = 'fsdp'
F32 = jnp.float32
BF16 = jnp.bfloat16
MESH = pl.DeviceIdType.MESH


def rope_tables(positions, head_dim):
    half_dim = head_dim // 2
    inv_freq = jnp.exp(jnp.arange(half_dim, dtype=jnp.float32) * (-2.0 * math.log(ROPE_THETA) / head_dim))
    angles = positions.astype(jnp.float32)[:, :, None] * inv_freq
    return jnp.cos(angles), jnp.sin(angles)


def rotate(values, cos_t, sin_t):
    half_dim = values.shape[-1] // 2
    lead_half = values[..., :half_dim]
    tail_half = values[..., half_dim:]
    return jnp.concatenate([lead_half * cos_t - tail_half * sin_t, tail_half * cos_t + lead_half * sin_t], axis=-1)


def norm_fwd(values):
    values_f = values.astype(jnp.float32)
    inv_rms = lax.rsqrt(jnp.mean(values_f * values_f, axis=-1, keepdims=True) + NORM_EPS)
    return values_f * inv_rms, inv_rms


def norm_bwd(grad_out, normed, inv_rms, norm_gain):
    grad_normed = grad_out * norm_gain.astype(jnp.float32)
    mean_term = jnp.mean(grad_normed * normed, axis=-1, keepdims=True)
    return inv_rms * (grad_normed - normed * mean_term)


def attn_fwd(q_rot, k_rot, v_raw):
    seq_len = q_rot.shape[1]
    attn_scale = q_rot.shape[-1] ** -0.5
    scores = jnp.einsum('bqgrh,bkgh->bgrqk', q_rot, k_rot, preferred_element_type=jnp.float32) * attn_scale
    causal = lax.broadcasted_iota(jnp.int32, (seq_len, seq_len), 0) >= lax.broadcasted_iota(jnp.int32, (seq_len, seq_len), 1)
    attn_probs = jax.nn.softmax(jnp.where(causal, scores, -1e30), axis=-1)
    attn_heads = jnp.einsum('bgrqk,bkgh->bqgrh', attn_probs.astype(jnp.bfloat16), v_raw, preferred_element_type=jnp.float32)
    return attn_heads.astype(jnp.bfloat16), attn_probs


def attn_bwd(grad_out, q_rot, k_rot, v_raw, attn_probs):
    attn_scale = q_rot.shape[-1] ** -0.5
    grad_b = grad_out.astype(jnp.bfloat16)
    probs_b = attn_probs.astype(jnp.bfloat16)
    grad_probs = jnp.einsum('bqgrh,bkgh->bgrqk', grad_b, v_raw, preferred_element_type=jnp.float32)
    grad_v = jnp.einsum('bgrqk,bqgrh->bkgh', probs_b, grad_b, preferred_element_type=jnp.float32)
    grad_scores = attn_probs * (grad_probs - jnp.sum(grad_probs * attn_probs, axis=-1, keepdims=True)) * attn_scale
    scores_b = grad_scores.astype(jnp.bfloat16)
    grad_q = jnp.einsum('bgrqk,bkgh->bqgrh', scores_b, k_rot, preferred_element_type=jnp.float32)
    grad_k = jnp.einsum('bgrqk,bqgrh->bkgh', scores_b, q_rot, preferred_element_type=jnp.float32)
    return grad_q, grad_k, grad_v


def dot(a, b, ca, cb):
    return lax.dot_general(a, b, (((ca,), (cb,)), ((), ())), preferred_element_type=F32)


def _unpack(code):
    return code // 64, code // 32 % 2, code // 8 % 4, code % 8


def _via(u, key, orders):
    da, db, p, piece = key
    last = None
    for axis in orders[piece]:
        if axis == 'a' and da or axis == 'b' and db:
            last = axis
        if axis == 'z' and p != u:
            last = 'z+' if p > u else 'z-'
    return last


def _onward(u, key, orders):
    order = orders[key[3]]
    via = _via(u, key, orders)
    left = order if via is None else order[order.index(via[0]) + 1:]
    out = []
    if u < 3 and (via == 'z-' or 'z' in left):
        out.append('z+')
    if u > 0 and (via == 'z+' or 'z' in left):
        out.append('z-')
    return out + [axis for axis in 'ba' if axis in left]


def _seen_by_parent(u, key, orders):
    da, db, p, piece = key
    via = _via(u, key, orders)
    if via == 'a':
        return u, (0, db, p, piece), 'a'
    if via == 'b':
        return u, (da, 0, p, piece), 'b'
    if via == 'z-':
        return u - 1, key, 'z+'
    if u == 0:
        return 1, key, 'z-'
    return 1, (da, db, 3 - p, piece), 'z+'


class _Place:
    def __init__(self, me, swapped=False):
        self.me = me
        self.core = me % 2
        x, y, self.z = (me // 2) % 2, (me // 4) % 2, me // 8
        other = 1 - self.core if swapped else self.core
        self.a = y * (1 - other) + x * other
        self.b = x * (1 - other) + y * other
        self.a_str, self.b_str = 4 - 2 * other, 2 + 2 * other
        self.far = self.z // 2
        self.u = 3 * self.far + (1 - 2 * self.far) * self.z
        self.partner = me + 1 - 2 * self.core

    def chip(self, key):
        da, db, p = key[:3]
        a = self.a + da * (1 - 2 * self.a)
        b = self.b + db * (1 - 2 * self.b)
        z = 3 * self.far + (1 - 2 * self.far) * p
        return (8 * z + a * self.a_str + b * self.b_str) // 2

    def side(self, name):
        if name == 'a':
            return self.me + (1 - 2 * self.a) * self.a_str
        if name == 'b':
            return self.me + (1 - 2 * self.b) * self.b_str
        return self.me + 8 * (1 - 2 * self.far) * (1 if name == 'z+' else -1)


def _remote(src, dst, send_sem, recv_sem, dev):
    return pltpu.make_async_remote_copy(src_ref=src, dst_ref=dst, send_sem=send_sem, recv_sem=recv_sem, device_id=(dev,), device_id_type=MESH)


def _meet(peers, me=None, ends=()):
    sem = pltpu.get_barrier_semaphore()

    def meet(everyone):
        for peer in everyone:
            pl.semaphore_signal(sem, inc=1, device_id=(peer,), device_id_type=MESH)
        pl.semaphore_wait(sem, len(everyone))

    if not ends:
        meet(peers)
        return
    to, frm = ends
    pl.when(to != me)(lambda: meet(peers + [to, frm]))
    pl.when(to == me)(lambda: meet(peers))


def _landed(ref, sem):
    pltpu.make_async_copy(ref, ref, sem).wait()


def _passes(moves, me):
    for kind in moves:
        if kind == 'pair':
            other = me + 1 - 2 * (me % 2)
            yield other, other
        elif kind == 'use':
            yield 2 * (me % 16) + me // 16, 16 * (me % 2) + me // 2
        else:
            yield 16 * (me % 2) + me // 2, 2 * (me % 16) + me // 16


def _start_move(kind, src, dst, send_sem, recv_sem, to, me):
    copy = _remote(src, dst, send_sem, recv_sem, to)
    if kind == 'pair':
        copy.start()
    else:
        pl.when(to != me)(copy.start)
        pl.when(to == me)(pltpu.make_async_copy(src, dst, recv_sem).start)
    return copy


def _end_move(kind, copy, dst, recv_sem, to, me):
    _landed(dst, recv_sem)
    if kind == 'pair':
        copy.wait_send()
    else:
        pl.when(to != me)(copy.wait_send)


def _all_rows_kernel(n_dev, moves, *refs):
    n = len(moves)
    in_ref, src, out_ref, dst = refs[0], refs[1:1 + n], refs[1 + n], refs[2 + n:2 + 2 * n]
    send_sem, recv_sem, m_send, m_recv = refs[2 + 2 * n:]
    me = lax.axis_index(AXIS_NAME)
    peers = [(me + d) % n_dev for d in range(1, n_dev)]
    _meet(peers)
    copies = [_remote(in_ref, out_ref.at[me], send_sem.at[i], recv_sem.at[i], peer) for i, peer in enumerate(peers)]
    for copy in copies:
        copy.start()
    ends = [to for to, _ in _passes(moves, me)]
    moving = [_start_move(moves[i], src[i], dst[i], m_send.at[i], m_recv.at[i], to, me) for i, to in enumerate(ends)]
    out_ref[me] = in_ref[...]
    for copy in copies:
        copy.wait()
    for i, copy in enumerate(moving):
        _end_move(moves[i], copy, dst[i], m_recv.at[i], ends[i], me)


def all_rows(block, n_dev, moved, moves, collective_id):
    n = len(moves)
    dma = pltpu.SemaphoreType.DMA
    vmem, hbm = pl.BlockSpec(memory_space=pltpu.VMEM), pl.BlockSpec(memory_space=pl.ANY)
    res = pl.pallas_call(
        functools.partial(_all_rows_kernel, n_dev, moves),
        out_shape=[jax.ShapeDtypeStruct((n_dev,) + block.shape, block.dtype)] + [jax.ShapeDtypeStruct(v.shape, v.dtype) for v in moved],
        in_specs=[vmem] + [hbm] * n,
        out_specs=[vmem] + [hbm] * n,
        scratch_shapes=[dma((n_dev - 1,)), dma((n_dev - 1,)), dma((n,)), dma((n,))],
        compiler_params=pltpu.CompilerParams(collective_id=collective_id, has_side_effects=True),
        cost_estimate=pl.CostEstimate(flops=10_000_000, bytes_accessed=1 << 20, transcendentals=0),
        name='all_rows',
    )(block, *moved)
    return res[0], res[1:]


def _gather_kernel(cuts, orders, seq, moves, *refs):
    n = len(moves)
    in_ref, src, out_ref, dst = refs[0], refs[1:1 + n], refs[1 + n], refs[2 + n:2 + 2 * n]
    own_sem, send_sem, recv_sem, p_send, p_recv, m_send, m_recv = refs[2 + 2 * n:]
    me = lax.axis_index(AXIS_NAME)
    at = _Place(me)
    ends = list(_passes(moves, me))
    starts = [sum(cuts[:i]) for i in range(len(cuts))]

    def part(slot, piece):
        return out_ref.at[slot] if len(cuts) == 1 else out_ref.at[slot, pl.ds(starts[piece], cuts[piece])]

    def run(u):
        sides = ['a', 'b', 'z+'] + (['z-'] if u else [])
        far = [end for kind, end in zip(moves, ends) if kind != 'pair']
        _meet([at.side(s) for s in sides] + [at.partner], me, far[0] if far else ())
        started, moving = [], []

        def send(src_ref, slot, piece, s_sem, r_sem, dev):
            copy = _remote(src_ref, part(slot, piece), s_sem, r_sem, dev)
            copy.start()
            started.append(copy)

        own = pltpu.make_async_copy(in_ref, out_ref.at[me], own_sem)
        own.start()
        count, handed = 0, [0] * len(cuts)
        for key in [(0, 0, u, i) for i in range(len(cuts))] + [_unpack(c) for c in seq[u]]:
            piece = key[3]
            kc = at.chip(key)
            slot = 2 * kc + at.core
            if _via(u, key, orders) is None:
                ref = in_ref if len(cuts) == 1 else in_ref.at[pl.ds(starts[piece], cuts[piece])]
            else:
                ref = part(slot, piece)
                _landed(ref, recv_sem.at[piece, kc])
            for side in _onward(u, key, orders):
                send(ref, slot, piece, send_sem.at[count], recv_sem.at[piece, kc], at.side(side))
                count += 1
            send(ref, slot, piece, p_send.at[piece, handed[piece]], p_recv.at[piece, kc], at.partner)
            handed[piece] += 1
            if key[:3] == (0, 0, u) and piece == len(cuts) - 1:
                for i, (to, _) in enumerate(ends):
                    moving.append(_start_move(moves[i], src[i], dst[i], m_send.at[i], m_recv.at[i], to, me))
        for piece in range(len(cuts)):
            for kc in range(16):
                _landed(part(2 * kc + 1 - at.core, piece), p_recv.at[piece, kc])
        for i, (to, _) in enumerate(ends):
            _end_move(moves[i], moving[i], dst[i], m_recv.at[i], to, me)
        own.wait()
        for copy in started:
            copy.wait_send()

    for u in (0, 1):
        pl.when(at.u == u)(functools.partial(run, u))


def gather_all(block, cuts, orders, seq, moved, moves, n_dev, collective_id):
    n, m = len(moves), len(cuts)
    dma = pltpu.SemaphoreType.DMA
    vmem, hbm = pl.BlockSpec(memory_space=pltpu.VMEM), pl.BlockSpec(memory_space=pl.ANY)
    nbytes = block.size * block.dtype.itemsize
    res = pl.pallas_call(
        functools.partial(_gather_kernel, cuts, orders, seq, moves),
        out_shape=[jax.ShapeDtypeStruct((n_dev,) + block.shape, block.dtype)] + [jax.ShapeDtypeStruct(v.shape, v.dtype) for v in moved],
        in_specs=[vmem] + [hbm] * n,
        out_specs=[hbm] * (1 + n),
        scratch_shapes=[dma, dma((24 * m,)), dma((m, 16)), dma((m, 16)), dma((m, 16)), dma((max(n, 1),)), dma((max(n, 1),))],
        compiler_params=pltpu.CompilerParams(collective_id=collective_id, has_side_effects=True, vmem_limit_bytes=nbytes + (8 << 20)),
        cost_estimate=pl.CostEstimate(flops=200_000_000, bytes_accessed=nbytes * 64, transcendentals=0),
        name='gather_all',
    )(block, *moved)
    return res[0], res[1:]


def _slots(pieces, orders, seq):
    table, most = {}, [1] * len(pieces)
    for u in (0, 1):
        used = [0] * len(pieces)
        for key in [_unpack(c) for c in reversed(seq[u])] + [(0, 0, u, i) for i in range(len(pieces))]:
            for side in _onward(u, key, orders):
                table[u, key, side] = used[key[3]]
                used[key[3]] += 1
        most = [max(a, b) for a, b in zip(most, used)]
    return table, most


def _scatter_kernel(pieces, orders, seq, n_arr, *refs):
    table, _ = _slots(pieces, orders, seq)
    n = len(pieces)
    n_pair = sum(1 for p in pieces if p[3])
    ins, outs = refs[:n_arr], refs[n_arr:2 * n_arr]
    k = 2 * n_arr
    land, stage, pair = refs[k:k + n], refs[k + n:k + 2 * n], list(refs[k + 2 * n:k + 2 * n + n_pair])
    load_sem, send_sem, recv_sem, d_send, d_recv = refs[k + 2 * n + n_pair:]
    got = [pair.pop(0) if p[3] else None for p in pieces]
    me = lax.axis_index(AXIS_NAME)
    at, partner_at = _Place(me), _Place(me, swapped=True)

    def rows_of(ref, piece):
        arr, r0, rows, _ = pieces[piece]
        return ref if rows == ins[arr].shape[1] else ref.at[pl.ds(r0, rows)]

    def term(piece, kc, core):
        arr, _, _, paired = pieces[piece]
        return rows_of(ins[arr].at[2 * kc + core if paired else kc], piece)

    def run(u):
        sides = ['a', 'b', 'z+'] + (['z-'] if u else [])
        _meet([at.side(s) for s in sides] + [at.partner])
        keys = [_unpack(c) for c in reversed(seq[u])] + [(0, 0, u, i) for i in range(n)]
        started = []
        given = [0] * n
        for key in keys:
            piece = key[3]
            if pieces[piece][3]:
                kc = partner_at.chip(key)
                copy = _remote(term(piece, kc, 1 - at.core), got[piece].at[kc], d_send.at[piece, given[piece]], d_recv.at[piece, kc], at.partner)
                given[piece] += 1
                copy.start()
                started.append(copy)
        adds = [[key for key in keys if key[3] == i and (pieces[i][3] or _onward(u, key, orders))] for i in range(n)]

        def load(piece, j):
            return pltpu.make_async_copy(term(piece, at.chip(adds[piece][j]), at.core), stage[piece].at[j % 2], load_sem.at[piece, j % 2])

        for i in range(n):
            for j in range(2):
                load(i, j).start()
        done = [0] * n
        count = 0
        for key in keys:
            piece = key[3]
            arr, r0, rows, paired = pieces[piece]
            kc = at.chip(key)
            children = _onward(u, key, orders)
            if not children and not paired:
                src = term(piece, kc, at.core)
            else:
                j = done[piece]
                done[piece] += 1
                parts = []
                if paired:
                    _landed(got[piece].at[kc], d_recv.at[piece, kc])
                    parts.append(got[piece].at[kc])
                for side in children:
                    slot = table[u, key, side]
                    _landed(land[piece].at[slot], recv_sem.at[piece, slot])
                    parts.append(land[piece].at[slot])
                load(piece, j).wait()
                parts.append(stage[piece].at[j % 2])
                root = key[:3] == (0, 0, u)
                src = rows_of(outs[arr], piece) if root else parts[0]
                dtype = ins[arr].dtype
                step = 8 if dtype == F32 else 16

                def body(r, _, parts=parts, dst=src, step=step, dtype=dtype):
                    some = pl.ds(pl.multiple_of(r * step, step), step)
                    total = parts[0][some, :].astype(F32)
                    for ref in parts[1:]:
                        total = total + ref[some, :].astype(F32)
                    dst[some, :] = total.astype(dtype)
                    return 0

                lax.fori_loop(0, rows // step, body, 0)
                if j + 2 < len(adds[piece]):
                    load(piece, j + 2).start()
                if root:
                    continue
            side = _via(u, key, orders)
            slot = table[_seen_by_parent(u, key, orders)]
            copy = _remote(src, land[piece].at[slot], send_sem.at[count], recv_sem.at[piece, slot], at.side(side))
            copy.start()
            started.append(copy)
            count += 1
        for copy in started:
            copy.wait_send()

    for u in (0, 1):
        pl.when(at.u == u)(functools.partial(run, u))


def scatter_sum(arrays, pieces, orders, seq, collective_id):
    n_arr, n = len(arrays), len(pieces)
    dma, hbm, vmem = pltpu.SemaphoreType.DMA, pl.BlockSpec(memory_space=pl.ANY), pl.BlockSpec(memory_space=pltpu.VMEM)
    _, most = _slots(pieces, orders, seq)
    shapes = [(rows, arrays[arr].shape[2], arrays[arr].dtype) for arr, _, rows, _ in pieces]
    scratch = [pltpu.VMEM((m, r, c), d) for m, (r, c, d) in zip(most, shapes)]
    scratch += [pltpu.VMEM((2, r, c), d) for r, c, d in shapes]
    scratch += [pltpu.VMEM((16, r, c), d) for (r, c, d), p in zip(shapes, pieces) if p[3]]
    nbytes = sum(v.size // v.shape[0] * v.dtype.itemsize for v in arrays) + sum(
        (m + 2 + 16 * int(p[3])) * (-(-r // 16) * 16) * c * d.itemsize for m, (r, c, d), p in zip(most, shapes, pieces))
    scratch += [dma((n, 2)), dma((16 * n,)), dma((n, max(most))), dma((n, 16)), dma((n, 16))]
    return pl.pallas_call(
        functools.partial(_scatter_kernel, tuple(pieces), orders, seq, n_arr),
        out_shape=[jax.ShapeDtypeStruct(v.shape[1:], v.dtype) for v in arrays],
        in_specs=[hbm] * n_arr,
        out_specs=[vmem] * n_arr,
        scratch_shapes=scratch,
        compiler_params=pltpu.CompilerParams(collective_id=collective_id, has_side_effects=True, vmem_limit_bytes=nbytes + (6 << 20)),
        cost_estimate=pl.CostEstimate(flops=200_000_000, bytes_accessed=nbytes * 4, transcendentals=0),
        name='scatter_sum',
    )(*arrays)


ROWS_SEQ = (
    (8, 32, 64, 9, 33, 65, 10, 34, 66, 16, 40, 72, 96, 17, 41, 48, 18, 42, 74, 73, 97, 49, 98, 24, 80, 104, 25, 56, 57, 81, 105, 26, 50, 82, 112, 113, 58, 90, 88, 89, 122, 120, 106, 121, 114),
    (0, 16, 40, 72, 1, 17, 41, 73, 2, 18, 42, 74, 24, 34, 66, 32, 48, 64, 80, 25, 104, 26, 50, 82, 33, 49, 58, 90, 56, 65, 81, 105, 98, 122, 57, 106, 114, 88, 96, 112, 89, 97, 113, 120, 121),
)
ATTN_SEQ = (
    (8, 32, 64, 16, 40, 72, 96, 24, 48, 80, 104, 56, 88, 112, 120),
    (0, 16, 40, 72, 24, 32, 48, 64, 80, 104, 56, 88, 96, 112, 120),
)
LOOKUP_SEQ = (
    (8, 32, 64, 9, 33, 65, 10, 34, 66, 16, 40, 72, 96, 17, 41, 48, 18, 42, 74, 73, 97, 49, 98, 24, 80, 104, 25, 56, 26, 50, 82, 81, 105, 57, 112, 58, 90, 113, 88, 106, 89, 122, 120, 114, 121),
    (0, 16, 40, 72, 1, 17, 41, 73, 2, 18, 42, 74, 24, 34, 66, 32, 48, 64, 80, 104, 25, 26, 50, 82, 33, 49, 58, 90, 65, 81, 56, 105, 98, 57, 106, 122, 88, 96, 114, 112, 89, 97, 113, 120, 121),
)
GRAD_SEQ = (
    (8, 32, 64, 9, 33, 65, 10, 34, 66, 11, 35, 67, 41, 16, 40, 72, 96, 42, 73, 97, 17, 18, 74, 98, 49, 19, 43, 75, 99, 50, 105, 80, 104, 24, 48, 106, 81, 82, 25, 113, 26, 57, 114, 27, 51, 83, 58, 88, 112, 89, 56, 90, 59, 91, 121, 122, 107, 120, 123, 115),
    (0, 16, 40, 72, 1, 17, 41, 73, 2, 18, 42, 74, 3, 19, 43, 75, 32, 24, 33, 48, 49, 35, 67, 64, 80, 104, 25, 34, 50, 26, 27, 51, 83, 65, 81, 57, 105, 99, 58, 56, 106, 66, 82, 59, 91, 107, 123, 115, 96, 88, 113, 97, 112, 89, 98, 114, 90, 121, 122, 120),
)


def solution(mesh):
    n_dev = mesh.shape[AXIS_NAME]
    n_chip = n_dev // 2
    pair = [(i, i ^ 1) for i in range(n_dev)]
    groups = [[2 * k + c for k in range(n_chip)] for c in range(2)]

    row_spec = P(AXIS_NAME, None)
    vec_spec = P(AXIS_NAME)
    full_spec = P(None)
    batch_spec = P(AXIS_NAME, None, None)
    weight_specs = (vec_spec, row_spec, row_spec, row_spec, full_spec, full_spec, row_spec, vec_spec, row_spec, row_spec, row_spec)

    def swap(v):
        return lax.ppermute(v, AXIS_NAME, pair)

    def gather_group(v):
        return lax.all_gather(v, AXIS_NAME, axis_index_groups=groups, tiled=True)

    def device_step(tokens, positions, table_shard, attn_norm, w_query, w_key, w_value, q_norm, k_norm, w_out, mlp_norm, w_gate, w_up, w_down, dy_out):
        me = lax.axis_index(AXIS_NAME)
        core = lax.rem(me, 2)
        seq_len = tokens.shape[1]
        rows_local, model_dim = table_shard.shape
        rows_w, ff = w_gate.shape
        half = ff // 2
        nq, nk = w_query.shape[1], w_key.shape[1]
        head_dim = q_norm.shape[0]
        kv_heads = nk // head_dim
        q_per_kv = nq // nk

        mine_gu = jnp.concatenate([lax.dynamic_slice(w_gate, (0, core * half), (rows_w, half)), lax.dynamic_slice(w_up, (0, core * half), (rows_w, half))], axis=1)
        other_gu = jnp.concatenate([lax.dynamic_slice(w_gate, (0, (1 - core) * half), (rows_w, half)), lax.dynamic_slice(w_up, (0, (1 - core) * half), (rows_w, half))], axis=1)
        token_rows = jnp.pad(tokens.reshape(-1, 128), ((0, 4), (0, 0)))
        dy = dy_out.reshape(seq_len, model_dim)
        all_tokens, (down_block, recv_gu, dy_other) = all_rows(token_rows, n_dev, [w_down, other_gu, dy], ('use', 'pair', 'pair'), 0)
        block_gu = jnp.where(core == 0, jnp.concatenate([mine_gu, recv_gu], axis=0), jnp.concatenate([recv_gu, mine_gu], axis=0))
        wgu = gather_group(block_gu)
        wd = gather_group(down_block)
        w_g, w_u = wgu[:, :half], wgu[:, half:]

        gains = jnp.pad(jnp.stack([attn_norm, mlp_norm], axis=1), ((0, 0), (0, 126)))
        attn_pack = jnp.concatenate([w_query, w_out, w_key, w_value, gains], axis=1)
        attn_full = gather_all(attn_pack, (rows_w,), ('zba',), ATTN_SEQ, [], (), n_dev, 1)[0].reshape(-1, attn_pack.shape[1])

        all_ids = all_tokens[:, :seq_len // 128].reshape(-1)
        local_ids = all_ids - me * rows_local
        is_owner = (local_ids >= 0) & (local_ids < rows_local)
        picked = jnp.take(table_shard, jnp.clip(local_ids, 0, rows_local - 1), axis=0)
        picked = jnp.where(is_owner[:, None], picked, jnp.zeros((), picked.dtype)).reshape(n_dev, seq_len, model_dim)
        x_emb = scatter_sum([picked], [(0, 0, 192, True), (0, 192, 208, True), (0, 400, 112, True)], ('zba', 'zba', 'baz'), LOOKUP_SEQ, 2)[0]

        dy2 = jnp.concatenate([dy, dy_other], axis=0)

        wq = attn_full[:, :nq]
        wo = attn_full[:, nq:2 * nq]
        wk = attn_full[:, 2 * nq:2 * nq + nk]
        wv = attn_full[:, 2 * nq + nk:2 * nq + 2 * nk]
        g_attn = attn_full[:, 2 * nq + 2 * nk]
        g_mlp = attn_full[:, 2 * nq + 2 * nk + 1]

        cos_t, sin_t = rope_tables(positions, head_dim)
        cos_q, sin_q = cos_t[:, :, None, None, :], sin_t[:, :, None, None, :]
        cos_k, sin_k = cos_t[:, :, None, :], sin_t[:, :, None, :]
        normed1, norm1_inv = norm_fwd(x_emb)
        attn_in = (normed1 * g_attn.astype(F32)).astype(BF16)
        q_raw = dot(attn_in, wq, 1, 0).astype(BF16).reshape(1, seq_len, kv_heads, q_per_kv, head_dim)
        k_raw = dot(attn_in, wk, 1, 0).astype(BF16).reshape(1, seq_len, kv_heads, head_dim)
        v_raw = dot(attn_in, wv, 1, 0).astype(BF16).reshape(1, seq_len, kv_heads, head_dim)
        q_normed, q_inv = norm_fwd(q_raw)
        k_normed, k_inv = norm_fwd(k_raw)
        q_rot = rotate(q_normed * q_norm.astype(F32), cos_q, sin_q).astype(BF16)
        k_rot = rotate(k_normed * k_norm.astype(F32), cos_k, sin_k).astype(BF16)
        attn_heads, attn_probs = attn_fwd(q_rot, k_rot, v_raw)
        attn_flat = attn_heads.reshape(seq_len, nq)
        hidden = (x_emb.astype(F32) + dot(attn_flat, wo, 1, 0)).astype(BF16)
        normed2, norm2_inv = norm_fwd(hidden)
        mlp_in = (normed2 * g_mlp.astype(F32)).astype(BF16)

        mlp2 = jnp.concatenate([mlp_in, swap(mlp_in)], axis=0)
        gate_pre = dot(mlp2, w_g, 1, 0)
        up_proj = dot(mlp2, w_u, 1, 0)
        gate_sig = jax.nn.sigmoid(gate_pre)
        mlp_act = (gate_pre * gate_sig * up_proj).astype(BF16)
        grad_w_down = dot(mlp_act, dy2, 0, 0)
        grad_act = dot(dy2, wd, 1, 1)
        grad_gate = (grad_act * up_proj * gate_sig * (1.0 + gate_pre * (1.0 - gate_sig))).astype(BF16)
        grad_up = (grad_act * gate_pre * gate_sig).astype(BF16)
        part_in = dot(grad_gate, w_g, 1, 1) + dot(grad_up, w_u, 1, 1)
        grad_mlp_in = part_in[:seq_len] + swap(part_in[seq_len:])
        grad_w_gate = dot(mlp2, grad_gate, 0, 0)
        grad_w_up = dot(mlp2, grad_up, 0, 0)
        part_y = dot(mlp_act, wd, 1, 0)
        layer_out = (hidden.astype(F32) + (part_y[:seq_len] + swap(part_y[seq_len:]))).astype(BF16)

        grad_mlp_norm = jnp.sum(grad_mlp_in * normed2, axis=0)
        grad_hidden = dy.astype(F32) + norm_bwd(grad_mlp_in, normed2, norm2_inv, g_mlp)
        hidden_b = grad_hidden.astype(BF16)
        grad_w_out = dot(attn_flat, hidden_b, 0, 0)
        grad_heads = dot(hidden_b, wo, 1, 1).reshape(q_rot.shape)
        grad_q, grad_k, grad_v = attn_bwd(grad_heads, q_rot, k_rot, v_raw, attn_probs)
        grad_qt = rotate(grad_q, cos_q, -sin_q)
        grad_kt = rotate(grad_k, cos_k, -sin_k)
        grad_q_norm = jnp.sum(grad_qt * q_normed, axis=(0, 1, 2, 3))
        grad_k_norm = jnp.sum(grad_kt * k_normed, axis=(0, 1, 2))
        grad_q_raw = norm_bwd(grad_qt, q_normed, q_inv, q_norm).astype(BF16).reshape(seq_len, nq)
        grad_k_raw = norm_bwd(grad_kt, k_normed, k_inv, k_norm).astype(BF16).reshape(seq_len, nk)
        grad_v_raw = grad_v.astype(BF16).reshape(seq_len, nk)
        grad_attn_in = dot(grad_q_raw, wq, 1, 1) + dot(grad_k_raw, wk, 1, 1) + dot(grad_v_raw, wv, 1, 1)
        grad_attn_norm = jnp.sum(grad_attn_in * normed1, axis=0)
        grad_x_emb = grad_hidden + norm_bwd(grad_attn_in, normed1, norm1_inv, g_attn)

        grad_w_query = dot(attn_in, grad_q_raw, 0, 0)
        grad_w_key = dot(attn_in, grad_k_raw, 0, 0)
        grad_w_value = dot(attn_in, grad_v_raw, 0, 0)
        vecs = jnp.pad(jnp.stack([grad_attn_norm, grad_mlp_norm], axis=1), ((0, 0), (0, 126)))
        zeros = jnp.zeros_like(vecs)
        pack0 = jnp.concatenate([grad_w_query, grad_w_key, vecs], axis=1)
        pack1 = jnp.concatenate([grad_w_out, grad_w_value, zeros], axis=1)
        packs = jnp.stack([pack0.reshape(n_chip, 2 * rows_w, -1), pack1.reshape(n_chip, 2 * rows_w, -1)], axis=1).reshape(n_dev, 2 * rows_w, -1)
        by_chip = [v.reshape(n_chip, -1, v.shape[1]) for v in (grad_w_down, grad_w_gate, grad_w_up)]
        down_rows, gate_shard, up_shard, attn_shard = scatter_sum(
            by_chip + [packs], [(i, 0, v.shape[1], False) for i, v in enumerate(by_chip)] + [(3, 0, 2 * rows_w, True)], ('bza', 'zba', 'zba', 'baz'), GRAD_SEQ, 3)

        chip_rows = jnp.concatenate([gate_shard, up_shard, attn_shard], axis=1)
        mine = lax.dynamic_slice(chip_rows, (core * rows_w, 0), (rows_w, chip_rows.shape[1]))
        give = lax.dynamic_slice(chip_rows, ((1 - core) * rows_w, 0), (rows_w, chip_rows.shape[1]))
        qk = jnp.pad(jnp.concatenate([grad_q_norm, grad_k_norm])[None], ((0, 7), (0, model_dim - 2 * head_dim)))
        all_dx, (down_shard, recv) = gather_all(
            jnp.concatenate([grad_x_emb, qk], axis=0), (200, 200, 120), ('zba', 'zba', 'baz'), ROWS_SEQ, [down_rows, give], ('store', 'pair'), n_dev, 4)
        seg = jnp.pad(jnp.where(is_owner, local_ids, rows_local).reshape(n_dev, seq_len), ((0, 0), (0, 8)), constant_values=rows_local)
        d_table = jax.ops.segment_sum(all_dx.reshape(-1, model_dim), seg.reshape(-1), num_segments=rows_local)
        qk = jnp.sum(all_dx[:, seq_len, :2 * head_dim], axis=0)
        low = jnp.where(core == 0, mine, recv)
        high = jnp.where(core == 0, recv, mine)
        d_gate = jnp.concatenate([low[:, :half], high[:, :half]], axis=1)
        d_up = jnp.concatenate([low[:, half:ff], high[:, half:ff]], axis=1)
        d_query, d_key = low[:, ff:ff + nq], low[:, ff + nq:ff + nq + nk]
        d_attn_norm, d_mlp_norm = low[:, ff + nq + nk], low[:, ff + nq + nk + 1]
        d_out, d_value = high[:, ff:ff + nq], high[:, ff + nq:ff + nq + nk]
        return (layer_out.reshape(1, seq_len, model_dim), d_table, d_attn_norm, d_query, d_key, d_value, qk[:head_dim], qk[head_dim:], d_out, d_mlp_norm, d_gate, d_up, down_shard)

    return jax.shard_map(device_step, mesh=mesh, in_specs=(row_spec, row_spec, row_spec) + weight_specs + (batch_spec,), out_specs=(batch_spec, row_spec) + weight_specs, check_vma=False)
```

```python
import functools
import math
import jax
import jax.numpy as jnp
from jax import lax
from jax.experimental import pallas as pl
from jax.experimental.pallas import tpu as pltpu
from jax.sharding import PartitionSpec as P

NORM_EPS = 1e-6
ROPE_THETA = 1.0e6
AXIS_NAME = 'fsdp'
F32 = jnp.float32
BF16 = jnp.bfloat16
MESH = pl.DeviceIdType.MESH


def rope_tables(positions, head_dim):
    half_dim = head_dim // 2
    inv_freq = jnp.exp(jnp.arange(half_dim, dtype=jnp.float32) * (-2.0 * math.log(ROPE_THETA) / head_dim))
    angles = positions.astype(jnp.float32)[:, :, None] * inv_freq
    return jnp.cos(angles), jnp.sin(angles)


def rotate(values, cos_t, sin_t):
    half_dim = values.shape[-1] // 2
    lead_half = values[..., :half_dim]
    tail_half = values[..., half_dim:]
    return jnp.concatenate([lead_half * cos_t - tail_half * sin_t, tail_half * cos_t + lead_half * sin_t], axis=-1)


def norm_fwd(values):
    values_f = values.astype(jnp.float32)
    inv_rms = lax.rsqrt(jnp.mean(values_f * values_f, axis=-1, keepdims=True) + NORM_EPS)
    return values_f * inv_rms, inv_rms


def norm_bwd(grad_out, normed, inv_rms, norm_gain):
    grad_normed = grad_out * norm_gain.astype(jnp.float32)
    mean_term = jnp.mean(grad_normed * normed, axis=-1, keepdims=True)
    return inv_rms * (grad_normed - normed * mean_term)


def attn_fwd(q_rot, k_rot, v_raw):
    seq_len = q_rot.shape[1]
    attn_scale = q_rot.shape[-1] ** -0.5
    scores = jnp.einsum('bqgrh,bkgh->bgrqk', q_rot, k_rot, preferred_element_type=jnp.float32) * attn_scale
    causal = lax.broadcasted_iota(jnp.int32, (seq_len, seq_len), 0) >= lax.broadcasted_iota(jnp.int32, (seq_len, seq_len), 1)
    attn_probs = jax.nn.softmax(jnp.where(causal, scores, -1e30), axis=-1)
    attn_heads = jnp.einsum('bgrqk,bkgh->bqgrh', attn_probs.astype(jnp.bfloat16), v_raw, preferred_element_type=jnp.float32)
    return attn_heads.astype(jnp.bfloat16), attn_probs


def attn_bwd(grad_out, q_rot, k_rot, v_raw, attn_probs):
    attn_scale = q_rot.shape[-1] ** -0.5
    grad_b = grad_out.astype(jnp.bfloat16)
    probs_b = attn_probs.astype(jnp.bfloat16)
    grad_probs = jnp.einsum('bqgrh,bkgh->bgrqk', grad_b, v_raw, preferred_element_type=jnp.float32)
    grad_v = jnp.einsum('bgrqk,bqgrh->bkgh', probs_b, grad_b, preferred_element_type=jnp.float32)
    grad_scores = attn_probs * (grad_probs - jnp.sum(grad_probs * attn_probs, axis=-1, keepdims=True)) * attn_scale
    scores_b = grad_scores.astype(jnp.bfloat16)
    grad_q = jnp.einsum('bgrqk,bkgh->bqgrh', scores_b, k_rot, preferred_element_type=jnp.float32)
    grad_k = jnp.einsum('bgrqk,bqgrh->bkgh', scores_b, q_rot, preferred_element_type=jnp.float32)
    return grad_q, grad_k, grad_v


def dot(a, b, ca, cb):
    return lax.dot_general(a, b, (((ca,), (cb,)), ((), ())), preferred_element_type=F32)


def _unpack(code):
    return code // 64, code // 32 % 2, code // 8 % 4, code % 8


def _via(u, key, orders):
    da, db, p, piece = key
    last = None
    for axis in orders[piece]:
        if axis == 'a' and da or axis == 'b' and db:
            last = axis
        if axis == 'z' and p != u:
            last = 'z+' if p > u else 'z-'
    return last


def _onward(u, key, orders):
    order = orders[key[3]]
    via = _via(u, key, orders)
    left = order if via is None else order[order.index(via[0]) + 1:]
    out = []
    if u < 3 and (via == 'z-' or 'z' in left):
        out.append('z+')
    if u > 0 and (via == 'z+' or 'z' in left):
        out.append('z-')
    return out + [axis for axis in 'ba' if axis in left]


def _seen_by_parent(u, key, orders):
    da, db, p, piece = key
    via = _via(u, key, orders)
    if via == 'a':
        return u, (0, db, p, piece), 'a'
    if via == 'b':
        return u, (da, 0, p, piece), 'b'
    if via == 'z-':
        return u - 1, key, 'z+'
    if u == 0:
        return 1, key, 'z-'
    return 1, (da, db, 3 - p, piece), 'z+'


class _Place:
    def __init__(self, me, swapped=False):
        self.me = me
        self.core = me % 2
        x, y, self.z = (me // 2) % 2, (me // 4) % 2, me // 8
        other = 1 - self.core if swapped else self.core
        self.a = y * (1 - other) + x * other
        self.b = x * (1 - other) + y * other
        self.a_str, self.b_str = 4 - 2 * other, 2 + 2 * other
        self.far = self.z // 2
        self.u = 3 * self.far + (1 - 2 * self.far) * self.z
        self.partner = me + 1 - 2 * self.core

    def chip(self, key):
        da, db, p = key[:3]
        a = self.a + da * (1 - 2 * self.a)
        b = self.b + db * (1 - 2 * self.b)
        z = 3 * self.far + (1 - 2 * self.far) * p
        return (8 * z + a * self.a_str + b * self.b_str) // 2

    def side(self, name):
        if name == 'a':
            return self.me + (1 - 2 * self.a) * self.a_str
        if name == 'b':
            return self.me + (1 - 2 * self.b) * self.b_str
        return self.me + 8 * (1 - 2 * self.far) * (1 if name == 'z+' else -1)


def _remote(src, dst, send_sem, recv_sem, dev):
    return pltpu.make_async_remote_copy(src_ref=src, dst_ref=dst, send_sem=send_sem, recv_sem=recv_sem, device_id=(dev,), device_id_type=MESH)


def _meet(peers, me=None, ends=()):
    sem = pltpu.get_barrier_semaphore()

    def meet(everyone):
        for peer in everyone:
            pl.semaphore_signal(sem, inc=1, device_id=(peer,), device_id_type=MESH)
        pl.semaphore_wait(sem, len(everyone))

    if not ends:
        meet(peers)
        return
    to, frm = ends
    pl.when(to != me)(lambda: meet(peers + [to, frm]))
    pl.when(to == me)(lambda: meet(peers))


def _landed(ref, sem):
    pltpu.make_async_copy(ref, ref, sem).wait()


def _passes(moves, me):
    for kind in moves:
        if kind == 'pair':
            other = me + 1 - 2 * (me % 2)
            yield other, other
        elif kind == 'use':
            yield 2 * (me % 16) + me // 16, 16 * (me % 2) + me // 2
        else:
            yield 16 * (me % 2) + me // 2, 2 * (me % 16) + me // 16


def _start_move(kind, src, dst, send_sem, recv_sem, to, me):
    copy = _remote(src, dst, send_sem, recv_sem, to)
    if kind == 'pair':
        copy.start()
    else:
        pl.when(to != me)(copy.start)
        pl.when(to == me)(pltpu.make_async_copy(src, dst, recv_sem).start)
    return copy


def _end_move(kind, copy, dst, recv_sem, to, me):
    _landed(dst, recv_sem)
    if kind == 'pair':
        copy.wait_send()
    else:
        pl.when(to != me)(copy.wait_send)


def _all_rows_kernel(n_dev, moves, *refs):
    n = len(moves)
    in_ref, src, out_ref, dst = refs[0], refs[1:1 + n], refs[1 + n], refs[2 + n:2 + 2 * n]
    send_sem, recv_sem, m_send, m_recv = refs[2 + 2 * n:]
    me = lax.axis_index(AXIS_NAME)
    peers = [(me + d) % n_dev for d in range(1, n_dev)]
    _meet(peers)
    copies = [_remote(in_ref, out_ref.at[me], send_sem.at[i], recv_sem.at[i], peer) for i, peer in enumerate(peers)]
    for copy in copies:
        copy.start()
    ends = [to for to, _ in _passes(moves, me)]
    moving = [_start_move(moves[i], src[i], dst[i], m_send.at[i], m_recv.at[i], to, me) for i, to in enumerate(ends)]
    out_ref[me] = in_ref[...]
    for copy in copies:
        copy.wait()
    for i, copy in enumerate(moving):
        _end_move(moves[i], copy, dst[i], m_recv.at[i], ends[i], me)


def all_rows(block, n_dev, moved, moves, collective_id):
    n = len(moves)
    dma = pltpu.SemaphoreType.DMA
    vmem, hbm = pl.BlockSpec(memory_space=pltpu.VMEM), pl.BlockSpec(memory_space=pl.ANY)
    res = pl.pallas_call(
        functools.partial(_all_rows_kernel, n_dev, moves),
        out_shape=[jax.ShapeDtypeStruct((n_dev,) + block.shape, block.dtype)] + [jax.ShapeDtypeStruct(v.shape, v.dtype) for v in moved],
        in_specs=[vmem] + [hbm] * n,
        out_specs=[vmem] + [hbm] * n,
        scratch_shapes=[dma((n_dev - 1,)), dma((n_dev - 1,)), dma((n,)), dma((n,))],
        compiler_params=pltpu.CompilerParams(collective_id=collective_id, has_side_effects=True),
        cost_estimate=pl.CostEstimate(flops=10_000_000, bytes_accessed=1 << 20, transcendentals=0),
        name='all_rows',
    )(block, *moved)
    return res[0], res[1:]


def _gather_kernel(cuts, orders, seq, moves, *refs):
    n = len(moves)
    in_ref, src, out_ref, dst = refs[0], refs[1:1 + n], refs[1 + n], refs[2 + n:2 + 2 * n]
    own_sem, send_sem, recv_sem, p_send, p_recv, m_send, m_recv = refs[2 + 2 * n:]
    me = lax.axis_index(AXIS_NAME)
    at = _Place(me)
    ends = list(_passes(moves, me))
    starts = [sum(cuts[:i]) for i in range(len(cuts))]

    def part(slot, piece):
        return out_ref.at[slot] if len(cuts) == 1 else out_ref.at[slot, pl.ds(starts[piece], cuts[piece])]

    def run(u):
        sides = ['a', 'b', 'z+'] + (['z-'] if u else [])
        far = [end for kind, end in zip(moves, ends) if kind != 'pair']
        _meet([at.side(s) for s in sides] + [at.partner], me, far[0] if far else ())
        started, moving = [], []

        def send(src_ref, slot, piece, s_sem, r_sem, dev):
            copy = _remote(src_ref, part(slot, piece), s_sem, r_sem, dev)
            copy.start()
            started.append(copy)

        own = pltpu.make_async_copy(in_ref, out_ref.at[me], own_sem)
        own.start()
        count, handed = 0, [0] * len(cuts)
        for key in [(0, 0, u, i) for i in range(len(cuts))] + [_unpack(c) for c in seq[u]]:
            piece = key[3]
            kc = at.chip(key)
            slot = 2 * kc + at.core
            if _via(u, key, orders) is None:
                ref = in_ref if len(cuts) == 1 else in_ref.at[pl.ds(starts[piece], cuts[piece])]
            else:
                ref = part(slot, piece)
                _landed(ref, recv_sem.at[piece, kc])
            for side in _onward(u, key, orders):
                send(ref, slot, piece, send_sem.at[count], recv_sem.at[piece, kc], at.side(side))
                count += 1
            send(ref, slot, piece, p_send.at[piece, handed[piece]], p_recv.at[piece, kc], at.partner)
            handed[piece] += 1
            if key[:3] == (0, 0, u) and piece == len(cuts) - 1:
                for i, (to, _) in enumerate(ends):
                    moving.append(_start_move(moves[i], src[i], dst[i], m_send.at[i], m_recv.at[i], to, me))
        for piece in range(len(cuts)):
            for kc in range(16):
                _landed(part(2 * kc + 1 - at.core, piece), p_recv.at[piece, kc])
        for i, (to, _) in enumerate(ends):
            _end_move(moves[i], moving[i], dst[i], m_recv.at[i], to, me)
        own.wait()
        for copy in started:
            copy.wait_send()

    for u in (0, 1):
        pl.when(at.u == u)(functools.partial(run, u))


def gather_all(block, cuts, orders, seq, moved, moves, n_dev, collective_id):
    n, m = len(moves), len(cuts)
    dma = pltpu.SemaphoreType.DMA
    vmem, hbm = pl.BlockSpec(memory_space=pltpu.VMEM), pl.BlockSpec(memory_space=pl.ANY)
    nbytes = block.size * block.dtype.itemsize
    res = pl.pallas_call(
        functools.partial(_gather_kernel, cuts, orders, seq, moves),
        out_shape=[jax.ShapeDtypeStruct((n_dev,) + block.shape, block.dtype)] + [jax.ShapeDtypeStruct(v.shape, v.dtype) for v in moved],
        in_specs=[vmem] + [hbm] * n,
        out_specs=[hbm] * (1 + n),
        scratch_shapes=[dma, dma((24 * m,)), dma((m, 16)), dma((m, 16)), dma((m, 16)), dma((max(n, 1),)), dma((max(n, 1),))],
        compiler_params=pltpu.CompilerParams(collective_id=collective_id, has_side_effects=True, vmem_limit_bytes=nbytes + (8 << 20)),
        cost_estimate=pl.CostEstimate(flops=200_000_000, bytes_accessed=nbytes * 64, transcendentals=0),
        name='gather_all',
    )(block, *moved)
    return res[0], res[1:]


def _slots(pieces, orders, seq):
    table, most = {}, [1] * len(pieces)
    for u in (0, 1):
        used = [0] * len(pieces)
        for key in [_unpack(c) for c in reversed(seq[u])] + [(0, 0, u, i) for i in range(len(pieces))]:
            for side in _onward(u, key, orders):
                table[u, key, side] = used[key[3]]
                used[key[3]] += 1
        most = [max(a, b) for a, b in zip(most, used)]
    return table, most


def _scatter_kernel(pieces, orders, seq, n_arr, *refs):
    table, _ = _slots(pieces, orders, seq)
    n = len(pieces)
    n_pair = sum(1 for p in pieces if p[3] != 'chip')
    ins, outs = refs[:n_arr], refs[n_arr:2 * n_arr]
    k = 2 * n_arr
    land, stage, pair = refs[k:k + n], refs[k + n:k + 2 * n], list(refs[k + 2 * n:k + 2 * n + n_pair])
    load_sem, send_sem, recv_sem, d_send, d_recv = refs[k + 2 * n + n_pair:]
    got = [pair.pop(0) if p[3] != 'chip' else None for p in pieces]
    me = lax.axis_index(AXIS_NAME)
    at, partner_at = _Place(me), _Place(me, swapped=True)

    def rows_of(ref, piece):
        _, r0, rows, _ = pieces[piece]
        return ref if rows == ref.shape[0] else ref.at[pl.ds(r0, rows)]

    def term(piece, kc, core):
        arr, _, rows, kind = pieces[piece]
        if kind == 'rows':
            return ins[arr].at[kc, pl.ds(pl.multiple_of(24 * core, 8), rows)]
        return rows_of(ins[arr].at[2 * kc + core if kind == 'device' else kc], piece)

    def run(u):
        sides = ['a', 'b', 'z+'] + (['z-'] if u else [])
        _meet([at.side(s) for s in sides] + [at.partner])
        keys = [_unpack(c) for c in reversed(seq[u])] + [(0, 0, u, i) for i in range(n)]
        started = []
        given = [0] * n
        for key in keys:
            piece = key[3]
            if pieces[piece][3] != 'chip':
                kc = partner_at.chip(key)
                copy = _remote(term(piece, kc, 1 - at.core), got[piece].at[kc], d_send.at[piece, given[piece]], d_recv.at[piece, kc], at.partner)
                given[piece] += 1
                copy.start()
                started.append(copy)
        adds = [[key for key in keys if key[3] == i and (pieces[i][3] != 'chip' or _onward(u, key, orders))] for i in range(n)]

        def load(piece, j):
            return pltpu.make_async_copy(term(piece, at.chip(adds[piece][j]), at.core), stage[piece].at[j % 2], load_sem.at[piece, j % 2])

        for i in range(n):
            for j in range(2):
                load(i, j).start()
        done = [0] * n
        count = 0
        for key in keys:
            piece = key[3]
            arr, r0, rows, kind = pieces[piece]
            paired = kind != 'chip'
            kc = at.chip(key)
            children = _onward(u, key, orders)
            if not children and not paired:
                src = term(piece, kc, at.core)
            else:
                j = done[piece]
                done[piece] += 1
                parts = []
                if paired:
                    _landed(got[piece].at[kc], d_recv.at[piece, kc])
                    parts.append(got[piece].at[kc])
                for side in children:
                    slot = table[u, key, side]
                    _landed(land[piece].at[slot], recv_sem.at[piece, slot])
                    parts.append(land[piece].at[slot])
                load(piece, j).wait()
                parts.append(stage[piece].at[j % 2])
                root = key[:3] == (0, 0, u)
                src = rows_of(outs[arr], piece) if root else parts[0]
                dtype = ins[arr].dtype
                step = 8 if dtype == F32 else 16

                def body(r, _, parts=parts, dst=src, step=step, dtype=dtype):
                    some = pl.ds(pl.multiple_of(r * step, step), step)
                    total = parts[0][some, :].astype(F32)
                    for ref in parts[1:]:
                        total = total + ref[some, :].astype(F32)
                    dst[some, :] = total.astype(dtype)
                    return 0

                lax.fori_loop(0, rows // step, body, 0)
                if j + 2 < len(adds[piece]):
                    load(piece, j + 2).start()
                if root:
                    continue
            side = _via(u, key, orders)
            slot = table[_seen_by_parent(u, key, orders)]
            copy = _remote(src, land[piece].at[slot], send_sem.at[count], recv_sem.at[piece, slot], at.side(side))
            copy.start()
            started.append(copy)
            count += 1
        for copy in started:
            copy.wait_send()

    for u in (0, 1):
        pl.when(at.u == u)(functools.partial(run, u))


def scatter_sum(arrays, pieces, orders, seq, collective_id):
    n_arr, n = len(arrays), len(pieces)
    dma, hbm, vmem = pltpu.SemaphoreType.DMA, pl.BlockSpec(memory_space=pl.ANY), pl.BlockSpec(memory_space=pltpu.VMEM)
    _, most = _slots(pieces, orders, seq)
    shapes = [(rows, arrays[arr].shape[2], arrays[arr].dtype) for arr, _, rows, _ in pieces]
    scratch = [pltpu.VMEM((m, r, c), d) for m, (r, c, d) in zip(most, shapes)]
    scratch += [pltpu.VMEM((2, r, c), d) for r, c, d in shapes]
    scratch += [pltpu.VMEM((16, r, c), d) for (r, c, d), p in zip(shapes, pieces) if p[3] != 'chip']
    outs = [jax.ShapeDtypeStruct((sum(p[2] for p in pieces if p[0] == i), v.shape[2]), v.dtype) for i, v in enumerate(arrays)]
    nbytes = sum(v.size * v.dtype.itemsize for v in outs) + sum(
        (m + 2 + 16 * int(p[3] != 'chip')) * (-(-r // 16) * 16) * c * d.itemsize for m, (r, c, d), p in zip(most, shapes, pieces))
    scratch += [dma((n, 2)), dma((16 * n,)), dma((n, max(most))), dma((n, 16)), dma((n, 16))]
    return pl.pallas_call(
        functools.partial(_scatter_kernel, tuple(pieces), orders, seq, n_arr),
        out_shape=outs,
        in_specs=[hbm] * n_arr,
        out_specs=[vmem] * n_arr,
        scratch_shapes=scratch,
        compiler_params=pltpu.CompilerParams(collective_id=collective_id, has_side_effects=True, vmem_limit_bytes=nbytes + (6 << 20)),
        cost_estimate=pl.CostEstimate(flops=200_000_000, bytes_accessed=nbytes * 4, transcendentals=0),
        name='scatter_sum',
    )(*arrays)


def _lookup_kernel(counts, codes, table_ref, out_ref, rows, block, sem):
    b = pl.program_id(0)
    n_col = out_ref.shape[2] // 128
    n_rows = rows.shape[0] // n_col

    @pl.when(b == 0)
    def _():
        def widen(i, _):
            for j in range(n_col):
                part = table_ref[pl.ds(pl.multiple_of(i * 16, 16), 16), j * 128:(j + 1) * 128].astype(F32)
                line = pl.multiple_of(i * 16 * n_col, 8)
                rows[pl.ds(line + j * 8, 8), :] = part[:8]
                rows[pl.ds(line + (n_col + j) * 8, 8), :] = part[8:]
            return 0
        lax.fori_loop(0, n_rows // 16, widen, 0)

    seq = out_ref.shape[1]

    def clear(i, _):
        block[pl.ds(pl.multiple_of(i * 8 * n_col, 8), 8 * n_col), :] = jnp.zeros((8 * n_col, 128), F32)
        return 0
    lax.fori_loop(0, seq // 8, clear, 0)

    def pick(i, _):
        for t in range(4):
            code = codes[b * seq + i * 4 + t]
            row, pos = code & 8191, code >> 13
            block[pl.ds((pos >> 3) * (8 * n_col) + (pos & 7), n_col, stride=8), :] = rows[pl.ds((row >> 3) * (8 * n_col) + (row & 7), n_col, stride=8), :]
        return 0
    lax.fori_loop(0, (counts[b] + 3) // 4, pick, 0)

    def narrow(i, _):
        line = pl.multiple_of(i * 16 * n_col, 8)
        for j in range(n_col):
            part = jnp.concatenate([block[pl.ds(line + j * 8, 8), :], block[pl.ds(line + (n_col + j) * 8, 8), :]], axis=0)
            out_ref[0, pl.ds(pl.multiple_of(i * 16, 16), 16), j * 128:(j + 1) * 128] = part.astype(BF16)
        return 0
    lax.fori_loop(0, seq // 16, narrow, 0)


def lookup(table, counts, codes, seq):
    n_rows, dim = table.shape
    n_src = counts.shape[0]
    lines = dim // 128
    return pl.pallas_call(
        _lookup_kernel,
        grid_spec=pltpu.PrefetchScalarGridSpec(
            num_scalar_prefetch=2,
            grid=(n_src,),
            in_specs=[pl.BlockSpec(memory_space=pltpu.VMEM)],
            out_specs=pl.BlockSpec((1, seq, dim), lambda b, *_: (b, 0, 0)),
            scratch_shapes=[pltpu.VMEM((n_rows * lines, 128), F32), pltpu.VMEM(((seq + 8) * lines, 128), F32), pltpu.SemaphoreType.DMA],
        ),
        out_shape=jax.ShapeDtypeStruct((n_src, seq, dim), table.dtype),
        compiler_params=pltpu.CompilerParams(vmem_limit_bytes=40 << 20, dimension_semantics=('arbitrary',)),
        cost_estimate=pl.CostEstimate(flops=50_000_000, bytes_accessed=40 << 20, transcendentals=0),
        name='lookup',
    )(counts, codes, table)


def _add_rows_kernel(counts, codes, dx_ref, out_ref):
    b = pl.program_id(0)
    n_col = 7

    @pl.when(b == 0)
    def _():
        def clear(i, _):
            out_ref[pl.ds(pl.multiple_of(i * 8 * n_col, 8), 8 * n_col), :] = jnp.zeros((8 * n_col, 128), F32)
            return 0
        lax.fori_loop(0, out_ref.shape[0] // (8 * n_col), clear, 0)

    seq = codes.shape[0] // counts.shape[0]

    def add(i, _):
        for t in range(4):
            code = codes[b * seq + i * 4 + t]
            row, pos = code & 8191, code >> 13
            src = dx_ref[0, pl.ds((pos >> 3) * (8 * n_col) + (pos & 7), n_col, stride=8), :]
            at = pl.ds((row >> 3) * (8 * n_col) + (row & 7), n_col, stride=8)
            out_ref[at, :] = out_ref[at, :] + src
        return 0
    lax.fori_loop(0, counts[b] // 4, add, 0)

    def add_one(i, _):
        code = codes[b * seq + i]
        row, pos = code & 8191, code >> 13
        src = dx_ref[0, pl.ds((pos >> 3) * (8 * n_col) + (pos & 7), n_col, stride=8), :]
        at = pl.ds((row >> 3) * (8 * n_col) + (row & 7), n_col, stride=8)
        out_ref[at, :] = out_ref[at, :] + src
        return 0
    lax.fori_loop((counts[b] // 4) * 4, counts[b], add_one, 0)


def add_rows(dx, counts, codes, n_rows):
    n_src, lines, _ = dx.shape
    return pl.pallas_call(
        _add_rows_kernel,
        grid_spec=pltpu.PrefetchScalarGridSpec(
            num_scalar_prefetch=2,
            grid=(n_src,),
            in_specs=[pl.BlockSpec((1, lines, 128), lambda b, *_: (b, 0, 0))],
            out_specs=pl.BlockSpec((n_rows * 7, 128), lambda b, *_: (0, 0)),
        ),
        out_shape=jax.ShapeDtypeStruct((n_rows * 7, 128), F32),
        compiler_params=pltpu.CompilerParams(vmem_limit_bytes=48 << 20, dimension_semantics=('arbitrary',)),
        cost_estimate=pl.CostEstimate(flops=50_000_000, bytes_accessed=80 << 20, transcendentals=0),
        name='add_rows',
    )(counts, codes, dx)


def to_lines(v):
    rows, dim = v.shape
    return v.reshape(rows // 8, 8, dim // 128, 128).transpose(0, 2, 1, 3).reshape(rows * dim // 128, 128)


def from_lines(v, dim):
    rows = v.shape[0] * 128 // dim
    return v.reshape(rows // 8, dim // 128, 8, 128).transpose(0, 2, 1, 3).reshape(rows, dim)


ROWS_SEQ = (
    (8, 32, 64, 9, 33, 65, 10, 34, 66, 16, 40, 72, 96, 17, 41, 48, 18, 42, 74, 73, 97, 49, 98, 24, 80, 104, 25, 56, 57, 81, 105, 26, 50, 82, 112, 113, 58, 90, 88, 89, 122, 120, 106, 121, 114),
    (0, 16, 40, 72, 1, 17, 41, 73, 2, 18, 42, 74, 24, 34, 66, 32, 48, 64, 80, 25, 104, 26, 50, 82, 33, 49, 58, 90, 56, 65, 81, 105, 98, 122, 57, 106, 114, 88, 96, 112, 89, 97, 113, 120, 121),
)
ATTN_SEQ = (
    (8, 32, 64, 16, 40, 72, 96, 24, 48, 80, 104, 56, 88, 112, 120),
    (0, 16, 40, 72, 24, 32, 48, 64, 80, 104, 56, 88, 96, 112, 120),
)
LOOKUP_SEQ = (
    (8, 32, 64, 9, 33, 65, 10, 34, 66, 16, 40, 72, 96, 17, 41, 48, 18, 42, 74, 73, 97, 49, 98, 24, 80, 104, 25, 56, 26, 50, 82, 81, 105, 57, 112, 58, 90, 113, 88, 106, 89, 122, 120, 114, 121),
    (0, 16, 40, 72, 1, 17, 41, 73, 2, 18, 42, 74, 24, 34, 66, 32, 48, 64, 80, 104, 25, 26, 50, 82, 33, 49, 58, 90, 65, 81, 56, 105, 98, 57, 106, 122, 88, 96, 114, 112, 89, 97, 113, 120, 121),
)
GRAD_SEQ = (
    (8, 32, 64, 9, 33, 65, 10, 34, 66, 11, 35, 67, 12, 36, 68, 41, 16, 40, 72, 96, 42, 73, 97, 17, 18, 74, 98, 49, 19, 43, 75, 99, 100, 20, 44, 76, 50, 105, 80, 104, 24, 48, 106, 81, 82, 25, 113, 26, 114, 57, 27, 51, 83, 28, 52, 84, 58, 88, 112, 89, 56, 90, 59, 91, 121, 60, 92, 107, 122, 123, 108, 120, 124, 115, 116),
    (0, 16, 40, 72, 1, 17, 41, 73, 2, 18, 42, 74, 3, 19, 43, 75, 4, 20, 44, 76, 32, 35, 67, 24, 33, 48, 49, 36, 68, 64, 80, 104, 25, 34, 50, 26, 27, 51, 83, 57, 105, 65, 81, 28, 52, 84, 99, 100, 58, 56, 59, 91, 106, 66, 82, 60, 92, 107, 123, 108, 124, 115, 116, 96, 88, 113, 112, 97, 89, 98, 114, 90, 121, 122, 120),
)


def solution(mesh):
    n_dev = mesh.shape[AXIS_NAME]
    n_chip = n_dev // 2
    pair = [(i, i ^ 1) for i in range(n_dev)]
    groups = [[2 * k + c for k in range(n_chip)] for c in range(2)]

    row_spec = P(AXIS_NAME, None)
    vec_spec = P(AXIS_NAME)
    full_spec = P(None)
    batch_spec = P(AXIS_NAME, None, None)
    weight_specs = (vec_spec, row_spec, row_spec, row_spec, full_spec, full_spec, row_spec, vec_spec, row_spec, row_spec, row_spec)

    def swap(v):
        return lax.ppermute(v, AXIS_NAME, pair)

    def gather_group(v):
        return lax.all_gather(v, AXIS_NAME, axis_index_groups=groups, tiled=True)

    def device_step(tokens, positions, table_shard, attn_norm, w_query, w_key, w_value, q_norm, k_norm, w_out, mlp_norm, w_gate, w_up, w_down, dy_out):
        me = lax.axis_index(AXIS_NAME)
        core = lax.rem(me, 2)
        seq_len = tokens.shape[1]
        rows_local, model_dim = table_shard.shape
        rows_w, ff = w_gate.shape
        half = ff // 2
        nq, nk = w_query.shape[1], w_key.shape[1]
        head_dim = q_norm.shape[0]
        kv_heads = nk // head_dim
        q_per_kv = nq // nk

        mine_gu = jnp.concatenate([lax.dynamic_slice(w_gate, (0, core * half), (rows_w, half)), lax.dynamic_slice(w_up, (0, core * half), (rows_w, half))], axis=1)
        other_gu = jnp.concatenate([lax.dynamic_slice(w_gate, (0, (1 - core) * half), (rows_w, half)), lax.dynamic_slice(w_up, (0, (1 - core) * half), (rows_w, half))], axis=1)
        token_rows = jnp.pad(tokens.reshape(-1, 128), ((0, 4), (0, 0)))
        dy = dy_out.reshape(seq_len, model_dim)
        all_tokens, (down_block, recv_gu, dy_other) = all_rows(token_rows, n_dev, [w_down, other_gu, dy], ('use', 'pair', 'pair'), 0)
        block_gu = jnp.where(core == 0, jnp.concatenate([mine_gu, recv_gu], axis=0), jnp.concatenate([recv_gu, mine_gu], axis=0))
        wgu = gather_group(block_gu)
        wd = gather_group(down_block)
        w_g, w_u = wgu[:, :half], wgu[:, half:]

        gains = jnp.pad(jnp.stack([attn_norm, mlp_norm], axis=1), ((0, 0), (0, 126)))
        attn_pack = jnp.concatenate([w_query, w_key, w_value, w_out, gains], axis=1)
        attn_full = gather_all(attn_pack, (rows_w,), ('zba',), ATTN_SEQ, [], (), n_dev, 1)[0].reshape(-1, attn_pack.shape[1])

        all_ids = all_tokens[:, :seq_len // 128].reshape(-1)
        local_ids = all_ids - me * rows_local
        is_owner = (local_ids >= 0) & (local_ids < rows_local)
        own = is_owner.reshape(n_dev, seq_len)
        slot = jnp.arange(seq_len, dtype=jnp.int32)
        upto = (slot[:, None] <= slot[None, :]).astype(BF16)
        rank = jnp.where(own, dot(own.astype(BF16), upto, 1, 0).astype(jnp.int32) - 1, -1)
        counts = jnp.sum(own.astype(jnp.int32), axis=1)
        code = slot[None] * 8192 + jnp.where(own, local_ids.reshape(n_dev, seq_len), 0)
        codes = jnp.sum(jnp.where(rank[:, :, None] == slot, code[:, :, None], 0), axis=1)
        codes = jnp.where(slot[None] < counts[:, None], codes, seq_len * 8192).reshape(-1)
        picked = lookup(table_shard, counts, codes, seq_len)
        x_emb = scatter_sum([picked], [(0, 0, 192, 'device'), (0, 192, 208, 'device'), (0, 400, 112, 'device')], ('zba', 'zba', 'baz'), LOOKUP_SEQ, 2)[0]

        dy2 = jnp.concatenate([dy, dy_other], axis=0)

        n_in = nq + 2 * nk
        w_in = attn_full[:, :n_in]
        wo = attn_full[:, n_in:n_in + nq]
        g_attn = attn_full[:, n_in + nq]
        g_mlp = attn_full[:, n_in + nq + 1]

        cos_t, sin_t = rope_tables(positions, head_dim)
        cos_q, sin_q = cos_t[:, :, None, None, :], sin_t[:, :, None, None, :]
        cos_k, sin_k = cos_t[:, :, None, :], sin_t[:, :, None, :]
        normed1, norm1_inv = norm_fwd(x_emb)
        attn_in = (normed1 * g_attn.astype(F32)).astype(BF16)
        qkv = dot(attn_in, w_in, 1, 0).astype(BF16)
        q_raw = qkv[:, :nq].reshape(1, seq_len, kv_heads, q_per_kv, head_dim)
        k_raw = qkv[:, nq:nq + nk].reshape(1, seq_len, kv_heads, head_dim)
        v_raw = qkv[:, nq + nk:].reshape(1, seq_len, kv_heads, head_dim)
        q_normed, q_inv = norm_fwd(q_raw)
        k_normed, k_inv = norm_fwd(k_raw)
        q_rot = rotate(q_normed * q_norm.astype(F32), cos_q, sin_q).astype(BF16)
        k_rot = rotate(k_normed * k_norm.astype(F32), cos_k, sin_k).astype(BF16)
        attn_heads, attn_probs = attn_fwd(q_rot, k_rot, v_raw)
        attn_flat = attn_heads.reshape(seq_len, nq)
        hidden = (x_emb.astype(F32) + dot(attn_flat, wo, 1, 0)).astype(BF16)
        normed2, norm2_inv = norm_fwd(hidden)
        mlp_in = (normed2 * g_mlp.astype(F32)).astype(BF16)

        mlp2 = jnp.concatenate([mlp_in, swap(mlp_in)], axis=0)
        gate_pre = dot(mlp2, w_g, 1, 0)
        up_proj = dot(mlp2, w_u, 1, 0)
        gate_sig = jax.nn.sigmoid(gate_pre)
        mlp_act = (gate_pre * gate_sig * up_proj).astype(BF16)
        grad_w_down = dot(mlp_act, dy2, 0, 0)
        grad_act = dot(dy2, wd, 1, 1)
        grad_gate = (grad_act * up_proj * gate_sig * (1.0 + gate_pre * (1.0 - gate_sig))).astype(BF16)
        grad_up = (grad_act * gate_pre * gate_sig).astype(BF16)
        part_in = dot(grad_gate, w_g, 1, 1) + dot(grad_up, w_u, 1, 1)
        grad_mlp_in = part_in[:seq_len] + swap(part_in[seq_len:])
        grad_w_gate = dot(mlp2, grad_gate, 0, 0)
        grad_w_up = dot(mlp2, grad_up, 0, 0)
        part_y = dot(mlp_act, wd, 1, 0)
        layer_out = (hidden.astype(F32) + (part_y[:seq_len] + swap(part_y[seq_len:]))).astype(BF16)

        grad_mlp_norm = jnp.sum(grad_mlp_in * normed2, axis=0)
        grad_hidden = dy.astype(F32) + norm_bwd(grad_mlp_in, normed2, norm2_inv, g_mlp)
        hidden_b = grad_hidden.astype(BF16)
        grad_w_out = dot(attn_flat, hidden_b, 0, 0)
        grad_heads = dot(hidden_b, wo, 1, 1).reshape(q_rot.shape)
        grad_q, grad_k, grad_v = attn_bwd(grad_heads, q_rot, k_rot, v_raw, attn_probs)
        grad_qt = rotate(grad_q, cos_q, -sin_q)
        grad_kt = rotate(grad_k, cos_k, -sin_k)
        grad_q_norm = jnp.sum(grad_qt * q_normed, axis=(0, 1, 2, 3))
        grad_k_norm = jnp.sum(grad_kt * k_normed, axis=(0, 1, 2))
        grad_q_raw = norm_bwd(grad_qt, q_normed, q_inv, q_norm).astype(BF16).reshape(seq_len, nq)
        grad_k_raw = norm_bwd(grad_kt, k_normed, k_inv, k_norm).astype(BF16).reshape(seq_len, nk)
        grad_v_raw = grad_v.astype(BF16).reshape(seq_len, nk)
        grad_qkv = jnp.concatenate([grad_q_raw, grad_k_raw, grad_v_raw], axis=1)
        grad_attn_in = dot(grad_qkv, w_in, 1, 1)
        grad_attn_norm = jnp.sum(grad_attn_in * normed1, axis=0)
        grad_x_emb = grad_hidden + norm_bwd(grad_attn_in, normed1, norm1_inv, g_attn)

        by_chip = [u.reshape(n_chip, -1, u.shape[1]) for u in (grad_w_down, grad_w_gate, grad_w_up, dot(attn_in, grad_qkv, 0, 0), grad_w_out)]
        down_rows, gate_shard, up_shard, in_shard, out_shard = scatter_sum(
            by_chip, [(i, 0, u.shape[1], 'chip') for i, u in enumerate(by_chip[:3])] + [(3, 0, 32, 'rows'), (4, 0, 32, 'rows')], ('bza', 'zba', 'zba', 'baz', 'baz'), GRAD_SEQ, 3)

        chip_rows = jnp.concatenate([gate_shard, up_shard], axis=1)
        mine = lax.dynamic_slice(chip_rows, (core * rows_w, 0), (rows_w, chip_rows.shape[1]))
        give = lax.dynamic_slice(chip_rows, ((1 - core) * rows_w, 0), (rows_w, chip_rows.shape[1]))
        qk = jnp.pad(jnp.concatenate([grad_q_norm, grad_k_norm])[None], ((0, 0), (0, model_dim - 2 * head_dim)))
        gains_grad = jnp.concatenate([qk, grad_attn_norm[None], grad_mlp_norm[None], jnp.zeros((5, model_dim), F32)], axis=0)
        lines = model_dim // 128
        all_dx, (down_shard, recv) = gather_all(
            to_lines(jnp.concatenate([grad_x_emb, gains_grad], axis=0)), (200 * lines, 200 * lines, 120 * lines), ('zba', 'zba', 'baz'), ROWS_SEQ, [down_rows, give], ('store', 'pair'), n_dev, 4)
        d_table = from_lines(add_rows(all_dx, counts, codes, rows_local), model_dim)
        gains_grad = from_lines(jnp.sum(all_dx[:, seq_len * lines:], axis=0), model_dim)
        qk = gains_grad[0]
        d_attn_norm, d_mlp_norm = (lax.dynamic_slice(gains_grad[i], (me * rows_w,), (rows_w,)) for i in (1, 2))
        low = jnp.where(core == 0, mine, recv)
        high = jnp.where(core == 0, recv, mine)
        d_gate = jnp.concatenate([low[:, :half], high[:, :half]], axis=1)
        d_up = jnp.concatenate([low[:, half:ff], high[:, half:ff]], axis=1)
        in_rows = lax.dynamic_slice(in_shard, (core * (rows_w - 24), 0), (rows_w, n_in))
        d_query, d_key, d_value = in_rows[:, :nq], in_rows[:, nq:nq + nk], in_rows[:, nq + nk:]
        d_out = lax.dynamic_slice(out_shard, (core * (rows_w - 24), 0), (rows_w, nq))
        return (layer_out.reshape(1, seq_len, model_dim), d_table, d_attn_norm, d_query, d_key, d_value, qk[:head_dim], qk[head_dim:2 * head_dim], d_out, d_mlp_norm, d_gate, d_up, down_shard)

    return jax.shard_map(device_step, mesh=mesh, in_specs=(row_spec, row_spec, row_spec) + weight_specs + (batch_spec,), out_specs=(batch_spec, row_spec) + weight_specs, check_vma=False)
```

```python
import functools
import math
import jax
import jax.numpy as jnp
from jax import lax
from jax.experimental import pallas as pl
from jax.experimental.pallas import tpu as pltpu
from jax.sharding import PartitionSpec as P

NORM_EPS = 1e-6
ROPE_THETA = 1.0e6
AXIS_NAME = 'fsdp'
F32 = jnp.float32
BF16 = jnp.bfloat16
MESH = pl.DeviceIdType.MESH


def dot(a, b, ca, cb):
    return lax.dot_general(a, b, (((ca,), (cb,)), ((), ())), preferred_element_type=F32)


def _unpack(code):
    return code // 64, code // 32 % 2, code // 8 % 4, code % 8


def _via(u, key, orders):
    da, db, p, piece = key
    last = None
    for axis in orders[piece]:
        if axis == 'a' and da or axis == 'b' and db:
            last = axis
        if axis == 'z' and p != u:
            last = 'z+' if p > u else 'z-'
    return last


def _onward(u, key, orders):
    order = orders[key[3]]
    via = _via(u, key, orders)
    left = order if via is None else order[order.index(via[0]) + 1:]
    out = []
    if u < 3 and (via == 'z-' or 'z' in left):
        out.append('z+')
    if u > 0 and (via == 'z+' or 'z' in left):
        out.append('z-')
    return out + [axis for axis in 'ba' if axis in left]


def _seen_by_parent(u, key, orders):
    da, db, p, piece = key
    via = _via(u, key, orders)
    if via == 'a':
        return u, (0, db, p, piece), 'a'
    if via == 'b':
        return u, (da, 0, p, piece), 'b'
    if via == 'z-':
        return u - 1, key, 'z+'
    if u == 0:
        return 1, key, 'z-'
    return 1, (da, db, 3 - p, piece), 'z+'


class _Place:
    def __init__(self, me, swapped=False):
        self.me = me
        self.core = me % 2
        x, y, self.z = (me // 2) % 2, (me // 4) % 2, me // 8
        other = 1 - self.core if swapped else self.core
        self.a = y * (1 - other) + x * other
        self.b = x * (1 - other) + y * other
        self.a_str, self.b_str = 4 - 2 * other, 2 + 2 * other
        self.far = self.z // 2
        self.u = 3 * self.far + (1 - 2 * self.far) * self.z
        self.partner = me + 1 - 2 * self.core

    def chip(self, key):
        da, db, p = key[:3]
        a = self.a + da * (1 - 2 * self.a)
        b = self.b + db * (1 - 2 * self.b)
        z = 3 * self.far + (1 - 2 * self.far) * p
        return (8 * z + a * self.a_str + b * self.b_str) // 2

    def side(self, name):
        if name == 'a':
            return self.me + (1 - 2 * self.a) * self.a_str
        if name == 'b':
            return self.me + (1 - 2 * self.b) * self.b_str
        return self.me + 8 * (1 - 2 * self.far) * (1 if name == 'z+' else -1)


def _remote(src, dst, send_sem, recv_sem, dev):
    return pltpu.make_async_remote_copy(src_ref=src, dst_ref=dst, send_sem=send_sem, recv_sem=recv_sem, device_id=(dev,), device_id_type=MESH)


def _meet(peers, me=None, ends=()):
    sem = pltpu.get_barrier_semaphore()

    def meet(everyone):
        for peer in everyone:
            pl.semaphore_signal(sem, inc=1, device_id=(peer,), device_id_type=MESH)
        pl.semaphore_wait(sem, len(everyone))

    if not ends:
        meet(peers)
        return
    to, frm = ends
    pl.when(to != me)(lambda: meet(peers + [to, frm]))
    pl.when(to == me)(lambda: meet(peers))


def _landed(ref, sem):
    pltpu.make_async_copy(ref, ref, sem).wait()


def _passes(moves, me):
    for kind in moves:
        if kind == 'pair':
            other = me + 1 - 2 * (me % 2)
            yield other, other
        elif kind == 'use':
            yield 2 * (me % 16) + me // 16, 16 * (me % 2) + me // 2
        else:
            yield 16 * (me % 2) + me // 2, 2 * (me % 16) + me // 16


def _start_move(kind, src, dst, send_sem, recv_sem, to, me):
    copy = _remote(src, dst, send_sem, recv_sem, to)
    if kind == 'pair':
        copy.start()
    else:
        pl.when(to != me)(copy.start)
        pl.when(to == me)(pltpu.make_async_copy(src, dst, recv_sem).start)
    return copy


def _end_move(kind, copy, dst, recv_sem, to, me):
    _landed(dst, recv_sem)
    if kind == 'pair':
        copy.wait_send()
    else:
        pl.when(to != me)(copy.wait_send)


def _all_rows_kernel(n_dev, moves, *refs):
    n = len(moves)
    in_ref, src, out_ref, dst = refs[0], refs[1:1 + n], refs[1 + n], refs[2 + n:2 + 2 * n]
    send_sem, recv_sem, m_send, m_recv = refs[2 + 2 * n:]
    me = lax.axis_index(AXIS_NAME)
    peers = [(me + d) % n_dev for d in range(1, n_dev)]
    _meet(peers)
    copies = [_remote(in_ref, out_ref.at[me], send_sem.at[i], recv_sem.at[i], peer) for i, peer in enumerate(peers)]
    for copy in copies:
        copy.start()
    ends = [to for to, _ in _passes(moves, me)]
    moving = [_start_move(moves[i], src[i], dst[i], m_send.at[i], m_recv.at[i], to, me) for i, to in enumerate(ends)]
    out_ref[me] = in_ref[...]
    for copy in copies:
        copy.wait()
    for i, copy in enumerate(moving):
        _end_move(moves[i], copy, dst[i], m_recv.at[i], ends[i], me)


def all_rows(block, n_dev, moved, moves, collective_id):
    n = len(moves)
    dma = pltpu.SemaphoreType.DMA
    vmem, hbm = pl.BlockSpec(memory_space=pltpu.VMEM), pl.BlockSpec(memory_space=pl.ANY)
    res = pl.pallas_call(
        functools.partial(_all_rows_kernel, n_dev, moves),
        out_shape=[jax.ShapeDtypeStruct((n_dev,) + block.shape, block.dtype)] + [jax.ShapeDtypeStruct(v.shape, v.dtype) for v in moved],
        in_specs=[vmem] + [hbm] * n,
        out_specs=[vmem] + [hbm] * n,
        scratch_shapes=[dma((n_dev - 1,)), dma((n_dev - 1,)), dma((n,)), dma((n,))],
        compiler_params=pltpu.CompilerParams(collective_id=collective_id, has_side_effects=True),
        cost_estimate=pl.CostEstimate(flops=10_000_000, bytes_accessed=1 << 20, transcendentals=0),
        name='all_rows',
    )(block, *moved)
    return res[0], res[1:]


def _gather_kernel(pieces, orders, seq, moves, n_arr, *refs):
    n, m = len(moves), len(pieces)
    ins, src, outs, dst = refs[:n_arr], refs[n_arr:n_arr + n], refs[n_arr + n:2 * n_arr + n], refs[2 * n_arr + n:2 * n_arr + 2 * n]
    own_sem, send_sem, recv_sem, p_send, p_recv, m_send, m_recv = refs[2 * n_arr + 2 * n:]
    me = lax.axis_index(AXIS_NAME)
    at = _Place(me)
    ends = list(_passes(moves, me))

    def part(kc, core, piece):
        arr, r0, rows, shared = pieces[piece]
        slot = 2 * kc + core if shared else kc
        return outs[arr].at[slot] if rows == outs[arr].shape[1] else outs[arr].at[slot, pl.ds(r0, rows)]

    def run(u):
        sides = ['a', 'b', 'z+'] + (['z-'] if u else [])
        far = [end for kind, end in zip(moves, ends) if kind != 'pair']
        _meet([at.side(s) for s in sides] + [at.partner], me, far[0] if far else ())
        started, moving = [], []

        def send(src_ref, dst_ref, s_sem, r_sem, dev):
            copy = _remote(src_ref, dst_ref, s_sem, r_sem, dev)
            copy.start()
            started.append(copy)

        count, handed = 0, [0] * m
        for key in [(0, 0, u, i) for i in range(m)] + [_unpack(c) for c in seq[u]]:
            piece = key[3]
            arr, r0, rows, shared = pieces[piece]
            kc = at.chip(key)
            place = part(kc, at.core, piece)
            if _via(u, key, orders) is None:
                ref = ins[arr] if rows == ins[arr].shape[0] else ins[arr].at[pl.ds(r0, rows)]
            else:
                ref = place
                _landed(ref, recv_sem.at[piece, kc])
            for side in _onward(u, key, orders):
                send(ref, place, send_sem.at[count], recv_sem.at[piece, kc], at.side(side))
                count += 1
            if shared:
                send(ref, place, p_send.at[piece, handed[piece]], p_recv.at[piece, kc], at.partner)
                handed[piece] += 1
            if key == (0, 0, u, m - 1):
                for i, (to, _) in enumerate(ends):
                    moving.append(_start_move(moves[i], src[i], dst[i], m_send.at[i], m_recv.at[i], to, me))
                own = [pltpu.make_async_copy(ins[i], outs[i].at[me if pieces_shared[i] else me // 2], own_sem.at[i]) for i in range(n_arr)]
                for copy in own:
                    copy.start()
        for piece in range(m):
            if pieces[piece][3]:
                for kc in range(16):
                    _landed(part(kc, 1 - at.core, piece), p_recv.at[piece, kc])
        for i, (to, _) in enumerate(ends):
            _end_move(moves[i], moving[i], dst[i], m_recv.at[i], to, me)
        for copy in own:
            copy.wait()
        for copy in started:
            copy.wait_send()

    pieces_shared = {p[0]: p[3] for p in pieces}
    for u in (0, 1):
        pl.when(at.u == u)(functools.partial(run, u))


def gather_all(blocks, pieces, orders, seq, moved, moves, n_dev, collective_id):
    n, m, n_arr = len(moves), len(pieces), len(blocks)
    dma = pltpu.SemaphoreType.DMA
    vmem, hbm = pl.BlockSpec(memory_space=pltpu.VMEM), pl.BlockSpec(memory_space=pl.ANY)
    nbytes = sum(v.size * v.dtype.itemsize for v in blocks)
    shared = {p[0]: p[3] for p in pieces}
    res = pl.pallas_call(
        functools.partial(_gather_kernel, tuple(pieces), orders, seq, moves, n_arr),
        out_shape=[jax.ShapeDtypeStruct((n_dev if shared[i] else n_dev // 2,) + v.shape, v.dtype) for i, v in enumerate(blocks)] + [
            jax.ShapeDtypeStruct(v.shape, v.dtype) for v in moved],
        in_specs=[vmem] * n_arr + [hbm] * n,
        out_specs=[hbm] * (n_arr + n),
        scratch_shapes=[dma((n_arr,)), dma((24 * m,)), dma((m, 16)), dma((m, 16)), dma((m, 16)), dma((max(n, 1),)), dma((max(n, 1),))],
        compiler_params=pltpu.CompilerParams(collective_id=collective_id, has_side_effects=True, vmem_limit_bytes=nbytes + (8 << 20)),
        cost_estimate=pl.CostEstimate(flops=200_000_000, bytes_accessed=nbytes * 64, transcendentals=0),
        name='gather_all',
    )(*blocks, *moved)
    return res[:n_arr], res[n_arr:]


def _slots(pieces, orders, seq):
    table, most = {}, [1] * len(pieces)
    for u in (0, 1):
        used = [0] * len(pieces)
        for key in [_unpack(c) for c in reversed(seq[u])] + [(0, 0, u, i) for i in range(len(pieces))]:
            for side in _onward(u, key, orders):
                table[u, key, side] = used[key[3]]
                used[key[3]] += 1
        most = [max(a, b) for a, b in zip(most, used)]
    return table, most


def _scatter_kernel(pieces, orders, seq, n_arr, *refs):
    table, _ = _slots(pieces, orders, seq)
    n = len(pieces)
    n_pair = sum(1 for p in pieces if p[3] != 'chip')
    ins, outs = refs[:n_arr], refs[n_arr:2 * n_arr]
    k = 2 * n_arr
    land, stage, pair = refs[k:k + n], refs[k + n:k + 2 * n], list(refs[k + 2 * n:k + 2 * n + n_pair])
    load_sem, send_sem, recv_sem, d_send, d_recv = refs[k + 2 * n + n_pair:]
    got = [pair.pop(0) if p[3] != 'chip' else None for p in pieces]
    me = lax.axis_index(AXIS_NAME)
    at, partner_at = _Place(me), _Place(me, swapped=True)

    def rows_of(ref, piece):
        _, r0, rows, _ = pieces[piece]
        return ref if rows == ref.shape[0] else ref.at[pl.ds(r0, rows)]

    def term(piece, kc, core):
        arr, _, rows, kind = pieces[piece]
        if kind == 'rows':
            return ins[arr].at[kc, pl.ds(pl.multiple_of(24 * core, 8), rows)]
        return rows_of(ins[arr].at[2 * kc + core if kind == 'device' else kc], piece)

    def run(u):
        sides = ['a', 'b', 'z+'] + (['z-'] if u else [])
        _meet([at.side(s) for s in sides] + [at.partner])
        keys = [_unpack(c) for c in reversed(seq[u])] + [(0, 0, u, i) for i in range(n)]
        started = []
        given = [0] * n
        for key in keys:
            piece = key[3]
            if pieces[piece][3] != 'chip':
                kc = partner_at.chip(key)
                copy = _remote(term(piece, kc, 1 - at.core), got[piece].at[kc], d_send.at[piece, given[piece]], d_recv.at[piece, kc], at.partner)
                given[piece] += 1
                copy.start()
                started.append(copy)
        adds = [[key for key in keys if key[3] == i and (pieces[i][3] != 'chip' or _onward(u, key, orders))] for i in range(n)]

        def load(piece, j):
            return pltpu.make_async_copy(term(piece, at.chip(adds[piece][j]), at.core), stage[piece].at[j % 2], load_sem.at[piece, j % 2])

        for i in range(n):
            for j in range(2):
                load(i, j).start()
        done = [0] * n
        count = 0
        for key in keys:
            piece = key[3]
            arr, r0, rows, kind = pieces[piece]
            paired = kind != 'chip'
            kc = at.chip(key)
            children = _onward(u, key, orders)
            if not children and not paired:
                src = term(piece, kc, at.core)
            else:
                j = done[piece]
                done[piece] += 1
                parts = []
                if paired:
                    _landed(got[piece].at[kc], d_recv.at[piece, kc])
                    parts.append(got[piece].at[kc])
                for side in children:
                    slot = table[u, key, side]
                    _landed(land[piece].at[slot], recv_sem.at[piece, slot])
                    parts.append(land[piece].at[slot])
                load(piece, j).wait()
                parts.append(stage[piece].at[j % 2])
                root = key[:3] == (0, 0, u)
                src = rows_of(outs[arr], piece) if root else parts[0]
                dtype = ins[arr].dtype
                step = 8 if dtype == F32 else 16

                def body(r, _, parts=parts, dst=src, step=step, dtype=dtype):
                    some = pl.ds(pl.multiple_of(r * step, step), step)
                    total = parts[0][some, :].astype(F32)
                    for ref in parts[1:]:
                        total = total + ref[some, :].astype(F32)
                    dst[some, :] = total.astype(dtype)
                    return 0

                lax.fori_loop(0, rows // step, body, 0)
                if j + 2 < len(adds[piece]):
                    load(piece, j + 2).start()
                if root:
                    continue
            side = _via(u, key, orders)
            slot = table[_seen_by_parent(u, key, orders)]
            copy = _remote(src, land[piece].at[slot], send_sem.at[count], recv_sem.at[piece, slot], at.side(side))
            copy.start()
            started.append(copy)
            count += 1
        for copy in started:
            copy.wait_send()

    for u in (0, 1):
        pl.when(at.u == u)(functools.partial(run, u))


def scatter_sum(arrays, pieces, orders, seq, collective_id):
    n_arr, n = len(arrays), len(pieces)
    dma, hbm, vmem = pltpu.SemaphoreType.DMA, pl.BlockSpec(memory_space=pl.ANY), pl.BlockSpec(memory_space=pltpu.VMEM)
    _, most = _slots(pieces, orders, seq)
    shapes = [(rows, arrays[arr].shape[2], arrays[arr].dtype) for arr, _, rows, _ in pieces]
    scratch = [pltpu.VMEM((m, r, c), d) for m, (r, c, d) in zip(most, shapes)]
    scratch += [pltpu.VMEM((2, r, c), d) for r, c, d in shapes]
    scratch += [pltpu.VMEM((16, r, c), d) for (r, c, d), p in zip(shapes, pieces) if p[3] != 'chip']
    outs = [jax.ShapeDtypeStruct((sum(p[2] for p in pieces if p[0] == i), v.shape[2]), v.dtype) for i, v in enumerate(arrays)]
    nbytes = sum(v.size * v.dtype.itemsize for v in outs) + sum(
        (m + 2 + 16 * int(p[3] != 'chip')) * (-(-r // 16) * 16) * c * d.itemsize for m, (r, c, d), p in zip(most, shapes, pieces))
    scratch += [dma((n, 2)), dma((16 * n,)), dma((n, max(most))), dma((n, 16)), dma((n, 16))]
    return pl.pallas_call(
        functools.partial(_scatter_kernel, tuple(pieces), orders, seq, n_arr),
        out_shape=outs,
        in_specs=[hbm] * n_arr,
        out_specs=[vmem] * n_arr,
        scratch_shapes=scratch,
        compiler_params=pltpu.CompilerParams(collective_id=collective_id, has_side_effects=True, vmem_limit_bytes=nbytes + (6 << 20)),
        cost_estimate=pl.CostEstimate(flops=200_000_000, bytes_accessed=nbytes * 4, transcendentals=0),
        name='scatter_sum',
    )(*arrays)


def _lookup_kernel(counts, codes, table_ref, out_ref, rows, block, sem):
    b = pl.program_id(0)
    n_col = out_ref.shape[2] // 128
    n_rows = rows.shape[0] // n_col

    @pl.when(b == 0)
    def _():
        def widen(i, _):
            for j in range(n_col):
                part = table_ref[pl.ds(pl.multiple_of(i * 16, 16), 16), j * 128:(j + 1) * 128].astype(F32)
                line = pl.multiple_of(i * 16 * n_col, 8)
                rows[pl.ds(line + j * 8, 8), :] = part[:8]
                rows[pl.ds(line + (n_col + j) * 8, 8), :] = part[8:]
            return 0
        lax.fori_loop(0, n_rows // 16, widen, 0)

    seq = out_ref.shape[1]

    def clear(i, _):
        block[pl.ds(pl.multiple_of(i * 8 * n_col, 8), 8 * n_col), :] = jnp.zeros((8 * n_col, 128), F32)
        return 0
    lax.fori_loop(0, seq // 8, clear, 0)

    def pick(i, _):
        for t in range(8):
            code = codes[b * seq + i * 8 + t]
            block[pl.ds(code >> 16, n_col, stride=8), :] = rows[pl.ds(code & 65535, n_col, stride=8), :]
        return 0
    lax.fori_loop(0, (counts[b] + 7) // 8, pick, 0)

    def narrow(i, _):
        line = pl.multiple_of(i * 16 * n_col, 8)
        for j in range(n_col):
            part = jnp.concatenate([block[pl.ds(line + j * 8, 8), :], block[pl.ds(line + (n_col + j) * 8, 8), :]], axis=0)
            out_ref[0, pl.ds(pl.multiple_of(i * 16, 16), 16), j * 128:(j + 1) * 128] = part.astype(BF16)
        return 0
    lax.fori_loop(0, seq // 16, narrow, 0)


def lookup(table, counts, codes, seq):
    n_rows, dim = table.shape
    n_src = counts.shape[0]
    lines = dim // 128
    return pl.pallas_call(
        _lookup_kernel,
        grid_spec=pltpu.PrefetchScalarGridSpec(
            num_scalar_prefetch=2,
            grid=(n_src,),
            in_specs=[pl.BlockSpec(memory_space=pltpu.VMEM)],
            out_specs=pl.BlockSpec((1, seq, dim), lambda b, *_: (b, 0, 0)),
            scratch_shapes=[pltpu.VMEM((n_rows * lines, 128), F32), pltpu.VMEM(((seq + 8) * lines, 128), F32), pltpu.SemaphoreType.DMA],
        ),
        out_shape=jax.ShapeDtypeStruct((n_src, seq, dim), table.dtype),
        compiler_params=pltpu.CompilerParams(vmem_limit_bytes=40 << 20, dimension_semantics=('arbitrary',)),
        cost_estimate=pl.CostEstimate(flops=50_000_000, bytes_accessed=40 << 20, transcendentals=0),
        name='lookup',
    )(counts, codes, table)


def _add_rows_kernel(counts, codes, dx_ref, out_ref, buf, sem):
    n_src, lines, _ = dx_ref.shape
    n_col = 7
    seq = codes.shape[0] // n_src
    cut = lines // 5
    depth = buf.shape[0]

    def fetch(b):
        for i in range(5):
            some = pl.ds(i * cut, cut)
            pltpu.make_async_copy(dx_ref.at[b, some], buf.at[lax.rem(b, depth), some], sem.at[lax.rem(b, depth)]).start()

    for b in range(depth - 1):
        fetch(b)

    def clear(i, _):
        out_ref[pl.ds(pl.multiple_of(i * 16 * n_col, 8), 16 * n_col), :] = jnp.zeros((16 * n_col, 128), F32)
        return 0
    lax.fori_loop(0, out_ref.shape[0] // (16 * n_col), clear, 0)

    def source(b, _):
        at = lax.rem(b, depth)

        @pl.when(b + depth - 1 < n_src)
        def _():
            fetch(b + depth - 1)
        pltpu.make_async_copy(dx_ref.at[b], buf.at[at], sem.at[at]).wait()

        def add(first, i):
            code = codes[b * seq + first + i]
            line = pl.ds(code & 65535, n_col, stride=8)
            out_ref[line, :] = out_ref[line, :] + buf[at, pl.ds(code >> 16, n_col, stride=8), :]

        def add_pair(i, _):
            code0, code1 = codes[b * seq + i * 2], codes[b * seq + i * 2 + 1]
            line0, line1 = code0 & 65535, code1 & 65535
            new0 = buf[at, pl.ds(code0 >> 16, n_col, stride=8), :]
            new1 = buf[at, pl.ds(code1 >> 16, n_col, stride=8), :]
            old0 = out_ref[pl.ds(line0, n_col, stride=8), :]
            old1 = out_ref[pl.ds(line1, n_col, stride=8), :]
            sum0 = old0 + new0
            out_ref[pl.ds(line0, n_col, stride=8), :] = sum0
            out_ref[pl.ds(line1, n_col, stride=8), :] = jnp.where(line0 == line1, sum0, old1) + new1
            return 0

        def add_four(i, _):
            add_pair(2 * i, 0)
            add_pair(2 * i + 1, 0)
            return 0
        n = counts[b]
        lax.fori_loop(0, n // 4, add_four, 0)

        def add_one(i, _):
            add(0, i)
            return 0
        lax.fori_loop((n // 4) * 4, n, add_one, 0)
        return 0
    lax.fori_loop(0, n_src, source, 0)


def add_rows(dx, counts, codes, n_rows):
    n_src, lines, _ = dx.shape
    return pl.pallas_call(
        _add_rows_kernel,
        grid_spec=pltpu.PrefetchScalarGridSpec(
            num_scalar_prefetch=2,
            grid=(),
            in_specs=[pl.BlockSpec(memory_space=pl.ANY)],
            out_specs=pl.BlockSpec(memory_space=pltpu.VMEM),
            scratch_shapes=[pltpu.VMEM((4, lines, 128), F32), pltpu.SemaphoreType.DMA((4,))],
        ),
        out_shape=jax.ShapeDtypeStruct((n_rows * 7, 128), F32),
        compiler_params=pltpu.CompilerParams(vmem_limit_bytes=48 << 20),
        cost_estimate=pl.CostEstimate(flops=50_000_000, bytes_accessed=80 << 20, transcendentals=0),
        name='add_rows',
    )(counts, codes, dx)


def to_lines(v):
    rows, dim = v.shape
    return v.reshape(rows // 8, 8, dim // 128, 128).transpose(0, 2, 1, 3).reshape(rows * dim // 128, 128)


def from_lines(v, dim):
    rows = v.shape[0] * 128 // dim
    return v.reshape(rows // 8, dim // 128, 8, 128).transpose(0, 2, 1, 3).reshape(rows, dim)


def _rms(v):
    return lax.rsqrt(jnp.mean(v * v, axis=-1, keepdims=True) + NORM_EPS)


def _head_mean(v, low):
    first = jnp.sum(jnp.where(low, v, 0.0), axis=-1, keepdims=True)
    second = jnp.sum(jnp.where(low, 0.0, v), axis=-1, keepdims=True)
    return jnp.where(low, first, second) * (1.0 / 64.0)


def _turn(v, cos_t, sin_t, lead):
    return v * cos_t + jnp.where(lead, -pltpu.roll(v, 96, 1), pltpu.roll(v, 32, 1)) * sin_t


def _spread(tile, low, ref):
    first = jnp.where(low, tile, 0.0)
    second = jnp.where(low, 0.0, tile)
    ref[0] = first.astype(BF16)
    ref[1] = pltpu.roll(first, 64, 1).astype(BF16)
    ref[2] = pltpu.roll(second, 64, 1).astype(BF16)
    ref[3] = second.astype(BF16)


def _probs(q, k, block):
    scores = dot(q, k, 1, 1) * 0.125
    n = scores.shape[1]
    row = lax.broadcasted_iota(jnp.int32, scores.shape, 0) + block
    col = lax.broadcasted_iota(jnp.int32, scores.shape, 1)
    scores = jnp.where(row >= col, scores, -1e30)
    e = jnp.exp(scores - jnp.max(scores, axis=-1, keepdims=True))
    return e * (1.0 / jnp.sum(e, axis=-1, keepdims=True))


def _lanes(rows):
    lane = lax.broadcasted_iota(jnp.int32, (rows, 128), 1)
    return lane < 64, lane % 64 < 32


def _attn_fwd_kernel(x_ref, w_ref, gain_ref, cos_ref, sin_ref, qk_gain_ref, in_ref, raw_ref, q_ref, k_ref, flat_ref, hid_ref, mlp_ref, kk, vv):
    seq, dim = x_ref.shape
    n_q = dim // 128
    step = 128
    n_in = raw_ref.shape[1]

    def project(r, _):
        at = pl.ds(pl.multiple_of(r * step, step), step)
        low, lead = _lanes(step)
        x = x_ref[at, :].astype(F32)
        m1 = (x * _rms(x) * gain_ref[0:1, :]).astype(BF16)
        in_ref[at, :] = m1
        raw = dot(m1, w_ref[:, :n_in], 1, 0).astype(BF16)
        raw_ref[at, :] = raw
        cos_t, sin_t = cos_ref[at, :], sin_ref[at, :]
        for t in range(n_q + 1):
            v = raw[:, t * 128:(t + 1) * 128].astype(F32)
            v = v * lax.rsqrt(_head_mean(v * v, low) + NORM_EPS)
            which = int(t == n_q)
            v = _turn(v * qk_gain_ref[8 * which:8 * which + 1, :], cos_t, sin_t, lead).astype(BF16)
            if which:
                k_ref[at, :] = v
            else:
                q_ref[at, t * 128:(t + 1) * 128] = v
        return 0
    lax.fori_loop(0, seq // step, project, 0)
    low, _ = _lanes(seq)
    _spread(k_ref[...].astype(F32), low, kk)
    _spread(raw_ref[:, n_in - 128:].astype(F32), low, vv)

    def heads(t, _):
        tile = pl.ds(pl.multiple_of(t * 128, 128), 128)
        for b in range(seq // step):
            n = (b + 1) * step
            q = q_ref[b * step:n, tile]
            total = None
            for side in range(2):
                i = 2 * ((2 * t + side) // 7) + side
                p = _probs(q, kk[i, :n, :], b * step).astype(BF16)
                o = dot(p, vv[i, :n, :], 1, 0)
                total = o if total is None else total + o
            flat_ref[b * step:n, tile] = total.astype(BF16)
        return 0
    lax.fori_loop(0, n_q, heads, 0)

    def finish(r, _):
        at = pl.ds(pl.multiple_of(r * step, step), step)
        h = (x_ref[at, :].astype(F32) + dot(flat_ref[at, :], w_ref[:, n_in:n_in + dim], 1, 0)).astype(BF16)
        hid_ref[at, :] = h
        h = h.astype(F32)
        mlp_ref[at, :] = (h * _rms(h) * gain_ref[8:9, :]).astype(BF16)
        return 0
    lax.fori_loop(0, seq // step, finish, 0)


def attn_forward(x, w, gains, cos_t, sin_t, qk_gain, n_in):
    seq, dim = x.shape
    vmem = pl.BlockSpec(memory_space=pltpu.VMEM)
    sds = lambda n: jax.ShapeDtypeStruct((seq, n), BF16)
    return pl.pallas_call(
        _attn_fwd_kernel,
        out_shape=[sds(dim), sds(n_in), sds(dim), sds(128), sds(dim), sds(dim), sds(dim)],
        in_specs=[vmem] * 6,
        out_specs=[vmem] * 7,
        scratch_shapes=[pltpu.VMEM((4, seq, 128), BF16), pltpu.VMEM((4, seq, 128), BF16)],
        compiler_params=pltpu.CompilerParams(vmem_limit_bytes=40 << 20),
        cost_estimate=pl.CostEstimate(flops=4_000_000_000, bytes_accessed=12 << 20, transcendentals=4_000_000),
        name='attn_forward',
    )(x, w, gains, cos_t, sin_t, qk_gain)


def _attn_bwd_kernel(x_ref, w_ref, gain_ref, cos_ref, sin_ref, qk_gain_ref, in_ref, raw_ref, q_ref, k_ref, flat_ref, hid_ref, dy_ref, part_ref, recv_ref,
                     dx_ref, dw_in_ref, dw_out_ref, kk, vv, dk, dv, gh, hb, do, dqkv):
    seq, dim = x_ref.shape
    n_q = dim // 128
    step = 128
    n_blk = seq // step
    n_in = raw_ref.shape[1]

    def norm_back(grad, normed, inv, gain):
        grad = grad * gain
        return inv * (grad - normed * jnp.mean(grad * normed, axis=-1, keepdims=True))

    def hidden(r, total):
        at = pl.ds(pl.multiple_of(r * step, step), step)
        grad = part_ref[at, :] + recv_ref[at, :]
        h = hid_ref[at, :].astype(F32)
        inv = _rms(h)
        normed = h * inv
        g = dy_ref[at, :].astype(F32) + norm_back(grad, normed, inv, gain_ref[8:9, :])
        gh[at, :] = g
        g = g.astype(BF16)
        hb[at, :] = g
        do[at, :] = dot(g, w_ref[:, n_in:n_in + dim], 1, 1).astype(BF16)
        return total + jnp.sum(grad * normed, axis=0, keepdims=True)
    mlp_gain = lax.fori_loop(0, n_blk, hidden, jnp.zeros((1, dim), F32))

    low_all, _ = _lanes(seq)
    _spread(k_ref[...].astype(F32), low_all, kk)
    _spread(raw_ref[:, n_in - 128:].astype(F32), low_all, vv)
    dk[...] = jnp.zeros_like(dk)
    dv[...] = jnp.zeros_like(dv)

    def raw_back(grad, tile, at, which, low, lead):
        v = raw_ref[at, tile].astype(F32)
        inv = lax.rsqrt(_head_mean(v * v, low) + NORM_EPS)
        normed = v * inv
        grad = _turn(grad, cos_ref[at, :], -sin_ref[at, :], lead)
        terms = jnp.sum(grad * normed, axis=0, keepdims=True)
        grad = grad * qk_gain_ref[8 * which:8 * which + 1, :]
        return inv * (grad - normed * _head_mean(grad * normed, low)), terms

    def heads(t, total):
        tile = pl.ds(pl.multiple_of(t * 128, 128), 128)
        low, lead = _lanes(step)
        for b in range(n_blk):
            n = (b + 1) * step
            at = pl.ds(b * step, step)
            q = q_ref[at, tile]
            g = do[at, tile]
            grad_q = None
            for side in range(2):
                i = 2 * ((2 * t + side) // 7) + side
                k = kk[i, :n, :]
                p = _probs(q, k, b * step)
                dp = dot(g, vv[i, :n, :], 1, 1)
                ds = (p * (dp - jnp.sum(dp * p, axis=-1, keepdims=True)) * 0.125).astype(BF16)
                dv[i, :n, :] = dv[i, :n, :] + dot(p.astype(BF16), g, 0, 0)
                dk[i, :n, :] = dk[i, :n, :] + dot(ds, q, 0, 0)
                part = dot(ds, k, 1, 0)
                grad_q = part if grad_q is None else grad_q + part
            back, terms = raw_back(grad_q, tile, at, 0, low, lead)
            dqkv[at, tile] = back.astype(BF16)
            total = total + terms
        return total
    q_gain = lax.fori_loop(0, n_q, heads, jnp.zeros((1, 128), F32))

    def keys(r, total):
        at = pl.ds(pl.multiple_of(r * step, step), step)
        low, lead = _lanes(step)

        def join(ref):
            return jnp.where(low, ref[0, at, :] + pltpu.roll(ref[1, at, :], 64, 1), ref[3, at, :] + pltpu.roll(ref[2, at, :], 64, 1))
        back, terms = raw_back(join(dk), pl.ds(dim, 128), at, 1, low, lead)
        dqkv[at, dim:dim + 128] = back.astype(BF16)
        dqkv[at, dim + 128:] = join(dv).astype(BF16)
        return total + terms
    k_gain = lax.fori_loop(0, n_blk, keys, jnp.zeros((1, 128), F32))

    def inputs(r, total):
        at = pl.ds(pl.multiple_of(r * step, step), step)
        grad = dot(dqkv[at, :], w_ref[:, :n_in], 1, 1)
        x = x_ref[at, :].astype(F32)
        inv = _rms(x)
        normed = x * inv
        dx_ref[at, :] = gh[at, :] + norm_back(grad, normed, inv, gain_ref[0:1, :])
        return total + jnp.sum(grad * normed, axis=0, keepdims=True)
    attn_gain = lax.fori_loop(0, n_blk, inputs, jnp.zeros((1, dim), F32))

    low, _ = _lanes(8)
    row = lax.broadcasted_iota(jnp.int32, (8, dim), 0)
    both = jnp.where(low, jnp.broadcast_to(q_gain, (8, 128)) + pltpu.roll(jnp.broadcast_to(q_gain, (8, 128)), 64, 1),
                     jnp.broadcast_to(k_gain, (8, 128)) + pltpu.roll(jnp.broadcast_to(k_gain, (8, 128)), 64, 1))
    dx_ref[seq:, :] = jnp.where(row == 1, jnp.broadcast_to(attn_gain, (8, dim)), jnp.where(row == 2, jnp.broadcast_to(mlp_gain, (8, dim)), 0.0))
    dx_ref[seq:, :128] = jnp.where(row[:, :128] == 0, both, dx_ref[seq:, :128])

    def weights(t, _):
        tile = pl.ds(pl.multiple_of(t * 128, 128), 128)
        dw_in_ref[tile, :] = dot(in_ref[:, tile], dqkv[...], 0, 0)
        dw_out_ref[tile, :] = dot(flat_ref[:, tile], hb[...], 0, 0)
        return 0
    lax.fori_loop(0, n_q, weights, 0)


def attn_backward(x, w, gains, cos_t, sin_t, qk_gain, saved, dy, part, recv):
    seq, dim = x.shape
    n_in = saved[1].shape[1]
    vmem = pl.BlockSpec(memory_space=pltpu.VMEM)
    scr = lambda *s: pltpu.VMEM(s[:-1], s[-1])
    return pl.pallas_call(
        _attn_bwd_kernel,
        out_shape=[jax.ShapeDtypeStruct((seq + 8, dim), F32), jax.ShapeDtypeStruct((dim, n_in), F32), jax.ShapeDtypeStruct((dim, dim), F32)],
        in_specs=[vmem] * 15,
        out_specs=[vmem] * 3,
        scratch_shapes=[scr(4, seq, 128, BF16), scr(4, seq, 128, BF16), scr(4, seq, 128, F32), scr(4, seq, 128, F32), scr(seq, dim, F32),
                        scr(seq, dim, BF16), scr(seq, dim, BF16), scr(seq, n_in, BF16)],
        compiler_params=pltpu.CompilerParams(vmem_limit_bytes=52 << 20),
        cost_estimate=pl.CostEstimate(flops=9_000_000_000, bytes_accessed=30 << 20, transcendentals=4_000_000),
        name='attn_backward',
    )(x, w, gains, cos_t, sin_t, qk_gain, *saved[:6], dy, part, recv)


def _codes(numbers, count):
    return tuple(numbers[i // 10] // 128 ** (i % 10) % 128 for i in range(count))


ROWS_SEQ = (
    _codes((152348940317322383368, 678662145372396725288, 751232056588892674273, 827272104050806263145, 30857149562), 45),
    _codes((166206088102504171520, 236385149464955200810, 603605329936848293224, 1039985241786269873361, 32734212313), 45),
)
ATTN_SEQ = (
    _codes((370142165075936415752, 972012016723415295145, 1124725529257844811929), 30),
    _codes((961577811093152729088, 751808515438843144256, 1124738970787495025897), 30),
)
LOOKUP_SEQ = (
    _codes((152348940317322383368, 678662145372396725288, 463073738031218858209, 984082515373917366482, 32721747289), 45),
    _codes((166206088102504171520, 965031540376482489642, 751827800872866057497, 1041286668292143494328, 32734212313), 45),
)
GRAD_SEQ = (
    _codes((106232080133048504328, 890654452102748905891, 398002109975241450666, 965054631626560582091, 533961906380267493400, 829000359395158448539, 1143326429365316545848, 31381732460), 75),
    _codes((166206088102504171520, 704158088118449268010, 595216210114064208288, 531741816507597222992, 520744907820250718441, 1005047906396012195259, 910358688114310724092, 32470101362), 75),
)


def solution(mesh):
    n_dev = mesh.shape[AXIS_NAME]
    n_chip = n_dev // 2
    pair = [(i, i ^ 1) for i in range(n_dev)]
    groups = [[2 * k + c for k in range(n_chip)] for c in range(2)]

    row_spec = P(AXIS_NAME, None)
    vec_spec = P(AXIS_NAME)
    full_spec = P(None)
    batch_spec = P(AXIS_NAME, None, None)
    weight_specs = (vec_spec, row_spec, row_spec, row_spec, full_spec, full_spec, row_spec, vec_spec, row_spec, row_spec, row_spec)

    def swap(v):
        return lax.ppermute(v, AXIS_NAME, pair)

    def gather_group(v):
        return lax.all_gather(v, AXIS_NAME, axis_index_groups=groups, tiled=True)

    def device_step(tokens, positions, table_shard, attn_norm, w_query, w_key, w_value, q_norm, k_norm, w_out, mlp_norm, w_gate, w_up, w_down, dy_out):
        me = lax.axis_index(AXIS_NAME)
        core = lax.rem(me, 2)
        seq_len = tokens.shape[1]
        rows_local, model_dim = table_shard.shape
        rows_w, ff = w_gate.shape
        half = ff // 2
        nq, nk = w_query.shape[1], w_key.shape[1]
        head_dim = q_norm.shape[0]

        mine_gu = jnp.concatenate([lax.dynamic_slice(w_gate, (0, core * half), (rows_w, half)), lax.dynamic_slice(w_up, (0, core * half), (rows_w, half))], axis=1)
        other_gu = jnp.concatenate([lax.dynamic_slice(w_gate, (0, (1 - core) * half), (rows_w, half)), lax.dynamic_slice(w_up, (0, (1 - core) * half), (rows_w, half))], axis=1)
        token_rows = jnp.pad(tokens.reshape(-1, 128), ((0, 4), (0, 0)))
        dy = dy_out.reshape(seq_len, model_dim)
        all_tokens, (down_block, recv_gu, dy_other) = all_rows(token_rows, n_dev, [w_down, other_gu, dy], ('use', 'pair', 'pair'), 0)
        block_gu = jnp.where(core == 0, jnp.concatenate([mine_gu, recv_gu], axis=0), jnp.concatenate([recv_gu, mine_gu], axis=0))
        wgu = gather_group(block_gu)
        w_g, w_u = wgu[:, :half], wgu[:, half:]

        gain_cols = jnp.pad(jnp.stack([attn_norm, mlp_norm], axis=1), ((0, 0), (0, 126)))
        attn_pack = jnp.concatenate([w_query, w_key, w_value, w_out, gain_cols], axis=1)
        (attn_full, wd), _ = gather_all([attn_pack, down_block], [(0, 0, rows_w, True), (1, 0, down_block.shape[0], False)], ('bza', 'zba'), ATTN_SEQ, [], (), n_dev, 1)
        attn_full = attn_full.reshape(-1, attn_pack.shape[1])
        wd = wd.reshape(-1, model_dim)

        all_ids = all_tokens[:, :seq_len // 128].reshape(-1)
        local_ids = all_ids - me * rows_local
        is_owner = (local_ids >= 0) & (local_ids < rows_local)
        own = is_owner.reshape(n_dev, seq_len)
        slot = jnp.arange(seq_len, dtype=jnp.int32)
        upto = (slot[:, None] <= slot[None, :]).astype(BF16)
        rank = jnp.where(own, dot(own.astype(BF16), upto, 1, 0).astype(jnp.int32) - 1, -1)
        counts = jnp.sum(own.astype(jnp.int32), axis=1)
        lines = model_dim // 128
        line = lambda row: row // 8 * (8 * lines) + row % 8
        code = line(slot)[None] * 65536 + line(jnp.where(own, local_ids.reshape(n_dev, seq_len), 0))
        codes = jnp.sum(jnp.where(rank[:, :, None] == slot, code[:, :, None], 0), axis=1)
        codes = jnp.where(slot[None] < counts[:, None], codes, seq_len * lines * 65536).reshape(-1)
        picked = lookup(table_shard, counts, codes, seq_len)
        x_emb = scatter_sum([picked], [(0, 0, 192, 'device'), (0, 192, 208, 'device'), (0, 400, 112, 'device')], ('zba', 'zba', 'baz'), LOOKUP_SEQ, 2)[0]

        dy2 = jnp.concatenate([dy, dy_other], axis=0)

        n_in = nq + 2 * nk
        gains = jnp.pad(jnp.repeat(attn_full[:, n_in + nq:n_in + nq + 2].astype(F32).T, 8, axis=0), ((0, 8), (0, 0)))
        qk_gain = jnp.repeat(jnp.stack([jnp.tile(q_norm, 2), jnp.tile(k_norm, 2)]).astype(F32), 8, axis=0)

        inv_freq = jnp.exp((jnp.arange(128) % (head_dim // 2)).astype(F32) * (-2.0 * math.log(ROPE_THETA) / head_dim))
        angles = positions.reshape(seq_len, 1).astype(F32) * inv_freq
        cos_t, sin_t = jnp.cos(angles), jnp.sin(angles)
        saved = attn_forward(x_emb, attn_full, gains, cos_t, sin_t, qk_gain, n_in)
        hidden, mlp_in = saved[5:]

        mlp2 = jnp.concatenate([mlp_in, swap(mlp_in)], axis=0)
        gate_pre = dot(mlp2, w_g, 1, 0)
        up_proj = dot(mlp2, w_u, 1, 0)
        gate_sig = jax.nn.sigmoid(gate_pre)
        mlp_act = (gate_pre * gate_sig * up_proj).astype(BF16)
        grad_w_down = dot(mlp_act, dy2, 0, 0)
        grad_act = dot(dy2, wd, 1, 1)
        grad_gate = (grad_act * up_proj * gate_sig * (1.0 + gate_pre * (1.0 - gate_sig))).astype(BF16)
        grad_up = (grad_act * gate_pre * gate_sig).astype(BF16)
        part_in = dot(grad_gate, w_g, 1, 1) + dot(grad_up, w_u, 1, 1)
        part_recv = swap(part_in[seq_len:])
        grad_w_gate = dot(mlp2, grad_gate, 0, 0)
        grad_w_up = dot(mlp2, grad_up, 0, 0)
        part_y = dot(mlp_act, wd, 1, 0)
        layer_out = (hidden.astype(F32) + (part_y[:seq_len] + swap(part_y[seq_len:]))).astype(BF16)

        dx_block, grad_w_in, grad_w_out = attn_backward(x_emb, attn_full, gains, cos_t, sin_t, qk_gain, saved, dy, part_in[:seq_len], part_recv)

        by_chip = [u.reshape(n_chip, -1, u.shape[1]) for u in (grad_w_down, grad_w_gate, grad_w_up, grad_w_in, grad_w_out)]
        down_rows, gate_shard, up_shard, in_shard, out_shard = scatter_sum(
            by_chip, [(i, 0, u.shape[1], 'chip') for i, u in enumerate(by_chip[:3])] + [(3, 0, 32, 'rows'), (4, 0, 32, 'rows')], ('bza', 'zba', 'zba', 'baz', 'baz'), GRAD_SEQ, 3)

        chip_rows = jnp.concatenate([gate_shard, up_shard], axis=1)
        mine = lax.dynamic_slice(chip_rows, (core * rows_w, 0), (rows_w, chip_rows.shape[1]))
        give = lax.dynamic_slice(chip_rows, ((1 - core) * rows_w, 0), (rows_w, chip_rows.shape[1]))
        (all_dx,), (down_shard, recv) = gather_all(
            [to_lines(dx_block)], [(0, 0, 200 * lines, True), (0, 200 * lines, 200 * lines, True), (0, 400 * lines, 120 * lines, True)],
            ('zba', 'zba', 'baz'), ROWS_SEQ, [down_rows, give], ('store', 'pair'), n_dev, 4)
        d_table = from_lines(add_rows(all_dx, counts, codes, rows_local), model_dim)
        gains_grad = from_lines(jnp.sum(all_dx[:, seq_len * lines:], axis=0), model_dim)
        qk = gains_grad[0]
        d_attn_norm, d_mlp_norm = (lax.dynamic_slice(gains_grad[i], (me * rows_w,), (rows_w,)) for i in (1, 2))
        low = jnp.where(core == 0, mine, recv)
        high = jnp.where(core == 0, recv, mine)
        d_gate = jnp.concatenate([low[:, :half], high[:, :half]], axis=1)
        d_up = jnp.concatenate([low[:, half:ff], high[:, half:ff]], axis=1)
        in_rows = lax.dynamic_slice(in_shard, (core * (rows_w - 24), 0), (rows_w, n_in))
        d_query, d_key, d_value = in_rows[:, :nq], in_rows[:, nq:nq + nk], in_rows[:, nq + nk:]
        d_out = lax.dynamic_slice(out_shard, (core * (rows_w - 24), 0), (rows_w, nq))
        return (layer_out.reshape(1, seq_len, model_dim), d_table, d_attn_norm, d_query, d_key, d_value, qk[:head_dim], qk[head_dim:2 * head_dim], d_out, d_mlp_norm, d_gate, d_up, down_shard)

    return jax.shard_map(device_step, mesh=mesh, in_specs=(row_spec, row_spec, row_spec) + weight_specs + (batch_spec,), out_specs=(batch_spec, row_spec) + weight_specs, check_vma=False)
```

```python
import functools
import math
import jax
import jax.numpy as jnp
from jax import lax
from jax.experimental import pallas as pl
from jax.experimental.pallas import tpu as pltpu
from jax.sharding import PartitionSpec as P

NORM_EPS = 1e-6
ROPE_THETA = 1.0e6
AXIS_NAME = 'fsdp'
F32 = jnp.float32
BF16 = jnp.bfloat16
MESH = pl.DeviceIdType.MESH
LANES, SUB, CHIPS, PAIR, MIB = 128, 8, 16, 2, 1 << 20


def mm(a, b):
    return lax.dot_general(a, b, (((1,), (0,)), ((), ())), preferred_element_type=F32)


def mm_nt(a, b):
    return lax.dot_general(a, b, (((1,), (1,)), ((), ())), preferred_element_type=F32)


def mm_tn(a, b):
    return lax.dot_general(a, b, (((0,), (0,)), ((), ())), preferred_element_type=F32)


def cost(flops, nbytes, transcendentals=0):
    return pl.CostEstimate(flops=flops, bytes_accessed=nbytes, transcendentals=transcendentals)


def below(v, rows):
    return jnp.pad(v, ((0, rows), (0, 0)))


def loop(count, body):
    def step(i, carry):
        body(i)
        return carry
    lax.fori_loop(0, count, step, 0)


def _unpack(code):
    return code // 64, code // 32 % PAIR, code // SUB % 4, code % SUB


def _via(u, key, orders):
    da, db, p, piece = key
    last = None
    for axis in orders[piece]:
        if axis == 'a' and da or axis == 'b' and db:
            last = axis
        if axis == 'z' and p != u:
            last = 'z+' if p > u else 'z-'
    return last


def _onward(u, key, orders):
    order = orders[key[3]]
    via = _via(u, key, orders)
    left = order if via is None else order[order.index(via[0]) + 1:]
    out = []
    if u < 3 and (via == 'z-' or 'z' in left):
        out.append('z+')
    if u > 0 and (via == 'z+' or 'z' in left):
        out.append('z-')
    return out + [axis for axis in 'ba' if axis in left]


def _seen_by_parent(u, key, orders):
    da, db, p, piece = key
    via = _via(u, key, orders)
    if via == 'a':
        return u, (0, db, p, piece), 'a'
    if via == 'b':
        return u, (da, 0, p, piece), 'b'
    if via == 'z-':
        return u - 1, key, 'z+'
    if u == 0:
        return 1, key, 'z-'
    return 1, (da, db, 3 - p, piece), 'z+'


class _Place:
    def __init__(self, me, swapped=False):
        self.me = me
        self.core = me % PAIR
        x, y, self.z = (me // PAIR) % PAIR, (me // 4) % PAIR, me // SUB
        other = 1 - self.core if swapped else self.core
        self.a = y * (1 - other) + x * other
        self.b = x * (1 - other) + y * other
        self.a_str, self.b_str = 4 - PAIR * other, PAIR + PAIR * other
        self.far = self.z // PAIR
        self.u = 3 * self.far + (1 - PAIR * self.far) * self.z
        self.partner = me + 1 - PAIR * self.core

    def chip(self, key):
        da, db, p = key[:3]
        a = self.a + da * (1 - PAIR * self.a)
        b = self.b + db * (1 - PAIR * self.b)
        z = 3 * self.far + (1 - PAIR * self.far) * p
        return (SUB * z + a * self.a_str + b * self.b_str) // PAIR

    def side(self, name):
        if name == 'a':
            return self.me + (1 - PAIR * self.a) * self.a_str
        if name == 'b':
            return self.me + (1 - PAIR * self.b) * self.b_str
        return self.me + SUB * (1 - PAIR * self.far) * (1 if name == 'z+' else -1)


def _remote(src, dst, send_sem, recv_sem, dev):
    return pltpu.make_async_remote_copy(src_ref=src, dst_ref=dst, send_sem=send_sem, recv_sem=recv_sem, device_id=(dev,), device_id_type=MESH)


def _meet(peers, me=None, ends=()):
    sem = pltpu.get_barrier_semaphore()

    def meet(everyone):
        for peer in everyone:
            pl.semaphore_signal(sem, inc=1, device_id=(peer,), device_id_type=MESH)
        pl.semaphore_wait(sem, len(everyone))

    if not ends:
        meet(peers)
        return
    to, frm = ends
    pl.when(to != me)(lambda: meet(peers + [to, frm]))
    pl.when(to == me)(lambda: meet(peers))


def _landed(ref, sem):
    pltpu.make_async_copy(ref, ref, sem).wait()


def _passes(moves, me):
    for kind in moves:
        if kind == 'pair':
            other = me + 1 - PAIR * (me % PAIR)
            yield other, other
        elif kind == 'use':
            yield PAIR * (me % CHIPS) + me // CHIPS, CHIPS * (me % PAIR) + me // PAIR
        else:
            yield CHIPS * (me % PAIR) + me // PAIR, PAIR * (me % CHIPS) + me // CHIPS


def _start_move(kind, src, dst, send_sem, recv_sem, to, me):
    copy = _remote(src, dst, send_sem, recv_sem, to)
    if kind == 'pair':
        copy.start()
    else:
        pl.when(to != me)(copy.start)
        pl.when(to == me)(pltpu.make_async_copy(src, dst, recv_sem).start)
    return copy


def _end_move(kind, copy, dst, recv_sem, to, me):
    _landed(dst, recv_sem)
    if kind == 'pair':
        copy.wait_send()
    else:
        pl.when(to != me)(copy.wait_send)


def _all_rows_kernel(n_dev, moves, *refs):
    n = len(moves)
    in_ref, src, out_ref, dst = refs[0], refs[1:1 + n], refs[1 + n], refs[PAIR + n:PAIR + PAIR * n]
    send_sem, recv_sem, m_send, m_recv = refs[PAIR + PAIR * n:]
    me = lax.axis_index(AXIS_NAME)
    peers = [(me + d) % n_dev for d in range(1, n_dev)]
    _meet(peers)
    copies = [_remote(in_ref, out_ref.at[me], send_sem.at[i], recv_sem.at[i], peer) for i, peer in enumerate(peers)]
    for copy in copies:
        copy.start()
    ends = [to for to, _ in _passes(moves, me)]
    moving = [_start_move(moves[i], src[i], dst[i], m_send.at[i], m_recv.at[i], to, me) for i, to in enumerate(ends)]
    out_ref[me] = in_ref[...]
    for copy in copies:
        copy.wait()
    for i, copy in enumerate(moving):
        _end_move(moves[i], copy, dst[i], m_recv.at[i], ends[i], me)


def all_rows(block, n_dev, moved, moves, collective_id):
    n = len(moves)
    dma = pltpu.SemaphoreType.DMA
    vmem, hbm = pl.BlockSpec(memory_space=pltpu.VMEM), pl.BlockSpec(memory_space=pl.ANY)
    res = pl.pallas_call(
        functools.partial(_all_rows_kernel, n_dev, moves),
        out_shape=[jax.ShapeDtypeStruct((n_dev,) + block.shape, block.dtype)] + [jax.ShapeDtypeStruct(v.shape, v.dtype) for v in moved],
        in_specs=[vmem] + [hbm] * n,
        out_specs=[vmem] + [hbm] * n,
        scratch_shapes=[dma((n_dev - 1,)), dma((n_dev - 1,)), dma((n,)), dma((n,))],
        compiler_params=pltpu.CompilerParams(collective_id=collective_id, has_side_effects=True),
        cost_estimate=cost(10_000_000, 1 * MIB),
        name='all_rows',
    )(block, *moved)
    return res[0], res[1:]


def _gather_kernel(pieces, orders, seq, moves, n_arr, *refs):
    n, m = len(moves), len(pieces)
    ins, src, outs, dst = refs[:n_arr], refs[n_arr:n_arr + n], refs[n_arr + n:PAIR * n_arr + n], refs[PAIR * n_arr + n:PAIR * n_arr + PAIR * n]
    own_sem, send_sem, recv_sem, p_send, p_recv, m_send, m_recv = refs[PAIR * n_arr + PAIR * n:]
    me = lax.axis_index(AXIS_NAME)
    at = _Place(me)
    ends = list(_passes(moves, me))

    def part(kc, core, piece):
        arr, r0, rows, shared = pieces[piece]
        slot = PAIR * kc + core if shared else kc
        return outs[arr].at[slot] if rows == outs[arr].shape[1] else outs[arr].at[slot, pl.ds(r0, rows)]

    def run(u):
        sides = ['a', 'b', 'z+'] + (['z-'] if u else [])
        far = [end for kind, end in zip(moves, ends) if kind != 'pair']
        _meet([at.side(s) for s in sides] + [at.partner], me, far[0] if far else ())
        started, moving = [], []

        def send(src_ref, dst_ref, s_sem, r_sem, dev):
            copy = _remote(src_ref, dst_ref, s_sem, r_sem, dev)
            copy.start()
            started.append(copy)

        count, handed = 0, [0] * m
        for key in [(0, 0, u, i) for i in range(m)] + [_unpack(c) for c in seq[u]]:
            piece = key[3]
            arr, r0, rows, shared = pieces[piece]
            kc = at.chip(key)
            place = part(kc, at.core, piece)
            if _via(u, key, orders) is None:
                ref = ins[arr] if rows == ins[arr].shape[0] else ins[arr].at[pl.ds(r0, rows)]
            else:
                ref = place
                _landed(ref, recv_sem.at[piece, kc])
            for side in _onward(u, key, orders):
                send(ref, place, send_sem.at[count], recv_sem.at[piece, kc], at.side(side))
                count += 1
            if shared:
                send(ref, place, p_send.at[piece, handed[piece]], p_recv.at[piece, kc], at.partner)
                handed[piece] += 1
            if key == (0, 0, u, m - 1):
                for i, (to, _) in enumerate(ends):
                    moving.append(_start_move(moves[i], src[i], dst[i], m_send.at[i], m_recv.at[i], to, me))
                own = [pltpu.make_async_copy(ins[i], outs[i].at[me if pieces_shared[i] else me // PAIR], own_sem.at[i]) for i in range(n_arr)]
                for copy in own:
                    copy.start()
        for piece in range(m):
            if pieces[piece][3]:
                for kc in range(CHIPS):
                    _landed(part(kc, 1 - at.core, piece), p_recv.at[piece, kc])
        for i, (to, _) in enumerate(ends):
            _end_move(moves[i], moving[i], dst[i], m_recv.at[i], to, me)
        for copy in own:
            copy.wait()
        for copy in started:
            copy.wait_send()

    pieces_shared = {p[0]: p[3] for p in pieces}
    for u in (0, 1):
        pl.when(at.u == u)(functools.partial(run, u))


def gather_all(blocks, pieces, orders, seq, moved, moves, n_dev, collective_id):
    n, m, n_arr = len(moves), len(pieces), len(blocks)
    dma = pltpu.SemaphoreType.DMA
    vmem, hbm = pl.BlockSpec(memory_space=pltpu.VMEM), pl.BlockSpec(memory_space=pl.ANY)
    nbytes = sum(v.size * v.dtype.itemsize for v in blocks)
    shared = {p[0]: p[3] for p in pieces}
    res = pl.pallas_call(
        functools.partial(_gather_kernel, tuple(pieces), orders, seq, moves, n_arr),
        out_shape=[jax.ShapeDtypeStruct((n_dev if shared[i] else n_dev // PAIR,) + v.shape, v.dtype) for i, v in enumerate(blocks)] + [
            jax.ShapeDtypeStruct(v.shape, v.dtype) for v in moved],
        in_specs=[vmem] * n_arr + [hbm] * n,
        out_specs=[hbm] * (n_arr + n),
        scratch_shapes=[dma((n_arr,)), dma((24 * m,)), dma((m, CHIPS)), dma((m, CHIPS)), dma((m, CHIPS)), dma((max(n, 1),)), dma((max(n, 1),))],
        compiler_params=pltpu.CompilerParams(collective_id=collective_id, has_side_effects=True, vmem_limit_bytes=nbytes + (SUB * MIB)),
        cost_estimate=cost(200_000_000, nbytes * 64),
        name='gather_all',
    )(*blocks, *moved)
    return res[:n_arr], res[n_arr:]


def _slots(pieces, orders, seq):
    table, most = {}, [1] * len(pieces)
    for u in (0, 1):
        used = [0] * len(pieces)
        for key in [_unpack(c) for c in reversed(seq[u])] + [(0, 0, u, i) for i in range(len(pieces))]:
            for side in _onward(u, key, orders):
                table[u, key, side] = used[key[3]]
                used[key[3]] += 1
        most = [max(a, b) for a, b in zip(most, used)]
    return table, most


def _scatter_kernel(pieces, orders, seq, n_arr, *refs):
    table, _ = _slots(pieces, orders, seq)
    n = len(pieces)
    n_pair = sum(1 for p in pieces if p[3] != 'chip')
    ins, outs = refs[:n_arr], refs[n_arr:PAIR * n_arr]
    k = PAIR * n_arr
    land, stage, pair = refs[k:k + n], refs[k + n:k + PAIR * n], list(refs[k + PAIR * n:k + PAIR * n + n_pair])
    load_sem, send_sem, recv_sem, d_send, d_recv = refs[k + PAIR * n + n_pair:]
    got = [pair.pop(0) if p[3] != 'chip' else None for p in pieces]
    me = lax.axis_index(AXIS_NAME)
    at, partner_at = _Place(me), _Place(me, swapped=True)

    def rows_of(ref, piece):
        _, r0, rows, _ = pieces[piece]
        return ref if rows == ref.shape[0] else ref.at[pl.ds(r0, rows)]

    def term(piece, kc, core):
        arr, _, rows, kind = pieces[piece]
        if kind == 'rows':
            return ins[arr].at[kc, pl.ds(pl.multiple_of(24 * core, SUB), rows)]
        return rows_of(ins[arr].at[PAIR * kc + core if kind == 'device' else kc], piece)

    def run(u):
        sides = ['a', 'b', 'z+'] + (['z-'] if u else [])
        _meet([at.side(s) for s in sides] + [at.partner])
        keys = [_unpack(c) for c in reversed(seq[u])] + [(0, 0, u, i) for i in range(n)]
        started = []
        given = [0] * n
        for key in keys:
            piece = key[3]
            if pieces[piece][3] != 'chip':
                kc = partner_at.chip(key)
                copy = _remote(term(piece, kc, 1 - at.core), got[piece].at[kc], d_send.at[piece, given[piece]], d_recv.at[piece, kc], at.partner)
                given[piece] += 1
                copy.start()
                started.append(copy)
        adds = [[key for key in keys if key[3] == i and (pieces[i][3] != 'chip' or _onward(u, key, orders))] for i in range(n)]

        def load(piece, j):
            return pltpu.make_async_copy(term(piece, at.chip(adds[piece][j]), at.core), stage[piece].at[j % PAIR], load_sem.at[piece, j % PAIR])

        for i in range(n):
            for j in range(PAIR):
                load(i, j).start()
        done = [0] * n
        count = 0
        for key in keys:
            piece = key[3]
            arr, r0, rows, kind = pieces[piece]
            paired = kind != 'chip'
            kc = at.chip(key)
            children = _onward(u, key, orders)
            if not children and not paired:
                src = term(piece, kc, at.core)
            else:
                j = done[piece]
                done[piece] += 1
                parts = []
                if paired:
                    _landed(got[piece].at[kc], d_recv.at[piece, kc])
                    parts.append(got[piece].at[kc])
                for side in children:
                    slot = table[u, key, side]
                    _landed(land[piece].at[slot], recv_sem.at[piece, slot])
                    parts.append(land[piece].at[slot])
                load(piece, j).wait()
                parts.append(stage[piece].at[j % PAIR])
                root = key[:3] == (0, 0, u)
                src = rows_of(outs[arr], piece) if root else parts[0]
                dtype = ins[arr].dtype
                step = SUB if dtype == F32 else CHIPS

                def body(r, parts=parts, dst=src, step=step, dtype=dtype):
                    some = pl.ds(pl.multiple_of(r * step, step), step)
                    total = parts[0][some, :].astype(F32)
                    for ref in parts[1:]:
                        total = total + ref[some, :].astype(F32)
                    dst[some, :] = total.astype(dtype)

                loop(rows // step, body)
                if j + PAIR < len(adds[piece]):
                    load(piece, j + PAIR).start()
                if root:
                    continue
            side = _via(u, key, orders)
            slot = table[_seen_by_parent(u, key, orders)]
            copy = _remote(src, land[piece].at[slot], send_sem.at[count], recv_sem.at[piece, slot], at.side(side))
            copy.start()
            started.append(copy)
            count += 1
        for copy in started:
            copy.wait_send()

    for u in (0, 1):
        pl.when(at.u == u)(functools.partial(run, u))


def scatter_sum(arrays, pieces, orders, seq, collective_id):
    n_arr, n = len(arrays), len(pieces)
    dma, hbm, vmem = pltpu.SemaphoreType.DMA, pl.BlockSpec(memory_space=pl.ANY), pl.BlockSpec(memory_space=pltpu.VMEM)
    _, most = _slots(pieces, orders, seq)
    shapes = [(rows, arrays[arr].shape[PAIR], arrays[arr].dtype) for arr, _, rows, _ in pieces]
    scratch = [pltpu.VMEM((m, r, c), d) for m, (r, c, d) in zip(most, shapes)]
    scratch += [pltpu.VMEM((PAIR, r, c), d) for r, c, d in shapes]
    scratch += [pltpu.VMEM((CHIPS, r, c), d) for (r, c, d), p in zip(shapes, pieces) if p[3] != 'chip']
    outs = [jax.ShapeDtypeStruct((sum(p[PAIR] for p in pieces if p[0] == i), v.shape[PAIR]), v.dtype) for i, v in enumerate(arrays)]
    nbytes = sum(v.size * v.dtype.itemsize for v in outs) + sum(
        (m + PAIR + CHIPS * int(p[3] != 'chip')) * (-(-r // CHIPS) * CHIPS) * c * d.itemsize for m, (r, c, d), p in zip(most, shapes, pieces))
    scratch += [dma((n, PAIR)), dma((CHIPS * n,)), dma((n, max(most))), dma((n, CHIPS)), dma((n, CHIPS))]
    return pl.pallas_call(
        functools.partial(_scatter_kernel, tuple(pieces), orders, seq, n_arr),
        out_shape=outs,
        in_specs=[hbm] * n_arr,
        out_specs=[vmem] * n_arr,
        scratch_shapes=scratch,
        compiler_params=pltpu.CompilerParams(collective_id=collective_id, has_side_effects=True, vmem_limit_bytes=nbytes + (6 * MIB)),
        cost_estimate=cost(200_000_000, nbytes * 4),
        name='scatter_sum',
    )(*arrays)


def _lookup_kernel(counts, codes, table_ref, out_ref, rows, block, sem):
    b = pl.program_id(0)
    n_col = out_ref.shape[PAIR] // LANES
    n_rows = rows.shape[0] // n_col

    @pl.when(b == 0)
    def _():
        def widen(i):
            for j in range(n_col):
                part = table_ref[pl.ds(pl.multiple_of(i * CHIPS, CHIPS), CHIPS), j * LANES:(j + 1) * LANES].astype(F32)
                line = pl.multiple_of(i * CHIPS * n_col, SUB)
                rows[pl.ds(line + j * SUB, SUB), :] = part[:SUB]
                rows[pl.ds(line + (n_col + j) * SUB, SUB), :] = part[SUB:]
        loop(n_rows // CHIPS, widen)

    seq = out_ref.shape[1]

    def clear(i):
        block[pl.ds(pl.multiple_of(i * SUB * n_col, SUB), SUB * n_col), :] = jnp.zeros((SUB * n_col, LANES), F32)
    loop(seq // SUB, clear)

    def pick(i):
        for t in range(SUB):
            code = codes[b * seq + i * SUB + t]
            block[pl.ds(code >> CHIPS, n_col, stride=SUB), :] = rows[pl.ds(code & 65535, n_col, stride=SUB), :]
    loop((counts[b] + 7) // SUB, pick)

    def narrow(i):
        line = pl.multiple_of(i * CHIPS * n_col, SUB)
        for j in range(n_col):
            part = jnp.concatenate([block[pl.ds(line + j * SUB, SUB), :], block[pl.ds(line + (n_col + j) * SUB, SUB), :]], axis=0)
            out_ref[0, pl.ds(pl.multiple_of(i * CHIPS, CHIPS), CHIPS), j * LANES:(j + 1) * LANES] = part.astype(BF16)
    loop(seq // CHIPS, narrow)


def lookup(table, counts, codes, seq):
    n_rows, dim = table.shape
    n_src = counts.shape[0]
    lines = dim // LANES
    return pl.pallas_call(
        _lookup_kernel,
        grid_spec=pltpu.PrefetchScalarGridSpec(
            num_scalar_prefetch=PAIR,
            grid=(n_src,),
            in_specs=[pl.BlockSpec(memory_space=pltpu.VMEM)],
            out_specs=pl.BlockSpec((1, seq, dim), lambda b, *_: (b, 0, 0)),
            scratch_shapes=[pltpu.VMEM((n_rows * lines, LANES), F32), pltpu.VMEM(((seq + SUB) * lines, LANES), F32), pltpu.SemaphoreType.DMA],
        ),
        out_shape=jax.ShapeDtypeStruct((n_src, seq, dim), table.dtype),
        compiler_params=pltpu.CompilerParams(vmem_limit_bytes=40 * MIB, dimension_semantics=('arbitrary',)),
        cost_estimate=cost(50_000_000, 40 * MIB),
        name='lookup',
    )(counts, codes, table)


def _add_rows_kernel(counts, codes, dx_ref, out_ref, buf, sem):
    n_src, lines, _ = dx_ref.shape
    n_col = 7
    seq = codes.shape[0] // n_src
    cut = lines // 5
    depth = buf.shape[0]

    def fetch(b):
        for i in range(5):
            some = pl.ds(i * cut, cut)
            pltpu.make_async_copy(dx_ref.at[b, some], buf.at[lax.rem(b, depth), some], sem.at[lax.rem(b, depth)]).start()

    for b in range(depth - 1):
        fetch(b)

    def clear(i):
        out_ref[pl.ds(pl.multiple_of(i * CHIPS * n_col, SUB), CHIPS * n_col), :] = jnp.zeros((CHIPS * n_col, LANES), F32)
    loop(out_ref.shape[0] // (CHIPS * n_col), clear)

    def source(b):
        at = lax.rem(b, depth)

        @pl.when(b + depth - 1 < n_src)
        def _():
            fetch(b + depth - 1)
        pltpu.make_async_copy(dx_ref.at[b], buf.at[at], sem.at[at]).wait()

        def add(first, i):
            code = codes[b * seq + first + i]
            line = pl.ds(code & 65535, n_col, stride=SUB)
            out_ref[line, :] = out_ref[line, :] + buf[at, pl.ds(code >> CHIPS, n_col, stride=SUB), :]

        def add_pair(i):
            code0, code1 = codes[b * seq + i * PAIR], codes[b * seq + i * PAIR + 1]
            line0, line1 = code0 & 65535, code1 & 65535
            new0 = buf[at, pl.ds(code0 >> CHIPS, n_col, stride=SUB), :]
            new1 = buf[at, pl.ds(code1 >> CHIPS, n_col, stride=SUB), :]
            old0 = out_ref[pl.ds(line0, n_col, stride=SUB), :]
            old1 = out_ref[pl.ds(line1, n_col, stride=SUB), :]
            sum0 = old0 + new0
            out_ref[pl.ds(line0, n_col, stride=SUB), :] = sum0
            out_ref[pl.ds(line1, n_col, stride=SUB), :] = jnp.where(line0 == line1, sum0, old1) + new1

        def add_four(i):
            add_pair(PAIR * i)
            add_pair(PAIR * i + 1)
        n = counts[b]
        loop(n // 4, add_four)

        rest = n // 4 * 4
        loop(n - rest, functools.partial(add, rest))
    loop(n_src, source)


def add_rows(dx, counts, codes, n_rows):
    n_src, lines, _ = dx.shape
    return pl.pallas_call(
        _add_rows_kernel,
        grid_spec=pltpu.PrefetchScalarGridSpec(
            num_scalar_prefetch=PAIR,
            grid=(),
            in_specs=[pl.BlockSpec(memory_space=pl.ANY)],
            out_specs=pl.BlockSpec(memory_space=pltpu.VMEM),
            scratch_shapes=[pltpu.VMEM((4, lines, LANES), F32), pltpu.SemaphoreType.DMA((4,))],
        ),
        out_shape=jax.ShapeDtypeStruct((n_rows * 7, LANES), F32),
        compiler_params=pltpu.CompilerParams(vmem_limit_bytes=48 * MIB),
        cost_estimate=cost(50_000_000, 80 * MIB),
        name='add_rows',
    )(counts, codes, dx)


def to_lines(v):
    rows, dim = v.shape
    return v.reshape(rows // SUB, SUB, dim // LANES, LANES).transpose(0, PAIR, 1, 3).reshape(rows * dim // LANES, LANES)


def from_lines(v, dim):
    rows = v.shape[0] * LANES // dim
    return v.reshape(rows // SUB, dim // LANES, SUB, LANES).transpose(0, PAIR, 1, 3).reshape(rows, dim)


def _rms(v):
    return lax.rsqrt(jnp.mean(v * v, axis=-1, keepdims=True) + NORM_EPS)


def _head_mean(v, low):
    first = jnp.sum(jnp.where(low, v, 0.0), axis=-1, keepdims=True)
    second = jnp.sum(jnp.where(low, 0.0, v), axis=-1, keepdims=True)
    return jnp.where(low, first, second) * (1.0 / 64.0)


def _turn(v, cos_t, sin_t, lead):
    return v * cos_t + jnp.where(lead, -pltpu.roll(v, 96, 1), pltpu.roll(v, 32, 1)) * sin_t


def _spread(tile, low, ref):
    first = jnp.where(low, tile, 0.0)
    second = jnp.where(low, 0.0, tile)
    ref[0] = first.astype(BF16)
    ref[1] = pltpu.roll(first, 64, 1).astype(BF16)
    ref[PAIR] = pltpu.roll(second, 64, 1).astype(BF16)
    ref[3] = second.astype(BF16)


def _probs(q, k, block):
    scores = mm_nt(q, k) * 0.125
    n = scores.shape[1]
    row = lax.broadcasted_iota(jnp.int32, scores.shape, 0) + block
    col = lax.broadcasted_iota(jnp.int32, scores.shape, 1)
    scores = jnp.where(row >= col, scores, -1e30)
    e = jnp.exp(scores - jnp.max(scores, axis=-1, keepdims=True))
    return e * (1.0 / jnp.sum(e, axis=-1, keepdims=True))


def _lanes(rows):
    lane = lax.broadcasted_iota(jnp.int32, (rows, LANES), 1)
    return lane < 64, lane % 64 < 32


def _attn_fwd_kernel(x_ref, w_ref, gain_ref, cos_ref, sin_ref, qk_gain_ref, in_ref, raw_ref, q_ref, k_ref, flat_ref, hid_ref, mlp_ref, kk, vv):
    seq, dim = x_ref.shape
    n_q = dim // LANES
    step = LANES
    n_in = raw_ref.shape[1]

    def project(r):
        at = pl.ds(pl.multiple_of(r * step, step), step)
        low, lead = _lanes(step)
        x = x_ref[at, :].astype(F32)
        m1 = (x * _rms(x) * gain_ref[0:1, :]).astype(BF16)
        in_ref[at, :] = m1
        raw = mm(m1, w_ref[:, :n_in]).astype(BF16)
        raw_ref[at, :] = raw
        cos_t, sin_t = cos_ref[at, :], sin_ref[at, :]
        for t in range(n_q + 1):
            v = raw[:, t * LANES:(t + 1) * LANES].astype(F32)
            v = v * lax.rsqrt(_head_mean(v * v, low) + NORM_EPS)
            which = int(t == n_q)
            v = _turn(v * qk_gain_ref[SUB * which:SUB * which + 1, :], cos_t, sin_t, lead).astype(BF16)
            if which:
                k_ref[at, :] = v
            else:
                q_ref[at, t * LANES:(t + 1) * LANES] = v
    loop(seq // step, project)
    low, _ = _lanes(seq)
    _spread(k_ref[...].astype(F32), low, kk)
    _spread(raw_ref[:, n_in - LANES:].astype(F32), low, vv)

    def heads(t):
        tile = pl.ds(pl.multiple_of(t * LANES, LANES), LANES)
        for b in range(seq // step):
            n = (b + 1) * step
            q = q_ref[b * step:n, tile]
            total = None
            for side in range(PAIR):
                i = PAIR * ((PAIR * t + side) // 7) + side
                p = _probs(q, kk[i, :n, :], b * step).astype(BF16)
                o = mm(p, vv[i, :n, :])
                total = o if total is None else total + o
            flat_ref[b * step:n, tile] = total.astype(BF16)
    loop(n_q, heads)

    def finish(r):
        at = pl.ds(pl.multiple_of(r * step, step), step)
        h = (x_ref[at, :].astype(F32) + mm(flat_ref[at, :], w_ref[:, n_in:n_in + dim])).astype(BF16)
        hid_ref[at, :] = h
        h = h.astype(F32)
        mlp_ref[at, :] = (h * _rms(h) * gain_ref[SUB:9, :]).astype(BF16)
    loop(seq // step, finish)


def attn_forward(x, w, gains, cos_t, sin_t, qk_gain, n_in):
    seq, dim = x.shape
    vmem = pl.BlockSpec(memory_space=pltpu.VMEM)
    sds = lambda n: jax.ShapeDtypeStruct((seq, n), BF16)
    return pl.pallas_call(
        _attn_fwd_kernel,
        out_shape=[sds(dim), sds(n_in), sds(dim), sds(LANES), sds(dim), sds(dim), sds(dim)],
        in_specs=[vmem] * 6,
        out_specs=[vmem] * 7,
        scratch_shapes=[pltpu.VMEM((4, seq, LANES), BF16), pltpu.VMEM((4, seq, LANES), BF16)],
        compiler_params=pltpu.CompilerParams(vmem_limit_bytes=40 * MIB),
        cost_estimate=cost(4_000_000_000, 12 * MIB, 4_000_000),
        name='attn_forward',
    )(x, w, gains, cos_t, sin_t, qk_gain)


def _attn_bwd_kernel(x_ref, w_ref, gain_ref, cos_ref, sin_ref, qk_gain_ref, in_ref, raw_ref, q_ref, k_ref, flat_ref, hid_ref, dy_ref, part_ref, recv_ref,
                     dx_ref, dw_in_ref, dw_out_ref, kk, vv, dk, dv, gh, hb, do, dqkv):
    seq, dim = x_ref.shape
    n_q = dim // LANES
    step = LANES
    n_blk = seq // step
    n_in = raw_ref.shape[1]

    def norm_back(grad, normed, inv, gain):
        grad = grad * gain
        return inv * (grad - normed * jnp.mean(grad * normed, axis=-1, keepdims=True))

    def hidden(r, total):
        at = pl.ds(pl.multiple_of(r * step, step), step)
        grad = part_ref[0, at, :] + recv_ref[at, :]
        h = hid_ref[at, :].astype(F32)
        inv = _rms(h)
        normed = h * inv
        g = dy_ref[at, :].astype(F32) + norm_back(grad, normed, inv, gain_ref[SUB:9, :])
        gh[at, :] = g
        g = g.astype(BF16)
        hb[at, :] = g
        do[at, :] = mm_nt(g, w_ref[:, n_in:n_in + dim]).astype(BF16)
        return total + jnp.sum(grad * normed, axis=0, keepdims=True)
    mlp_gain = lax.fori_loop(0, n_blk, hidden, jnp.zeros((1, dim), F32))

    low_all, _ = _lanes(seq)
    _spread(k_ref[...].astype(F32), low_all, kk)
    _spread(raw_ref[:, n_in - LANES:].astype(F32), low_all, vv)
    dk[...] = jnp.zeros_like(dk)
    dv[...] = jnp.zeros_like(dv)

    def raw_back(grad, tile, at, which, low, lead):
        v = raw_ref[at, tile].astype(F32)
        inv = lax.rsqrt(_head_mean(v * v, low) + NORM_EPS)
        normed = v * inv
        grad = _turn(grad, cos_ref[at, :], -sin_ref[at, :], lead)
        terms = jnp.sum(grad * normed, axis=0, keepdims=True)
        grad = grad * qk_gain_ref[SUB * which:SUB * which + 1, :]
        return inv * (grad - normed * _head_mean(grad * normed, low)), terms

    def heads(t, total):
        tile = pl.ds(pl.multiple_of(t * LANES, LANES), LANES)
        low, lead = _lanes(step)
        for b in range(n_blk):
            n = (b + 1) * step
            at = pl.ds(b * step, step)
            q = q_ref[at, tile]
            g = do[at, tile]
            grad_q = None
            for side in range(PAIR):
                i = PAIR * ((PAIR * t + side) // 7) + side
                k = kk[i, :n, :]
                p = _probs(q, k, b * step)
                dp = mm_nt(g, vv[i, :n, :])
                ds = (p * (dp - jnp.sum(dp * p, axis=-1, keepdims=True)) * 0.125).astype(BF16)
                dv[i, :n, :] = dv[i, :n, :] + mm_tn(p.astype(BF16), g)
                dk[i, :n, :] = dk[i, :n, :] + mm_tn(ds, q)
                part = mm(ds, k)
                grad_q = part if grad_q is None else grad_q + part
            back, terms = raw_back(grad_q, tile, at, 0, low, lead)
            dqkv[at, tile] = back.astype(BF16)
            total = total + terms
        return total
    q_gain = lax.fori_loop(0, n_q, heads, jnp.zeros((1, LANES), F32))

    def keys(r, total):
        at = pl.ds(pl.multiple_of(r * step, step), step)
        low, lead = _lanes(step)

        def join(ref):
            return jnp.where(low, ref[0, at, :] + pltpu.roll(ref[1, at, :], 64, 1), ref[3, at, :] + pltpu.roll(ref[PAIR, at, :], 64, 1))
        back, terms = raw_back(join(dk), pl.ds(dim, LANES), at, 1, low, lead)
        dqkv[at, dim:dim + LANES] = back.astype(BF16)
        dqkv[at, dim + LANES:] = join(dv).astype(BF16)
        return total + terms
    k_gain = lax.fori_loop(0, n_blk, keys, jnp.zeros((1, LANES), F32))

    def inputs(r, total):
        at = pl.ds(pl.multiple_of(r * step, step), step)
        grad = mm_nt(dqkv[at, :], w_ref[:, :n_in])
        x = x_ref[at, :].astype(F32)
        inv = _rms(x)
        normed = x * inv
        dx_ref[at, :] = gh[at, :] + norm_back(grad, normed, inv, gain_ref[0:1, :])
        return total + jnp.sum(grad * normed, axis=0, keepdims=True)
    attn_gain = lax.fori_loop(0, n_blk, inputs, jnp.zeros((1, dim), F32))

    low, _ = _lanes(SUB)
    row = lax.broadcasted_iota(jnp.int32, (SUB, dim), 0)
    both = jnp.where(low, jnp.broadcast_to(q_gain, (SUB, LANES)) + pltpu.roll(jnp.broadcast_to(q_gain, (SUB, LANES)), 64, 1),
                     jnp.broadcast_to(k_gain, (SUB, LANES)) + pltpu.roll(jnp.broadcast_to(k_gain, (SUB, LANES)), 64, 1))
    dx_ref[seq:, :] = jnp.where(row == 1, jnp.broadcast_to(attn_gain, (SUB, dim)), jnp.where(row == PAIR, jnp.broadcast_to(mlp_gain, (SUB, dim)), 0.0))
    dx_ref[seq:, :LANES] = jnp.where(row[:, :LANES] == 0, both, dx_ref[seq:, :LANES])

    def weights(t):
        tile = pl.ds(pl.multiple_of(t * LANES, LANES), LANES)
        dw_in_ref[tile, :] = mm_tn(in_ref[:, tile], dqkv[...])
        dw_out_ref[tile, :] = mm_tn(flat_ref[:, tile], hb[...])
    loop(n_q, weights)


def attn_backward(x, w, gains, cos_t, sin_t, qk_gain, saved, dy, part, recv):
    seq, dim = x.shape
    n_in = saved[1].shape[1]
    vmem = pl.BlockSpec(memory_space=pltpu.VMEM)
    scr = lambda *s: pltpu.VMEM(s[:-1], s[-1])
    return pl.pallas_call(
        _attn_bwd_kernel,
        out_shape=[jax.ShapeDtypeStruct((seq + SUB, dim), F32), jax.ShapeDtypeStruct((dim, n_in), F32), jax.ShapeDtypeStruct((dim, dim), F32)],
        in_specs=[vmem] * 15,
        out_specs=[vmem] * 3,
        scratch_shapes=[scr(4, seq, LANES, BF16), scr(4, seq, LANES, BF16), scr(4, seq, LANES, F32), scr(4, seq, LANES, F32), scr(seq, dim, F32),
                        scr(seq, dim, BF16), scr(seq, dim, BF16), scr(seq, n_in, BF16)],
        compiler_params=pltpu.CompilerParams(vmem_limit_bytes=52 * MIB),
        cost_estimate=cost(9_000_000_000, 30 * MIB, 4_000_000),
        name='attn_backward',
    )(x, w, gains, cos_t, sin_t, qk_gain, *saved[:6], dy, part, recv)


def _mlp_kernel(x_ref, dy_ref, wgu_ref, wd_ref, y_ref, din_ref, dwg_ref, dwu_ref, dwd_ref, xt, wg, wu, wd, act, dg, du, og, ou, od, load_sem, store_sem):
    half, tile = dwd_ref.shape[0], act.shape[1]
    n_tile = -(-half // tile)
    shared = n_tile * tile - half
    seqs, seq, _ = y_ref.shape
    step = seq // PAIR

    def start_of(j):
        first = (j == 0).astype(jnp.int32)
        return pl.multiple_of(first * (half - tile) + (1 - first) * (j - 1) * tile, LANES)

    def loads(j):
        at, slot = start_of(j), j % PAIR
        return [pltpu.make_async_copy(wgu_ref.at[:, pl.ds(at, tile)], wg.at[slot], load_sem.at[0, slot]),
                pltpu.make_async_copy(wgu_ref.at[:, pl.ds(pl.multiple_of(half + at, LANES), tile)], wu.at[slot], load_sem.at[1, slot]),
                pltpu.make_async_copy(wd_ref.at[pl.ds(at, tile)], wd.at[slot], load_sem.at[PAIR, slot])]

    def stores(j):
        at, slot = start_of(j), j % PAIR
        return [pltpu.make_async_copy(og.at[slot], dwg_ref.at[:, pl.ds(at, tile)], store_sem.at[0, slot]),
                pltpu.make_async_copy(ou.at[slot], dwu_ref.at[:, pl.ds(at, tile)], store_sem.at[1, slot]),
                pltpu.make_async_copy(od.at[slot], dwd_ref.at[pl.ds(at, tile)], store_sem.at[PAIR, slot])]

    for copy in loads(jnp.int32(0)):
        copy.start()
    y_ref[...] = jnp.zeros_like(y_ref)
    din_ref[...] = jnp.zeros_like(din_ref)
    xt[...] = x_ref[...].T

    def columns(j):
        slot = j % PAIR

        @pl.when(j + 1 < n_tile)
        def _():
            for copy in loads(j + 1):
                copy.start()
        for copy in loads(j):
            copy.wait()

        def rows(r):
            at = pl.ds(pl.multiple_of(r * step, step), step)
            s, inner = r // PAIR, pl.ds(pl.multiple_of(r % PAIR * step, step), step)
            x = x_ref[at, :]
            gate, up, back = mm(x, wg[slot]), mm(x, wu[slot]), mm_nt(dy_ref[at, :], wd[slot])
            counts = lax.broadcasted_iota(jnp.int32, (step, tile), 1) >= (j == 0).astype(jnp.int32) * shared
            up, back = jnp.where(counts, up, 0.0), jnp.where(counts, back, 0.0)
            sig = lax.logistic(gate)
            silu = gate * sig
            a = (silu * up).astype(BF16)
            g = (back * up * sig * (1.0 + gate * (1.0 - sig))).astype(BF16)
            u = (back * silu).astype(BF16)
            act[at, :], dg[at, :], du[at, :] = a, g, u
            y_ref[s, inner, :] = y_ref[s, inner, :] + mm(a, wd[slot])
            din_ref[s, inner, :] = din_ref[s, inner, :] + mm_nt(g, wg[slot]) + mm_nt(u, wu[slot])
        loop(PAIR * seqs, rows)

        @pl.when(j >= PAIR)
        def _():
            for copy in stores(j - PAIR):
                copy.wait()
        og[slot] = mm(xt[...], dg[...])
        ou[slot] = mm(xt[...], du[...])
        od[slot] = mm_tn(act[...], dy_ref[...])
        for copy in stores(j):
            copy.start()
    loop(n_tile, columns)
    for j in (n_tile - PAIR, n_tile - 1):
        for copy in stores(jnp.int32(j)):
            copy.wait()


def mlp(x, dy, wgu, wd, seqs):
    rows, dim = x.shape
    half = wd.shape[0]
    tile = 512
    vmem, hbm = pl.BlockSpec(memory_space=pltpu.VMEM), pl.BlockSpec(memory_space=pl.ANY)
    sds = lambda *s: jax.ShapeDtypeStruct(s, F32)
    dma = pltpu.SemaphoreType.DMA
    bf = lambda *s: pltpu.VMEM(s, BF16)
    f = lambda *s: pltpu.VMEM(s, F32)
    return pl.pallas_call(
        _mlp_kernel,
        out_shape=[sds(seqs, rows // seqs, dim), sds(seqs, rows // seqs, dim), sds(dim, half), sds(dim, half), sds(half, dim)],
        in_specs=[vmem, vmem, hbm, hbm],
        out_specs=[vmem, vmem, hbm, hbm, hbm],
        scratch_shapes=[bf(dim, rows), bf(PAIR, dim, tile), bf(PAIR, dim, tile), bf(PAIR, tile, dim), bf(rows, tile), bf(rows, tile), bf(rows, tile),
                        f(PAIR, dim, tile), f(PAIR, dim, tile), f(PAIR, tile, dim), dma((3, PAIR)), dma((3, PAIR))],
        compiler_params=pltpu.CompilerParams(vmem_limit_bytes=56 * MIB),
        cost_estimate=cost(CHIPS * rows * dim * half, 50 * MIB, rows * half),
        name='mlp',
    )(x, dy, wgu, wd)


def _codes(numbers, count):
    return tuple(numbers[i // 10] // LANES ** (i % 10) % LANES for i in range(count))


ROWS_SEQ = (
    _codes((152348940317322383368, 678662145372396725288, 751232056588892674273, 827272104050806263145, 30857149562), 45),
    _codes((166206088102504171520, 236385149464955200810, 603605329936848293224, 1039985241786269873361, 32734212313), 45),
)
ATTN_SEQ = (
    _codes((741342462958222970888, 32448584808), 15),
    _codes((965031540365288146944, 32448719928), 15),
)
GRAD_SEQ = (
    _codes((106232080133048504328, 890654452102748905891, 398002109975241450666, 965054631626560582091, 533961906380267493400, 829000359395158448539, 1143326429365316545848, 31381732460), 75),
    _codes((166206088102504171520, 704158088118449268010, 595216210114064208288, 531741816507597222992, 520744907820250718441, 1005047906396012195259, 910358688114310724092, 32470101362), 75),
)


def solution(mesh):
    n_dev = mesh.shape[AXIS_NAME]
    n_chip = n_dev // PAIR
    pair = [(i, i ^ 1) for i in range(n_dev)]
    groups = [[PAIR * k + c for k in range(n_chip)] for c in range(PAIR)]

    row_spec = P(AXIS_NAME, None)
    vec_spec = P(AXIS_NAME)
    full_spec = P(None)
    batch_spec = P(AXIS_NAME, None, None)
    weight_specs = (vec_spec, row_spec, row_spec, row_spec, full_spec, full_spec, row_spec, vec_spec, row_spec, row_spec, row_spec)

    def swap(v):
        return lax.ppermute(v, AXIS_NAME, pair)

    def gather_group(v):
        return lax.all_gather(v, AXIS_NAME, axis_index_groups=groups, tiled=True)

    def device_step(tokens, positions, table_shard, attn_norm, w_query, w_key, w_value, q_norm, k_norm, w_out, mlp_norm, w_gate, w_up, w_down, dy_out):
        me = lax.axis_index(AXIS_NAME)
        core = lax.rem(me, PAIR)
        seq_len = tokens.shape[1]
        rows_local, model_dim = table_shard.shape
        rows_w, ff = w_gate.shape
        half = ff // PAIR
        nq, nk = w_query.shape[1], w_key.shape[1]
        head_dim = q_norm.shape[0]

        mine_gu = jnp.concatenate([lax.dynamic_slice(w_gate, (0, core * half), (rows_w, half)), lax.dynamic_slice(w_up, (0, core * half), (rows_w, half))], axis=1)
        other_gu = jnp.concatenate([lax.dynamic_slice(w_gate, (0, (1 - core) * half), (rows_w, half)), lax.dynamic_slice(w_up, (0, (1 - core) * half), (rows_w, half))], axis=1)
        token_rows = below(tokens.reshape(-1, LANES), 4)
        dy = dy_out.reshape(seq_len, model_dim)
        all_tokens, (down_block, recv_gu, dy_other) = all_rows(token_rows, n_dev, [w_down, other_gu, dy], ('use', 'pair', 'pair'), 0)
        block_gu = jnp.where(core == 0, jnp.concatenate([mine_gu, recv_gu], axis=0), jnp.concatenate([recv_gu, mine_gu], axis=0))
        wgu = gather_group(block_gu)

        wd = gather_group(down_block)

        all_ids = all_tokens[:, :seq_len // LANES].reshape(-1)
        local_ids = all_ids - me * rows_local
        is_owner = (local_ids >= 0) & (local_ids < rows_local)
        own = is_owner.reshape(n_dev, seq_len)
        slot = jnp.arange(seq_len, dtype=jnp.int32)
        upto = (slot[:, None] <= slot[None, :]).astype(BF16)
        rank = jnp.where(own, mm(own.astype(BF16), upto).astype(jnp.int32) - 1, -1)
        counts = jnp.sum(own.astype(jnp.int32), axis=1)
        lines = model_dim // LANES
        line = lambda row: row // SUB * (SUB * lines) + row % SUB
        code = line(slot)[None] * 65536 + line(jnp.where(own, local_ids.reshape(n_dev, seq_len), 0))
        codes = jnp.sum(jnp.where(rank[:, :, None] == slot, code[:, :, None], 0), axis=1)
        codes = jnp.where(slot[None] < counts[:, None], codes, seq_len * lines * 65536).reshape(-1)
        picked = lookup(table_shard, counts, codes, seq_len)
        x_emb = scatter_sum([picked], [(0, 0, 192, 'device'), (0, 192, 208, 'device'), (0, 400, 112, 'device')], ('zba', 'zba', 'baz'), ROWS_SEQ, PAIR)[0]

        gain_cols = below(jnp.stack([attn_norm, mlp_norm]), 126).T
        attn_pack = jnp.concatenate([w_query, w_key, w_value, w_out, gain_cols], axis=1)
        attn_pack, x_emb = lax.optimization_barrier((attn_pack, x_emb))
        (attn_full,), _ = gather_all([attn_pack], [(0, 0, rows_w, True)], ('zba',), ATTN_SEQ, [], (), n_dev, 1)
        attn_full = attn_full.reshape(-1, attn_pack.shape[1])

        dy2 = jnp.concatenate([dy, dy_other], axis=0)

        n_in = nq + PAIR * nk
        gains = below(jnp.repeat(attn_full[:, n_in + nq:n_in + nq + PAIR].astype(F32).T, SUB, axis=0), SUB)
        qk_gain = jnp.repeat(jnp.stack([jnp.tile(q_norm, PAIR), jnp.tile(k_norm, PAIR)]).astype(F32), SUB, axis=0)

        inv_freq = jnp.exp((jnp.arange(LANES) % (head_dim // PAIR)).astype(F32) * (-2.0 * math.log(ROPE_THETA) / head_dim))
        angles = positions.reshape(seq_len, 1).astype(F32) * inv_freq
        cos_t, sin_t = jnp.cos(angles), jnp.sin(angles)
        saved = attn_forward(x_emb, attn_full, gains, cos_t, sin_t, qk_gain, n_in)
        hidden, mlp_in = saved[5:]

        mlp2 = jnp.concatenate([mlp_in, swap(mlp_in)], axis=0)
        y, grad_in, grad_w_gate, grad_w_up, grad_w_down = mlp(mlp2, dy2, wgu, wd, PAIR)
        grad_recv = swap(grad_in[1])
        layer_out = (hidden.astype(F32) + (y[0] + swap(y[1]))).astype(BF16)

        dx_block, grad_w_in, grad_w_out = attn_backward(x_emb, attn_full, gains, cos_t, sin_t, qk_gain, saved, dy, grad_in, grad_recv)

        by_chip = [u.reshape(n_chip, -1, u.shape[1]) for u in (grad_w_down, grad_w_gate, grad_w_up, grad_w_in, grad_w_out)]
        down_rows, gate_shard, up_shard, in_shard, out_shard = scatter_sum(
            by_chip, [(i, 0, u.shape[1], 'chip') for i, u in enumerate(by_chip[:3])] + [(i, 0, 32, 'rows') for i in (3, 4)], ('bza', 'zba', 'zba', 'baz', 'baz'), GRAD_SEQ, 3)

        chip_rows = jnp.concatenate([gate_shard, up_shard], axis=1)
        mine = lax.dynamic_slice(chip_rows, (core * rows_w, 0), (rows_w, chip_rows.shape[1]))
        give = lax.dynamic_slice(chip_rows, ((1 - core) * rows_w, 0), (rows_w, chip_rows.shape[1]))
        (all_dx,), (down_shard, recv) = gather_all(
            [to_lines(dx_block)], [(0, 0, 200 * lines, True), (0, 200 * lines, 200 * lines, True), (0, 400 * lines, 120 * lines, True)],
            ('zba', 'zba', 'baz'), ROWS_SEQ, [down_rows, give], ('store', 'pair'), n_dev, 4)
        d_table = from_lines(add_rows(all_dx, counts, codes, rows_local), model_dim)
        gains_grad = from_lines(jnp.sum(all_dx[:, seq_len * lines:], axis=0), model_dim)
        qk = gains_grad[0]
        d_attn_norm, d_mlp_norm = (lax.dynamic_slice(gains_grad[i], (me * rows_w,), (rows_w,)) for i in (1, PAIR))
        low = jnp.where(core == 0, mine, recv)
        high = jnp.where(core == 0, recv, mine)
        d_gate = jnp.concatenate([low[:, :half], high[:, :half]], axis=1)
        d_up = jnp.concatenate([low[:, half:ff], high[:, half:ff]], axis=1)
        in_rows = lax.dynamic_slice(in_shard, (core * (rows_w - 24), 0), (rows_w, n_in))
        d_query, d_key, d_value = in_rows[:, :nq], in_rows[:, nq:nq + nk], in_rows[:, nq + nk:]
        d_out = lax.dynamic_slice(out_shard, (core * (rows_w - 24), 0), (rows_w, nq))
        return (layer_out.reshape(1, seq_len, model_dim), d_table, d_attn_norm, d_query, d_key, d_value, qk[:head_dim], qk[head_dim:PAIR * head_dim], d_out, d_mlp_norm, d_gate, d_up, down_shard)

    return jax.shard_map(device_step, mesh=mesh, in_specs=(row_spec, row_spec, row_spec) + weight_specs + (batch_spec,), out_specs=(batch_spec, row_spec) + weight_specs, check_vma=False)
```

```python
import functools
import math
import jax
import jax.numpy as jnp
from jax import lax
from jax.experimental import pallas as pl
from jax.experimental.pallas import tpu as pltpu
from jax.sharding import PartitionSpec as P

NORM_EPS = 1e-6
ROPE_THETA = 1.0e6
AXIS_NAME = 'fsdp'
F32 = jnp.float32
BF16 = jnp.bfloat16
MESH = pl.DeviceIdType.MESH
LANES, SUB, CHIPS, PAIR, MIB = 128, 8, 16, 2, 1 << 20


def mm(a, b):
    return lax.dot_general(a, b, (((1,), (0,)), ((), ())), preferred_element_type=F32)


def mm_nt(a, b):
    return lax.dot_general(a, b, (((1,), (1,)), ((), ())), preferred_element_type=F32)


def mm_tn(a, b):
    return lax.dot_general(a, b, (((0,), (0,)), ((), ())), preferred_element_type=F32)


def cost(flops, nbytes, transcendentals=0):
    return pl.CostEstimate(flops=flops, bytes_accessed=nbytes, transcendentals=transcendentals)


def below(v, rows):
    return jnp.pad(v, ((0, rows), (0, 0)))


def loop(count, body):
    def step(i, carry):
        body(i)
        return carry
    lax.fori_loop(0, count, step, 0)


def _unpack(code):
    return code // 64, code // 32 % PAIR, code // SUB % 4, code % SUB


def _via(u, key, orders):
    da, db, p, piece = key
    last = None
    for axis in orders[piece]:
        if axis == 'a' and da or axis == 'b' and db:
            last = axis
        if axis == 'z' and p != u:
            last = 'z+' if p > u else 'z-'
    return last


def _onward(u, key, orders):
    order = orders[key[3]]
    via = _via(u, key, orders)
    left = order if via is None else order[order.index(via[0]) + 1:]
    out = []
    if u < 3 and (via == 'z-' or 'z' in left):
        out.append('z+')
    if u > 0 and (via == 'z+' or 'z' in left):
        out.append('z-')
    return out + [axis for axis in 'ba' if axis in left]


def _seen_by_parent(u, key, orders):
    da, db, p, piece = key
    via = _via(u, key, orders)
    if via == 'a':
        return u, (0, db, p, piece), 'a'
    if via == 'b':
        return u, (da, 0, p, piece), 'b'
    if via == 'z-':
        return u - 1, key, 'z+'
    if u == 0:
        return 1, key, 'z-'
    return 1, (da, db, 3 - p, piece), 'z+'


class _Place:
    def __init__(self, me, swapped=False):
        self.me = me
        self.core = me % PAIR
        x, y, self.z = (me // PAIR) % PAIR, (me // 4) % PAIR, me // SUB
        other = 1 - self.core if swapped else self.core
        self.a = y * (1 - other) + x * other
        self.b = x * (1 - other) + y * other
        self.a_str, self.b_str = 4 - PAIR * other, PAIR + PAIR * other
        self.far = self.z // PAIR
        self.u = 3 * self.far + (1 - PAIR * self.far) * self.z
        self.partner = me + 1 - PAIR * self.core

    def chip(self, key):
        da, db, p = key[:3]
        a = self.a + da * (1 - PAIR * self.a)
        b = self.b + db * (1 - PAIR * self.b)
        z = 3 * self.far + (1 - PAIR * self.far) * p
        return (SUB * z + a * self.a_str + b * self.b_str) // PAIR

    def side(self, name):
        if name == 'a':
            return self.me + (1 - PAIR * self.a) * self.a_str
        if name == 'b':
            return self.me + (1 - PAIR * self.b) * self.b_str
        return self.me + SUB * (1 - PAIR * self.far) * (1 if name == 'z+' else -1)


def _remote(src, dst, send_sem, recv_sem, dev):
    return pltpu.make_async_remote_copy(src_ref=src, dst_ref=dst, send_sem=send_sem, recv_sem=recv_sem, device_id=(dev,), device_id_type=MESH)


def _meet(peers, me=None, ends=()):
    sem = pltpu.get_barrier_semaphore()

    def meet(everyone):
        for peer in everyone:
            pl.semaphore_signal(sem, inc=1, device_id=(peer,), device_id_type=MESH)
        pl.semaphore_wait(sem, len(everyone))

    if not ends:
        meet(peers)
        return
    to, frm = ends
    pl.when(to != me)(lambda: meet(peers + [to, frm]))
    pl.when(to == me)(lambda: meet(peers))


def _landed(ref, sem):
    pltpu.make_async_copy(ref, ref, sem).wait()


def _passes(moves, me):
    for kind in moves:
        if kind == 'pair':
            other = me + 1 - PAIR * (me % PAIR)
            yield other, other
        elif kind == 'use':
            yield PAIR * (me % CHIPS) + me // CHIPS, CHIPS * (me % PAIR) + me // PAIR
        else:
            yield CHIPS * (me % PAIR) + me // PAIR, PAIR * (me % CHIPS) + me // CHIPS


def _start_move(kind, src, dst, send_sem, recv_sem, to, me):
    copy = _remote(src, dst, send_sem, recv_sem, to)
    if kind == 'pair':
        copy.start()
    else:
        pl.when(to != me)(copy.start)
        pl.when(to == me)(pltpu.make_async_copy(src, dst, recv_sem).start)
    return copy


def _end_move(kind, copy, dst, recv_sem, to, me):
    _landed(dst, recv_sem)
    if kind == 'pair':
        copy.wait_send()
    else:
        pl.when(to != me)(copy.wait_send)


def _all_rows_kernel(n_dev, moves, *refs):
    n = len(moves)
    in_ref, src, out_ref, dst = refs[0], refs[1:1 + n], refs[1 + n], refs[PAIR + n:PAIR + PAIR * n]
    send_sem, recv_sem, m_send, m_recv = refs[PAIR + PAIR * n:]
    me = lax.axis_index(AXIS_NAME)
    peers = [(me + d) % n_dev for d in range(1, n_dev)]
    _meet(peers)
    copies = [_remote(in_ref, out_ref.at[me], send_sem.at[i], recv_sem.at[i], peer) for i, peer in enumerate(peers)]
    for copy in copies:
        copy.start()
    ends = [to for to, _ in _passes(moves, me)]
    moving = [_start_move(moves[i], src[i], dst[i], m_send.at[i], m_recv.at[i], to, me) for i, to in enumerate(ends)]
    out_ref[me] = in_ref[...]
    for copy in copies:
        copy.wait()
    for i, copy in enumerate(moving):
        _end_move(moves[i], copy, dst[i], m_recv.at[i], ends[i], me)


def all_rows(block, n_dev, moved, moves, collective_id):
    n = len(moves)
    dma = pltpu.SemaphoreType.DMA
    vmem, hbm = pl.BlockSpec(memory_space=pltpu.VMEM), pl.BlockSpec(memory_space=pl.ANY)
    res = pl.pallas_call(
        functools.partial(_all_rows_kernel, n_dev, moves),
        out_shape=[jax.ShapeDtypeStruct((n_dev,) + block.shape, block.dtype)] + [jax.ShapeDtypeStruct(v.shape, v.dtype) for v in moved],
        in_specs=[vmem] + [hbm] * n,
        out_specs=[vmem] + [hbm] * n,
        scratch_shapes=[dma((n_dev - 1,)), dma((n_dev - 1,)), dma((n,)), dma((n,))],
        compiler_params=pltpu.CompilerParams(collective_id=collective_id, has_side_effects=True),
        cost_estimate=cost(10_000_000, 1 * MIB),
        name='all_rows',
    )(block, *moved)
    return res[0], res[1:]


def _gather_kernel(pieces, orders, seq, moves, n_arr, *refs):
    n, m = len(moves), len(pieces)
    ins, src, outs, dst = refs[:n_arr], refs[n_arr:n_arr + n], refs[n_arr + n:PAIR * n_arr + n], refs[PAIR * n_arr + n:PAIR * n_arr + PAIR * n]
    own_sem, send_sem, recv_sem, p_send, p_recv, m_send, m_recv = refs[PAIR * n_arr + PAIR * n:]
    me = lax.axis_index(AXIS_NAME)
    at = _Place(me)
    ends = list(_passes(moves, me))

    def slot_of(kc, core, kind):
        return {'device': PAIR * kc + core, 'core': CHIPS * core + kc, 'chip': kc}[kind]

    def part(kc, core, piece):
        arr, r0, rows, kind = pieces[piece]
        slot = slot_of(kc, core, kind)
        return outs[arr].at[slot] if rows == outs[arr].shape[1] else outs[arr].at[slot, pl.ds(r0, rows)]

    def run(u):
        sides = ['a', 'b', 'z+'] + (['z-'] if u else [])
        far = [end for kind, end in zip(moves, ends) if kind != 'pair']
        _meet([at.side(s) for s in sides] + [at.partner], me, far[0] if far else ())
        started, moving = [], []

        def send(src_ref, dst_ref, s_sem, r_sem, dev):
            copy = _remote(src_ref, dst_ref, s_sem, r_sem, dev)
            copy.start()
            started.append(copy)

        count, handed = 0, [0] * m
        for key in [(0, 0, u, i) for i in range(m)] + [_unpack(c) for c in seq[u]]:
            piece = key[3]
            arr, r0, rows, kind = pieces[piece]
            kc = at.chip(key)
            place = part(kc, at.core, piece)
            if _via(u, key, orders) is None:
                ref = ins[arr] if rows == ins[arr].shape[0] else ins[arr].at[pl.ds(r0, rows)]
            else:
                ref = place
                _landed(ref, recv_sem.at[piece, kc])
            for side in _onward(u, key, orders):
                send(ref, place, send_sem.at[count], recv_sem.at[piece, kc], at.side(side))
                count += 1
            if kind != 'chip':
                send(ref, place, p_send.at[piece, handed[piece]], p_recv.at[piece, kc], at.partner)
                handed[piece] += 1
            if key == (0, 0, u, m - 1):
                for i, (to, _) in enumerate(ends):
                    moving.append(_start_move(moves[i], src[i], dst[i], m_send.at[i], m_recv.at[i], to, me))
                own = [pltpu.make_async_copy(ins[i], outs[i].at[slot_of(me // PAIR, at.core, kinds[i])], own_sem.at[i]) for i in range(n_arr)]
                for copy in own:
                    copy.start()
        for piece in range(m):
            if pieces[piece][3] != 'chip':
                for kc in range(CHIPS):
                    _landed(part(kc, 1 - at.core, piece), p_recv.at[piece, kc])
        for i, (to, _) in enumerate(ends):
            _end_move(moves[i], moving[i], dst[i], m_recv.at[i], to, me)
        for copy in own:
            copy.wait()
        for copy in started:
            copy.wait_send()

    kinds = {p[0]: p[3] for p in pieces}
    for u in (0, 1):
        pl.when(at.u == u)(functools.partial(run, u))


def gather_all(blocks, pieces, orders, seq, moved, moves, n_dev, collective_id):
    n, m, n_arr = len(moves), len(pieces), len(blocks)
    dma = pltpu.SemaphoreType.DMA
    vmem, hbm = pl.BlockSpec(memory_space=pltpu.VMEM), pl.BlockSpec(memory_space=pl.ANY)
    nbytes = sum(v.size * v.dtype.itemsize for v in blocks)
    kinds = {p[0]: p[3] for p in pieces}
    res = pl.pallas_call(
        functools.partial(_gather_kernel, tuple(pieces), orders, seq, moves, n_arr),
        out_shape=[jax.ShapeDtypeStruct((n_dev // PAIR if kinds[i] == 'chip' else n_dev,) + v.shape, v.dtype) for i, v in enumerate(blocks)] + [
            jax.ShapeDtypeStruct(v.shape, v.dtype) for v in moved],
        in_specs=[vmem] * n_arr + [hbm] * n,
        out_specs=[hbm] * (n_arr + n),
        scratch_shapes=[dma((n_arr,)), dma((24 * m,)), dma((m, CHIPS)), dma((m, CHIPS)), dma((m, CHIPS)), dma((max(n, 1),)), dma((max(n, 1),))],
        compiler_params=pltpu.CompilerParams(collective_id=collective_id, has_side_effects=True, vmem_limit_bytes=nbytes + (SUB * MIB)),
        cost_estimate=cost(200_000_000, nbytes * 64),
        name='gather_all',
    )(*blocks, *moved)
    return res[:n_arr], res[n_arr:]


def _slots(pieces, orders, seq):
    table, most = {}, [1] * len(pieces)
    for u in (0, 1):
        used = [0] * len(pieces)
        for key in [_unpack(c) for c in reversed(seq[u])] + [(0, 0, u, i) for i in range(len(pieces))]:
            for side in _onward(u, key, orders):
                table[u, key, side] = used[key[3]]
                used[key[3]] += 1
        most = [max(a, b) for a, b in zip(most, used)]
    return table, most


def _scatter_kernel(pieces, orders, seq, n_arr, *refs):
    table, _ = _slots(pieces, orders, seq)
    n = len(pieces)
    n_pair = sum(1 for p in pieces if p[3] != 'chip')
    ins, outs = refs[:n_arr], refs[n_arr:PAIR * n_arr]
    k = PAIR * n_arr
    land, stage, pair = refs[k:k + n], refs[k + n:k + PAIR * n], list(refs[k + PAIR * n:k + PAIR * n + n_pair])
    load_sem, send_sem, recv_sem, d_send, d_recv = refs[k + PAIR * n + n_pair:]
    got = [pair.pop(0) if p[3] != 'chip' else None for p in pieces]
    me = lax.axis_index(AXIS_NAME)
    at, partner_at = _Place(me), _Place(me, swapped=True)

    def rows_of(ref, piece):
        _, r0, rows, _ = pieces[piece]
        return ref if rows == ref.shape[0] else ref.at[pl.ds(r0, rows)]

    def term(piece, kc, core):
        arr, _, rows, kind = pieces[piece]
        if kind == 'rows':
            return ins[arr].at[kc, pl.ds(pl.multiple_of(24 * core, SUB), rows)]
        return rows_of(ins[arr].at[PAIR * kc + core if kind == 'device' else kc], piece)

    def run(u):
        sides = ['a', 'b', 'z+'] + (['z-'] if u else [])
        _meet([at.side(s) for s in sides] + [at.partner])
        keys = [_unpack(c) for c in reversed(seq[u])] + [(0, 0, u, i) for i in range(n)]
        started = []
        given = [0] * n
        for key in keys:
            piece = key[3]
            if pieces[piece][3] != 'chip':
                kc = partner_at.chip(key)
                copy = _remote(term(piece, kc, 1 - at.core), got[piece].at[kc], d_send.at[piece, given[piece]], d_recv.at[piece, kc], at.partner)
                given[piece] += 1
                copy.start()
                started.append(copy)
        adds = [[key for key in keys if key[3] == i and (pieces[i][3] != 'chip' or _onward(u, key, orders))] for i in range(n)]

        def load(piece, j):
            return pltpu.make_async_copy(term(piece, at.chip(adds[piece][j]), at.core), stage[piece].at[j % PAIR], load_sem.at[piece, j % PAIR])

        for i in range(n):
            for j in range(PAIR):
                load(i, j).start()
        done = [0] * n
        count = 0
        for key in keys:
            piece = key[3]
            arr, r0, rows, kind = pieces[piece]
            paired = kind != 'chip'
            kc = at.chip(key)
            children = _onward(u, key, orders)
            if not children and not paired:
                src = term(piece, kc, at.core)
            else:
                j = done[piece]
                done[piece] += 1
                parts = []
                if paired:
                    _landed(got[piece].at[kc], d_recv.at[piece, kc])
                    parts.append(got[piece].at[kc])
                for side in children:
                    slot = table[u, key, side]
                    _landed(land[piece].at[slot], recv_sem.at[piece, slot])
                    parts.append(land[piece].at[slot])
                load(piece, j).wait()
                parts.append(stage[piece].at[j % PAIR])
                root = key[:3] == (0, 0, u)
                src = rows_of(outs[arr], piece) if root else parts[0]
                dtype = ins[arr].dtype
                step = SUB if dtype == F32 else CHIPS

                def body(r, parts=parts, dst=src, step=step, dtype=dtype):
                    some = pl.ds(pl.multiple_of(r * step, step), step)
                    total = parts[0][some, :].astype(F32)
                    for ref in parts[1:]:
                        total = total + ref[some, :].astype(F32)
                    dst[some, :] = total.astype(dtype)

                loop(rows // step, body)
                if j + PAIR < len(adds[piece]):
                    load(piece, j + PAIR).start()
                if root:
                    continue
            side = _via(u, key, orders)
            slot = table[_seen_by_parent(u, key, orders)]
            copy = _remote(src, land[piece].at[slot], send_sem.at[count], recv_sem.at[piece, slot], at.side(side))
            copy.start()
            started.append(copy)
            count += 1
        for copy in started:
            copy.wait_send()

    for u in (0, 1):
        pl.when(at.u == u)(functools.partial(run, u))


def scatter_sum(arrays, pieces, orders, seq, collective_id):
    n_arr, n = len(arrays), len(pieces)
    dma, hbm, vmem = pltpu.SemaphoreType.DMA, pl.BlockSpec(memory_space=pl.ANY), pl.BlockSpec(memory_space=pltpu.VMEM)
    _, most = _slots(pieces, orders, seq)
    shapes = [(rows, arrays[arr].shape[PAIR], arrays[arr].dtype) for arr, _, rows, _ in pieces]
    scratch = [pltpu.VMEM((m, r, c), d) for m, (r, c, d) in zip(most, shapes)]
    scratch += [pltpu.VMEM((PAIR, r, c), d) for r, c, d in shapes]
    scratch += [pltpu.VMEM((CHIPS, r, c), d) for (r, c, d), p in zip(shapes, pieces) if p[3] != 'chip']
    outs = [jax.ShapeDtypeStruct((sum(p[PAIR] for p in pieces if p[0] == i), v.shape[PAIR]), v.dtype) for i, v in enumerate(arrays)]
    nbytes = sum(v.size * v.dtype.itemsize for v in outs) + sum(
        (m + PAIR + CHIPS * int(p[3] != 'chip')) * (-(-r // CHIPS) * CHIPS) * c * d.itemsize for m, (r, c, d), p in zip(most, shapes, pieces))
    scratch += [dma((n, PAIR)), dma((CHIPS * n,)), dma((n, max(most))), dma((n, CHIPS)), dma((n, CHIPS))]
    return pl.pallas_call(
        functools.partial(_scatter_kernel, tuple(pieces), orders, seq, n_arr),
        out_shape=outs,
        in_specs=[hbm] * n_arr,
        out_specs=[vmem] * n_arr,
        scratch_shapes=scratch,
        compiler_params=pltpu.CompilerParams(collective_id=collective_id, has_side_effects=True, vmem_limit_bytes=nbytes + (6 * MIB)),
        cost_estimate=cost(200_000_000, nbytes * 4),
        name='scatter_sum',
    )(*arrays)


def _lookup_kernel(counts, codes, table_ref, out_ref, rows, block, sem):
    b = pl.program_id(0)
    n_col = out_ref.shape[PAIR] // LANES
    n_rows = rows.shape[0] // n_col

    @pl.when(b == 0)
    def _():
        def widen(i):
            for j in range(n_col):
                part = table_ref[pl.ds(pl.multiple_of(i * CHIPS, CHIPS), CHIPS), j * LANES:(j + 1) * LANES].astype(F32)
                line = pl.multiple_of(i * CHIPS * n_col, SUB)
                rows[pl.ds(line + j * SUB, SUB), :] = part[:SUB]
                rows[pl.ds(line + (n_col + j) * SUB, SUB), :] = part[SUB:]
        loop(n_rows // CHIPS, widen)

    seq = out_ref.shape[1]

    def clear(i):
        block[pl.ds(pl.multiple_of(i * SUB * n_col, SUB), SUB * n_col), :] = jnp.zeros((SUB * n_col, LANES), F32)
    loop(seq // SUB, clear)

    def pick(i):
        for t in range(SUB):
            code = codes[b * seq + i * SUB + t]
            block[pl.ds(code >> CHIPS, n_col, stride=SUB), :] = rows[pl.ds(code & 65535, n_col, stride=SUB), :]
    loop((counts[b] + 7) // SUB, pick)

    def narrow(i):
        line = pl.multiple_of(i * CHIPS * n_col, SUB)
        for j in range(n_col):
            part = jnp.concatenate([block[pl.ds(line + j * SUB, SUB), :], block[pl.ds(line + (n_col + j) * SUB, SUB), :]], axis=0)
            out_ref[0, pl.ds(pl.multiple_of(i * CHIPS, CHIPS), CHIPS), j * LANES:(j + 1) * LANES] = part.astype(BF16)
    loop(seq // CHIPS, narrow)


def lookup(table, counts, codes, seq):
    n_rows, dim = table.shape
    n_src = counts.shape[0]
    lines = dim // LANES
    return pl.pallas_call(
        _lookup_kernel,
        grid_spec=pltpu.PrefetchScalarGridSpec(
            num_scalar_prefetch=PAIR,
            grid=(n_src,),
            in_specs=[pl.BlockSpec(memory_space=pltpu.VMEM)],
            out_specs=pl.BlockSpec((1, seq, dim), lambda b, *_: (b, 0, 0)),
            scratch_shapes=[pltpu.VMEM((n_rows * lines, LANES), F32), pltpu.VMEM(((seq + SUB) * lines, LANES), F32), pltpu.SemaphoreType.DMA],
        ),
        out_shape=jax.ShapeDtypeStruct((n_src, seq, dim), table.dtype),
        compiler_params=pltpu.CompilerParams(vmem_limit_bytes=40 * MIB, dimension_semantics=('arbitrary',)),
        cost_estimate=cost(50_000_000, 40 * MIB),
        name='lookup',
    )(counts, codes, table)


def _add_rows_kernel(counts, codes, dx_ref, out_ref, buf, sem):
    n_src, lines, _ = dx_ref.shape
    n_col = 7
    seq = codes.shape[0] // n_src
    cut = lines // 5
    depth = buf.shape[0]

    def fetch(b):
        for i in range(5):
            some = pl.ds(i * cut, cut)
            pltpu.make_async_copy(dx_ref.at[b, some], buf.at[lax.rem(b, depth), some], sem.at[lax.rem(b, depth)]).start()

    for b in range(depth - 1):
        fetch(b)

    def clear(i):
        out_ref[pl.ds(pl.multiple_of(i * CHIPS * n_col, SUB), CHIPS * n_col), :] = jnp.zeros((CHIPS * n_col, LANES), F32)
    loop(out_ref.shape[0] // (CHIPS * n_col), clear)

    def source(b):
        at = lax.rem(b, depth)

        @pl.when(b + depth - 1 < n_src)
        def _():
            fetch(b + depth - 1)
        pltpu.make_async_copy(dx_ref.at[b], buf.at[at], sem.at[at]).wait()

        def add(first, i):
            code = codes[b * seq + first + i]
            line = pl.ds(code & 65535, n_col, stride=SUB)
            out_ref[line, :] = out_ref[line, :] + buf[at, pl.ds(code >> CHIPS, n_col, stride=SUB), :]

        def add_four(i):
            code = [codes[b * seq + i * 4 + t] for t in range(4)]
            line = [c & 65535 for c in code]
            news = [buf[at, pl.ds(c >> CHIPS, n_col, stride=SUB), :] for c in code]
            sums = []
            for t in range(4):
                old = out_ref[pl.ds(line[t], n_col, stride=SUB), :]
                for before in range(t):
                    old = jnp.where(line[t] == line[before], sums[before], old)
                sums.append(old + news[t])
            for t in range(4):
                out_ref[pl.ds(line[t], n_col, stride=SUB), :] = sums[t]
        n = counts[b]
        loop(n // 4, add_four)

        rest = n // 4 * 4
        loop(n - rest, functools.partial(add, rest))
    loop(n_src, source)


def add_rows(dx, counts, codes, n_rows):
    n_src, lines, _ = dx.shape
    return pl.pallas_call(
        _add_rows_kernel,
        grid_spec=pltpu.PrefetchScalarGridSpec(
            num_scalar_prefetch=PAIR,
            grid=(),
            in_specs=[pl.BlockSpec(memory_space=pl.ANY)],
            out_specs=pl.BlockSpec(memory_space=pltpu.VMEM),
            scratch_shapes=[pltpu.VMEM((4, lines, LANES), F32), pltpu.SemaphoreType.DMA((4,))],
        ),
        out_shape=jax.ShapeDtypeStruct((n_rows * 7, LANES), F32),
        compiler_params=pltpu.CompilerParams(vmem_limit_bytes=48 * MIB),
        cost_estimate=cost(50_000_000, 80 * MIB),
        name='add_rows',
    )(counts, codes, dx)


def to_lines(v):
    rows, dim = v.shape
    return v.reshape(rows // SUB, SUB, dim // LANES, LANES).transpose(0, PAIR, 1, 3).reshape(rows * dim // LANES, LANES)


def from_lines(v, dim):
    rows = v.shape[0] * LANES // dim
    return v.reshape(rows // SUB, dim // LANES, SUB, LANES).transpose(0, PAIR, 1, 3).reshape(rows, dim)


def _rms(v):
    return lax.rsqrt(jnp.mean(v * v, axis=-1, keepdims=True) + NORM_EPS)


def _head_mean(v, low):
    first = jnp.sum(jnp.where(low, v, 0.0), axis=-1, keepdims=True)
    second = jnp.sum(jnp.where(low, 0.0, v), axis=-1, keepdims=True)
    return jnp.where(low, first, second) * (1.0 / 64.0)


def _turn(v, cos_t, sin_t, lead):
    return v * cos_t + jnp.where(lead, -pltpu.roll(v, 96, 1), pltpu.roll(v, 32, 1)) * sin_t


def _spread(tile, low, ref):
    first = jnp.where(low, tile, 0.0)
    second = jnp.where(low, 0.0, tile)
    ref[0] = first.astype(BF16)
    ref[1] = pltpu.roll(first, 64, 1).astype(BF16)
    ref[PAIR] = pltpu.roll(second, 64, 1).astype(BF16)
    ref[3] = second.astype(BF16)


def _probs(q, k, block):
    scores = mm_nt(q, k) * 0.125
    n = scores.shape[1]
    row = lax.broadcasted_iota(jnp.int32, scores.shape, 0) + block
    col = lax.broadcasted_iota(jnp.int32, scores.shape, 1)
    scores = jnp.where(row >= col, scores, -1e30)
    e = jnp.exp(scores - jnp.max(scores, axis=-1, keepdims=True))
    return e * (1.0 / jnp.sum(e, axis=-1, keepdims=True))


def _lanes(rows):
    lane = lax.broadcasted_iota(jnp.int32, (rows, LANES), 1)
    return lane < 64, lane % 64 < 32


def _attn_fwd_kernel(x_ref, w_ref, gain_ref, cos_ref, sin_ref, qk_gain_ref, in_ref, raw_ref, q_ref, k_ref, flat_ref, hid_ref, mlp_ref, kk, vv):
    seq, dim = x_ref.shape
    n_q = dim // LANES
    step = LANES
    n_in = raw_ref.shape[1]

    def project(r):
        at = pl.ds(pl.multiple_of(r * step, step), step)
        low, lead = _lanes(step)
        x = x_ref[at, :].astype(F32)
        m1 = (x * _rms(x) * gain_ref[0:1, :]).astype(BF16)
        in_ref[at, :] = m1
        raw = mm(m1, w_ref[0]).astype(BF16)
        raw_ref[at, :] = raw
        cos_t, sin_t = cos_ref[at, :], sin_ref[at, :]
        for t in range(n_q + 1):
            v = raw[:, t * LANES:(t + 1) * LANES].astype(F32)
            v = v * lax.rsqrt(_head_mean(v * v, low) + NORM_EPS)
            which = int(t == n_q)
            v = _turn(v * qk_gain_ref[SUB * which:SUB * which + 1, :], cos_t, sin_t, lead).astype(BF16)
            if which:
                k_ref[at, :] = v
            else:
                q_ref[at, t * LANES:(t + 1) * LANES] = v
    loop(seq // step, project)
    low, _ = _lanes(seq)
    _spread(k_ref[...].astype(F32), low, kk)
    _spread(raw_ref[:, n_in - LANES:].astype(F32), low, vv)

    def heads(t):
        tile = pl.ds(pl.multiple_of(t * LANES, LANES), LANES)
        for b in range(seq // step):
            n = (b + 1) * step
            q = q_ref[b * step:n, tile]
            total = None
            for side in range(PAIR):
                i = PAIR * ((PAIR * t + side) // 7) + side
                p = _probs(q, kk[i, :n, :], b * step).astype(BF16)
                o = mm(p, vv[i, :n, :])
                total = o if total is None else total + o
            flat_ref[b * step:n, tile] = total.astype(BF16)
    loop(n_q, heads)

    def finish(r):
        at = pl.ds(pl.multiple_of(r * step, step), step)
        h = (x_ref[at, :].astype(F32) + mm(flat_ref[at, :], w_ref[1, :, :dim])).astype(BF16)
        hid_ref[at, :] = h
        h = h.astype(F32)
        mlp_ref[at, :] = (h * _rms(h) * gain_ref[SUB:9, :]).astype(BF16)
    loop(seq // step, finish)


def attn_forward(x, w, gains, cos_t, sin_t, qk_gain):
    seq, dim = x.shape
    n_in = w.shape[PAIR]
    vmem = pl.BlockSpec(memory_space=pltpu.VMEM)
    sds = lambda n: jax.ShapeDtypeStruct((seq, n), BF16)
    return pl.pallas_call(
        _attn_fwd_kernel,
        out_shape=[sds(dim), sds(n_in), sds(dim), sds(LANES), sds(dim), sds(dim), sds(dim)],
        in_specs=[vmem] * 6,
        out_specs=[vmem] * 7,
        scratch_shapes=[pltpu.VMEM((4, seq, LANES), BF16), pltpu.VMEM((4, seq, LANES), BF16)],
        compiler_params=pltpu.CompilerParams(vmem_limit_bytes=40 * MIB),
        cost_estimate=cost(4_000_000_000, 12 * MIB, 4_000_000),
        name='attn_forward',
    )(x, w, gains, cos_t, sin_t, qk_gain)


def _attn_bwd_kernel(x_ref, w_ref, gain_ref, cos_ref, sin_ref, qk_gain_ref, in_ref, raw_ref, q_ref, k_ref, flat_ref, hid_ref, dy_ref, part_ref, recv_ref,
                     dx_ref, dw_in_ref, dw_out_ref, kk, vv, dk, dv, gh, hb, do, dqkv):
    seq, dim = x_ref.shape
    n_q = dim // LANES
    step = LANES
    n_blk = seq // step
    n_in = raw_ref.shape[1]

    def norm_back(grad, normed, inv, gain):
        grad = grad * gain
        return inv * (grad - normed * jnp.mean(grad * normed, axis=-1, keepdims=True))

    def hidden(r, total):
        at = pl.ds(pl.multiple_of(r * step, step), step)
        grad = part_ref[at, :] + recv_ref[at, :]
        h = hid_ref[at, :].astype(F32)
        inv = _rms(h)
        normed = h * inv
        g = dy_ref[at, :].astype(F32) + norm_back(grad, normed, inv, gain_ref[SUB:9, :])
        gh[at, :] = g
        g = g.astype(BF16)
        hb[at, :] = g
        do[at, :] = mm_nt(g, w_ref[1, :, :dim]).astype(BF16)
        return total + jnp.sum(grad * normed, axis=0, keepdims=True)
    mlp_gain = lax.fori_loop(0, n_blk, hidden, jnp.zeros((1, dim), F32))

    low_all, _ = _lanes(seq)
    _spread(k_ref[...].astype(F32), low_all, kk)
    _spread(raw_ref[:, n_in - LANES:].astype(F32), low_all, vv)
    dk[...] = jnp.zeros_like(dk)
    dv[...] = jnp.zeros_like(dv)

    def raw_back(grad, tile, at, which, low, lead):
        v = raw_ref[at, tile].astype(F32)
        inv = lax.rsqrt(_head_mean(v * v, low) + NORM_EPS)
        normed = v * inv
        grad = _turn(grad, cos_ref[at, :], -sin_ref[at, :], lead)
        terms = jnp.sum(grad * normed, axis=0, keepdims=True)
        grad = grad * qk_gain_ref[SUB * which:SUB * which + 1, :]
        return inv * (grad - normed * _head_mean(grad * normed, low)), terms

    def heads(t, total):
        tile = pl.ds(pl.multiple_of(t * LANES, LANES), LANES)
        low, lead = _lanes(step)
        for b in range(n_blk):
            n = (b + 1) * step
            at = pl.ds(b * step, step)
            q = q_ref[at, tile]
            g = do[at, tile]
            grad_q = None
            for side in range(PAIR):
                i = PAIR * ((PAIR * t + side) // 7) + side
                k = kk[i, :n, :]
                p = _probs(q, k, b * step)
                dp = mm_nt(g, vv[i, :n, :])
                ds = (p * (dp - jnp.sum(dp * p, axis=-1, keepdims=True)) * 0.125).astype(BF16)
                dv[i, :n, :] = dv[i, :n, :] + mm_tn(p.astype(BF16), g)
                dk[i, :n, :] = dk[i, :n, :] + mm_tn(ds, q)
                part = mm(ds, k)
                grad_q = part if grad_q is None else grad_q + part
            back, terms = raw_back(grad_q, tile, at, 0, low, lead)
            dqkv[at, tile] = back.astype(BF16)
            total = total + terms
        return total
    q_gain = lax.fori_loop(0, n_q, heads, jnp.zeros((1, LANES), F32))

    def keys(r, total):
        at = pl.ds(pl.multiple_of(r * step, step), step)
        low, lead = _lanes(step)

        def join(ref):
            return jnp.where(low, ref[0, at, :] + pltpu.roll(ref[1, at, :], 64, 1), ref[3, at, :] + pltpu.roll(ref[PAIR, at, :], 64, 1))
        back, terms = raw_back(join(dk), pl.ds(dim, LANES), at, 1, low, lead)
        dqkv[at, dim:dim + LANES] = back.astype(BF16)
        dqkv[at, dim + LANES:] = join(dv).astype(BF16)
        return total + terms
    k_gain = lax.fori_loop(0, n_blk, keys, jnp.zeros((1, LANES), F32))

    def inputs(r, total):
        at = pl.ds(pl.multiple_of(r * step, step), step)
        grad = mm_nt(dqkv[at, :], w_ref[0])
        x = x_ref[at, :].astype(F32)
        inv = _rms(x)
        normed = x * inv
        dx_ref[at, :] = gh[at, :] + norm_back(grad, normed, inv, gain_ref[0:1, :])
        return total + jnp.sum(grad * normed, axis=0, keepdims=True)
    attn_gain = lax.fori_loop(0, n_blk, inputs, jnp.zeros((1, dim), F32))

    low, _ = _lanes(SUB)
    row = lax.broadcasted_iota(jnp.int32, (SUB, dim), 0)
    both = jnp.where(low, jnp.broadcast_to(q_gain, (SUB, LANES)) + pltpu.roll(jnp.broadcast_to(q_gain, (SUB, LANES)), 64, 1),
                     jnp.broadcast_to(k_gain, (SUB, LANES)) + pltpu.roll(jnp.broadcast_to(k_gain, (SUB, LANES)), 64, 1))
    dx_ref[seq:, :] = jnp.where(row == 1, jnp.broadcast_to(attn_gain, (SUB, dim)), jnp.where(row == PAIR, jnp.broadcast_to(mlp_gain, (SUB, dim)), 0.0))
    dx_ref[seq:, :LANES] = jnp.where(row[:, :LANES] == 0, both, dx_ref[seq:, :LANES])

    def weights(t):
        tile = pl.ds(pl.multiple_of(t * LANES, LANES), LANES)
        dw_in_ref[tile, :] = mm_tn(in_ref[:, tile], dqkv[...])
        dw_out_ref[tile, :] = mm_tn(flat_ref[:, tile], hb[...])
    loop(n_q, weights)


def attn_backward(x, w, gains, cos_t, sin_t, qk_gain, saved, dy, part, recv):
    seq, dim = x.shape
    n_in = saved[1].shape[1]
    vmem = pl.BlockSpec(memory_space=pltpu.VMEM)
    scr = lambda *s: pltpu.VMEM(s[:-1], s[-1])
    return pl.pallas_call(
        _attn_bwd_kernel,
        out_shape=[jax.ShapeDtypeStruct((seq + SUB, dim), F32), jax.ShapeDtypeStruct((dim, n_in), F32), jax.ShapeDtypeStruct((dim, dim), F32)],
        in_specs=[vmem] * 15,
        out_specs=[vmem] * 3,
        scratch_shapes=[scr(4, seq, LANES, BF16), scr(4, seq, LANES, BF16), scr(4, seq, LANES, F32), scr(4, seq, LANES, F32), scr(seq, dim, F32),
                        scr(seq, dim, BF16), scr(seq, dim, BF16), scr(seq, n_in, BF16)],
        compiler_params=pltpu.CompilerParams(vmem_limit_bytes=44 * MIB),
        cost_estimate=cost(9_000_000_000, 30 * MIB, 4_000_000),
        name='attn_backward',
    )(x, w, gains, cos_t, sin_t, qk_gain, *saved[:6], dy, part, recv)


def _mlp_kernel(x_ref, dy_ref, wgu_ref, wd_ref, y_mine, y_other, din_mine, din_other, dwg_ref, dwu_ref, dwd_ref, xt, wg, wu, wd, act, dg, du, og, ou, od, load_sem, store_sem):
    half, tile = dwd_ref.shape[0], act.shape[1]
    n_tile = -(-half // tile)
    shared = n_tile * tile - half
    seq = y_mine.shape[0]
    step = seq // PAIR

    def start_of(j):
        first = (j == 0).astype(jnp.int32)
        return pl.multiple_of(first * (half - tile) + (1 - first) * (j - 1) * tile, LANES)

    def loads(j):
        at, slot = start_of(j), j % PAIR
        return [pltpu.make_async_copy(wgu_ref.at[:, pl.ds(at, tile)], wg.at[slot], load_sem.at[0, slot]),
                pltpu.make_async_copy(wgu_ref.at[:, pl.ds(pl.multiple_of(half + at, LANES), tile)], wu.at[slot], load_sem.at[1, slot]),
                pltpu.make_async_copy(wd_ref.at[pl.ds(at, tile)], wd.at[slot], load_sem.at[PAIR, slot])]

    def stores(j):
        at, slot = start_of(j), j % PAIR
        return [pltpu.make_async_copy(og.at[slot], dwg_ref.at[:, pl.ds(at, tile)], store_sem.at[0, slot]),
                pltpu.make_async_copy(ou.at[slot], dwu_ref.at[:, pl.ds(at, tile)], store_sem.at[1, slot]),
                pltpu.make_async_copy(od.at[slot], dwd_ref.at[pl.ds(at, tile)], store_sem.at[PAIR, slot])]

    for copy in loads(jnp.int32(0)):
        copy.start()
    for ref in (y_mine, y_other, din_mine, din_other):
        ref[...] = jnp.zeros_like(ref)
    xt[...] = x_ref[...].T

    def columns(j):
        slot = j % PAIR

        @pl.when(j + 1 < n_tile)
        def _():
            for copy in loads(j + 1):
                copy.start()
        for copy in loads(j):
            copy.wait()

        def rows(y_ref, din_ref, first, r):
            at, inner = pl.ds(pl.multiple_of(first + r * step, step), step), pl.ds(pl.multiple_of(r * step, step), step)
            x = x_ref[at, :]
            gate, up, back = mm(x, wg[slot]), mm(x, wu[slot]), mm_nt(dy_ref[at, :], wd[slot])
            counts = lax.broadcasted_iota(jnp.int32, (step, tile), 1) >= (j == 0).astype(jnp.int32) * shared
            up, back = jnp.where(counts, up, 0.0), jnp.where(counts, back, 0.0)
            sig = lax.logistic(gate)
            silu = gate * sig
            a = (silu * up).astype(BF16)
            g = (back * up * sig * (1.0 + gate * (1.0 - sig))).astype(BF16)
            u = (back * silu).astype(BF16)
            act[at, :], dg[at, :], du[at, :] = a, g, u
            y_ref[inner, :] = y_ref[inner, :] + mm(a, wd[slot])
            din_ref[inner, :] = din_ref[inner, :] + mm_nt(g, wg[slot]) + mm_nt(u, wu[slot])
        loop(PAIR, functools.partial(rows, y_mine, din_mine, 0))
        loop(PAIR, functools.partial(rows, y_other, din_other, seq))

        @pl.when(j >= PAIR)
        def _():
            for copy in stores(j - PAIR):
                copy.wait()
        og[slot] = mm(xt[...], dg[...])
        ou[slot] = mm(xt[...], du[...])
        od[slot] = mm_tn(act[...], dy_ref[...])
        for copy in stores(j):
            copy.start()
    loop(n_tile, columns)
    for j in (n_tile - PAIR, n_tile - 1):
        for copy in stores(jnp.int32(j)):
            copy.wait()


def mlp(x, dy, wgu, wd):
    rows, dim = x.shape
    half = wd.shape[0]
    tile = 512
    vmem, hbm = pl.BlockSpec(memory_space=pltpu.VMEM), pl.BlockSpec(memory_space=pl.ANY)
    sds = lambda *s: jax.ShapeDtypeStruct(s, F32)
    dma = pltpu.SemaphoreType.DMA
    bf = lambda *s: pltpu.VMEM(s, BF16)
    f = lambda *s: pltpu.VMEM(s, F32)
    return pl.pallas_call(
        _mlp_kernel,
        out_shape=[sds(rows // PAIR, dim)] * 4 + [sds(dim, half), sds(dim, half), sds(half, dim)],
        in_specs=[vmem, vmem, hbm, hbm],
        out_specs=[vmem] * 4 + [hbm] * 3,
        scratch_shapes=[bf(dim, rows), bf(PAIR, dim, tile), bf(PAIR, dim, tile), bf(PAIR, tile, dim), bf(rows, tile), bf(rows, tile), bf(rows, tile),
                        f(PAIR, dim, tile), f(PAIR, dim, tile), f(PAIR, tile, dim), dma((3, PAIR)), dma((3, PAIR))],
        compiler_params=pltpu.CompilerParams(vmem_limit_bytes=44 * MIB),
        cost_estimate=cost(CHIPS * rows * dim * half, 50 * MIB, rows * half),
        name='mlp',
    )(x, dy, wgu, wd)


def _codes(numbers, count):
    return tuple(numbers[i // 10] // LANES ** (i % 10) % LANES for i in range(count))


ROWS_SEQ = (
    _codes((152348940317322383368, 678662145372396725288, 751232056588892674273, 827272104050806263145, 30857149562), 45),
    _codes((166206088102504171520, 236385149464955200810, 603605329936848293224, 1039985241786269873361, 32734212313), 45),
)
ATTN_SEQ = (
    _codes((370142165075936415752, 972012016723415295145, 1124725529257844811929), 30),
    _codes((961577811093152729088, 751808515438843144256, 1124738970787495025897), 30),
)
GRAD_SEQ = (
    _codes((106232080133048504328, 890654452102748905891, 398002109975241450666, 965054631626560582091, 533961906380267493400, 829000359395158448539, 1143326429365316545848, 31381732460), 75),
    _codes((166206088102504171520, 704158088118449268010, 595216210114064208288, 531741816507597222992, 520744907820250718441, 1005047906396012195259, 910358688114310724092, 32470101362), 75),
)


def solution(mesh):
    n_dev = mesh.shape[AXIS_NAME]
    n_chip = n_dev // PAIR
    pair = [(i, i ^ 1) for i in range(n_dev)]
    groups = [[PAIR * k + c for k in range(n_chip)] for c in range(PAIR)]

    row_spec = P(AXIS_NAME, None)
    vec_spec = P(AXIS_NAME)
    full_spec = P(None)
    batch_spec = P(AXIS_NAME, None, None)
    weight_specs = (vec_spec, row_spec, row_spec, row_spec, full_spec, full_spec, row_spec, vec_spec, row_spec, row_spec, row_spec)

    def swap(v):
        return lax.ppermute(v, AXIS_NAME, pair)

    def gather_group(v):
        return lax.all_gather(v, AXIS_NAME, axis_index_groups=groups, tiled=True)

    def device_step(tokens, positions, table_shard, attn_norm, w_query, w_key, w_value, q_norm, k_norm, w_out, mlp_norm, w_gate, w_up, w_down, dy_out):
        me = lax.axis_index(AXIS_NAME)
        core = lax.rem(me, PAIR)
        seq_len = tokens.shape[1]
        rows_local, model_dim = table_shard.shape
        rows_w, ff = w_gate.shape
        half = ff // PAIR
        nq, nk = w_query.shape[1], w_key.shape[1]
        head_dim = q_norm.shape[0]

        n_in = nq + PAIR * nk

        def gate_up(c):
            return jnp.concatenate([lax.dynamic_slice(w, (0, c * half), (rows_w, half)) for w in (w_gate, w_up)], axis=1)

        def both_cores(mine, other):
            return jnp.where(core == 0, jnp.concatenate([mine, other], axis=0), jnp.concatenate([other, mine], axis=0))
        attn_in = jnp.concatenate([w_query, w_key, w_value], axis=1)
        attn_out = jnp.concatenate([w_out, below(jnp.stack([attn_norm, mlp_norm]), n_in - nq - PAIR).T], axis=1)
        mine_attn, other_attn = jnp.where(core == 0, attn_in, attn_out), jnp.where(core == 0, attn_out, attn_in)
        dy = dy_out.reshape(seq_len, model_dim)
        all_tokens, (down_block, recv_gu, recv_attn, dy_other) = all_rows(
            below(tokens.reshape(-1, LANES), 4), n_dev, [w_down, gate_up(1 - core), other_attn, dy], ('use', 'pair', 'pair', 'pair'), 0)
        wgu = gather_group(both_cores(gate_up(core), recv_gu))

        (attn_w, wd), _ = gather_all([both_cores(mine_attn, recv_attn), down_block], [(0, 0, PAIR * rows_w, 'core'), (1, 0, down_block.shape[0], 'chip')],
                                     ('bza', 'zba'), ATTN_SEQ, [], (), n_dev, 1)
        attn_w = attn_w.reshape(PAIR, model_dim, n_in)
        wd = wd.reshape(-1, model_dim)

        all_ids = all_tokens[:, :seq_len // LANES].reshape(-1)
        local_ids = all_ids - me * rows_local
        is_owner = (local_ids >= 0) & (local_ids < rows_local)
        own = is_owner.reshape(n_dev, seq_len)
        slot = jnp.arange(seq_len, dtype=jnp.int32)
        upto = (slot[:, None] <= slot[None, :]).astype(BF16)
        rank = jnp.where(own, mm(own.astype(BF16), upto).astype(jnp.int32) - 1, -1)
        counts = jnp.sum(own.astype(jnp.int32), axis=1)
        lines = model_dim // LANES
        line = lambda row: row // SUB * (SUB * lines) + row % SUB
        code = line(slot)[None] * 65536 + line(jnp.where(own, local_ids.reshape(n_dev, seq_len), 0))
        codes = jnp.sum(jnp.where(rank[:, :, None] == slot, code[:, :, None], 0), axis=1)
        codes = jnp.where(slot[None] < counts[:, None], codes, seq_len * lines * 65536).reshape(-1)
        picked = lookup(table_shard, counts, codes, seq_len)
        x_emb = scatter_sum([picked], [(0, 0, 192, 'device'), (0, 192, 208, 'device'), (0, 400, 112, 'device')], ('zba', 'zba', 'baz'), ROWS_SEQ, PAIR)[0]

        dy2 = jnp.concatenate([dy, dy_other], axis=0)

        gains = below(jnp.repeat(attn_w[1, :, nq:nq + PAIR].astype(F32).T, SUB, axis=0), SUB)
        qk_gain = jnp.repeat(jnp.stack([jnp.tile(q_norm, PAIR), jnp.tile(k_norm, PAIR)]).astype(F32), SUB, axis=0)

        inv_freq = jnp.exp((jnp.arange(LANES) % (head_dim // PAIR)).astype(F32) * (-2.0 * math.log(ROPE_THETA) / head_dim))
        angles = positions.reshape(seq_len, 1).astype(F32) * inv_freq
        cos_t, sin_t = jnp.cos(angles), jnp.sin(angles)
        saved = attn_forward(x_emb, attn_w, gains, cos_t, sin_t, qk_gain)
        hidden, mlp_in = saved[5:]

        mlp2 = jnp.concatenate([mlp_in, swap(mlp_in)], axis=0)
        y_mine, y_other, grad_in, grad_other, grad_w_gate, grad_w_up, grad_w_down = mlp(mlp2, dy2, wgu, wd)
        grad_recv = swap(grad_other)
        layer_out = (hidden.astype(F32) + (y_mine + swap(y_other))).astype(BF16)

        dx_block, grad_w_in, grad_w_out = attn_backward(x_emb, attn_w, gains, cos_t, sin_t, qk_gain, saved, dy, grad_in, grad_recv)

        by_chip = [u.reshape(n_chip, -1, u.shape[1]) for u in (grad_w_down, grad_w_gate, grad_w_up, grad_w_in, grad_w_out)]
        down_rows, gate_shard, up_shard, in_shard, out_shard = scatter_sum(
            by_chip, [(i, 0, u.shape[1], 'chip') for i, u in enumerate(by_chip[:3])] + [(i, 0, 32, 'rows') for i in (3, 4)], ('bza', 'zba', 'zba', 'baz', 'baz'), GRAD_SEQ, 3)

        chip_rows = jnp.concatenate([gate_shard, up_shard], axis=1)
        mine = lax.dynamic_slice(chip_rows, (core * rows_w, 0), (rows_w, chip_rows.shape[1]))
        give = lax.dynamic_slice(chip_rows, ((1 - core) * rows_w, 0), (rows_w, chip_rows.shape[1]))
        (all_dx,), (down_shard, recv) = gather_all(
            [to_lines(dx_block)], [(0, 0, 200 * lines, 'device'), (0, 200 * lines, 200 * lines, 'device'), (0, 400 * lines, 120 * lines, 'device')],
            ('zba', 'zba', 'baz'), ROWS_SEQ, [down_rows, give], ('store', 'pair'), n_dev, 4)
        d_table = from_lines(add_rows(all_dx, counts, codes, rows_local), model_dim)
        gains_grad = from_lines(jnp.sum(all_dx[:, seq_len * lines:], axis=0), model_dim)
        qk = gains_grad[0]
        d_attn_norm, d_mlp_norm = (lax.dynamic_slice(gains_grad[i], (me * rows_w,), (rows_w,)) for i in (1, PAIR))
        low = jnp.where(core == 0, mine, recv)
        high = jnp.where(core == 0, recv, mine)
        d_gate = jnp.concatenate([low[:, :half], high[:, :half]], axis=1)
        d_up = jnp.concatenate([low[:, half:ff], high[:, half:ff]], axis=1)
        in_rows = lax.dynamic_slice(in_shard, (core * (rows_w - 24), 0), (rows_w, n_in))
        d_query, d_key, d_value = in_rows[:, :nq], in_rows[:, nq:nq + nk], in_rows[:, nq + nk:]
        d_out = lax.dynamic_slice(out_shard, (core * (rows_w - 24), 0), (rows_w, nq))
        return (layer_out.reshape(1, seq_len, model_dim), d_table, d_attn_norm, d_query, d_key, d_value, qk[:head_dim], qk[head_dim:PAIR * head_dim], d_out, d_mlp_norm, d_gate, d_up, down_shard)

    return jax.shard_map(device_step, mesh=mesh, in_specs=(row_spec, row_spec, row_spec) + weight_specs + (batch_spec,), out_specs=(batch_spec, row_spec) + weight_specs, check_vma=False)
```

```python
import functools
import math
import jax
import jax.numpy as jnp
from jax import lax
from jax.experimental import pallas as pl
from jax.experimental.pallas import tpu as pltpu
from jax.sharding import PartitionSpec as P

NORM_EPS = 1e-6
ROPE_THETA = 1.0e6
AXIS_NAME = 'fsdp'
F32 = jnp.float32
BF16 = jnp.bfloat16
MESH = pl.DeviceIdType.MESH
LANES, HEAD, CHIPS, SUB, QUAD, PAIR, MIB = 128, 64, 16, 8, 4, 2, 1 << 20


def mm(a, b):
    return lax.dot_general(a, b, (((1,), (0,)), ((), ())), preferred_element_type=F32)


def mm_nt(a, b):
    return lax.dot_general(a, b, (((1,), (1,)), ((), ())), preferred_element_type=F32)


def mm_tn(a, b):
    return lax.dot_general(a, b, (((0,), (0,)), ((), ())), preferred_element_type=F32)


def cost(flops, nbytes, transcendentals=0):
    return pl.CostEstimate(flops=flops, bytes_accessed=nbytes, transcendentals=transcendentals)


def below(v, rows):
    return jnp.pad(v, ((0, rows), (0, 0)))


def loop(count, body):
    def step(i, carry):
        body(i)
        return carry
    lax.fori_loop(0, count, step, 0)


def _unpack(code):
    return code // HEAD, code // 32 % PAIR, code // SUB % QUAD, code % SUB


def _via(u, key, orders):
    da, db, p, piece = key
    last = None
    for axis in orders[piece]:
        if axis == 'a' and da or axis == 'b' and db:
            last = axis
        if axis == 'z' and p != u:
            last = 'z+' if p > u else 'z-'
    return last


def _onward(u, key, orders):
    order = orders[key[3]]
    via = _via(u, key, orders)
    left = order if via is None else order[order.index(via[0]) + 1:]
    out = []
    if u < 3 and (via == 'z-' or 'z' in left):
        out.append('z+')
    if u > 0 and (via == 'z+' or 'z' in left):
        out.append('z-')
    return out + [axis for axis in 'ba' if axis in left]


def _seen_by_parent(u, key, orders):
    da, db, p, piece = key
    via = _via(u, key, orders)
    if via == 'a':
        return u, (0, db, p, piece), 'a'
    if via == 'b':
        return u, (da, 0, p, piece), 'b'
    if via == 'z-':
        return u - 1, key, 'z+'
    if u == 0:
        return 1, key, 'z-'
    return 1, (da, db, 3 - p, piece), 'z+'


class _Place:
    def __init__(self, me, swapped=False):
        self.me = me
        self.core = me % PAIR
        x, y, self.z = (me // PAIR) % PAIR, (me // QUAD) % PAIR, me // SUB
        other = 1 - self.core if swapped else self.core
        self.a = y * (1 - other) + x * other
        self.b = x * (1 - other) + y * other
        self.a_str, self.b_str = QUAD - PAIR * other, PAIR + PAIR * other
        self.far = self.z // PAIR
        self.u = 3 * self.far + (1 - PAIR * self.far) * self.z
        self.partner = me + 1 - PAIR * self.core

    def chip(self, key):
        da, db, p = key[:3]
        a = self.a + da * (1 - PAIR * self.a)
        b = self.b + db * (1 - PAIR * self.b)
        z = 3 * self.far + (1 - PAIR * self.far) * p
        return (SUB * z + a * self.a_str + b * self.b_str) // PAIR

    def side(self, name):
        if name == 'a':
            return self.me + (1 - PAIR * self.a) * self.a_str
        if name == 'b':
            return self.me + (1 - PAIR * self.b) * self.b_str
        return self.me + SUB * (1 - PAIR * self.far) * (1 if name == 'z+' else -1)


def _remote(src, dst, send_sem, recv_sem, dev):
    return pltpu.make_async_remote_copy(src_ref=src, dst_ref=dst, send_sem=send_sem, recv_sem=recv_sem, device_id=(dev,), device_id_type=MESH)


def _meet(peers, me=None, ends=()):
    sem = pltpu.get_barrier_semaphore()

    def meet(everyone):
        for peer in everyone:
            pl.semaphore_signal(sem, inc=1, device_id=(peer,), device_id_type=MESH)
        pl.semaphore_wait(sem, len(everyone))

    if not ends:
        meet(peers)
        return
    to, frm = ends
    pl.when(to != me)(lambda: meet(peers + [to, frm]))
    pl.when(to == me)(lambda: meet(peers))


def _landed(ref, sem):
    pltpu.make_async_copy(ref, ref, sem).wait()


def _passes(moves, me):
    for kind in moves:
        if kind == 'pair':
            other = me + 1 - PAIR * (me % PAIR)
            yield other, other
        elif kind == 'use':
            yield PAIR * (me % CHIPS) + me // CHIPS, CHIPS * (me % PAIR) + me // PAIR
        else:
            yield CHIPS * (me % PAIR) + me // PAIR, PAIR * (me % CHIPS) + me // CHIPS


def _start_move(kind, src, dst, send_sem, recv_sem, to, me):
    copy = _remote(src, dst, send_sem, recv_sem, to)
    if kind == 'pair':
        copy.start()
    else:
        pl.when(to != me)(copy.start)
        pl.when(to == me)(pltpu.make_async_copy(src, dst, recv_sem).start)
    return copy


def _end_move(kind, copy, dst, recv_sem, to, me):
    _landed(dst, recv_sem)
    if kind == 'pair':
        copy.wait_send()
    else:
        pl.when(to != me)(copy.wait_send)


def _all_rows_kernel(n_dev, moves, *refs):
    n = len(moves)
    in_ref, src, out_ref, dst = refs[0], refs[1:1 + n], refs[1 + n], refs[PAIR + n:PAIR + PAIR * n]
    send_sem, recv_sem, m_send, m_recv = refs[PAIR + PAIR * n:]
    me = lax.axis_index(AXIS_NAME)
    peers = [(me + d) % n_dev for d in range(1, n_dev)]
    _meet(peers)
    copies = [_remote(in_ref, out_ref.at[me], send_sem.at[i], recv_sem.at[i], peer) for i, peer in enumerate(peers)]
    for copy in copies:
        copy.start()
    ends = [to for to, _ in _passes(moves, me)]
    moving = [_start_move(moves[i], src[i], dst[i], m_send.at[i], m_recv.at[i], to, me) for i, to in enumerate(ends)]
    out_ref[me] = in_ref[...]
    for copy in copies:
        copy.wait()
    for i, copy in enumerate(moving):
        _end_move(moves[i], copy, dst[i], m_recv.at[i], ends[i], me)


def all_rows(block, n_dev, moved, moves, collective_id):
    n = len(moves)
    dma = pltpu.SemaphoreType.DMA
    vmem, hbm = pl.BlockSpec(memory_space=pltpu.VMEM), pl.BlockSpec(memory_space=pl.ANY)
    res = pl.pallas_call(
        functools.partial(_all_rows_kernel, n_dev, moves),
        out_shape=[jax.ShapeDtypeStruct((n_dev,) + block.shape, block.dtype)] + [jax.ShapeDtypeStruct(v.shape, v.dtype) for v in moved],
        in_specs=[vmem] + [hbm] * n,
        out_specs=[vmem] + [hbm] * n,
        scratch_shapes=[dma((n_dev - 1,)), dma((n_dev - 1,)), dma((n,)), dma((n,))],
        compiler_params=pltpu.CompilerParams(collective_id=collective_id, has_side_effects=True),
        cost_estimate=cost(10_000_000, 1 * MIB),
        name='all_rows',
    )(block, *moved)
    return res[0], res[1:]


def _gather_kernel(pieces, orders, seq, moves, n_arr, *refs):
    n, m = len(moves), len(pieces)
    ins, src, outs, dst = refs[:n_arr], refs[n_arr:n_arr + n], refs[n_arr + n:PAIR * n_arr + n], refs[PAIR * n_arr + n:PAIR * n_arr + PAIR * n]
    own_sem, send_sem, recv_sem, p_send, p_recv, m_send, m_recv = refs[PAIR * n_arr + PAIR * n:]
    me = lax.axis_index(AXIS_NAME)
    at = _Place(me)
    ends = list(_passes(moves, me))

    def slot_of(kc, core, kind):
        return {'device': PAIR * kc + core, 'core': CHIPS * core + kc, 'chip': kc}[kind]

    def part(kc, core, piece):
        arr, r0, rows, kind = pieces[piece]
        slot = slot_of(kc, core, kind)
        return outs[arr].at[slot] if rows == outs[arr].shape[1] else outs[arr].at[slot, pl.ds(r0, rows)]

    def run(u):
        sides = ['a', 'b', 'z+'] + (['z-'] if u else [])
        far = [end for kind, end in zip(moves, ends) if kind != 'pair']
        _meet([at.side(s) for s in sides] + [at.partner], me, far[0] if far else ())
        started, moving = [], []

        def send(src_ref, dst_ref, s_sem, r_sem, dev):
            copy = _remote(src_ref, dst_ref, s_sem, r_sem, dev)
            copy.start()
            started.append(copy)

        count, handed = 0, [0] * m
        for key in [(0, 0, u, i) for i in range(m)] + [_unpack(c) for c in seq[u]]:
            piece = key[3]
            arr, r0, rows, kind = pieces[piece]
            kc = at.chip(key)
            place = part(kc, at.core, piece)
            if _via(u, key, orders) is None:
                ref = ins[arr] if rows == ins[arr].shape[0] else ins[arr].at[pl.ds(r0, rows)]
            else:
                ref = place
                _landed(ref, recv_sem.at[piece, kc])
            for side in _onward(u, key, orders):
                send(ref, place, send_sem.at[count], recv_sem.at[piece, kc], at.side(side))
                count += 1
            if kind != 'chip':
                send(ref, place, p_send.at[piece, handed[piece]], p_recv.at[piece, kc], at.partner)
                handed[piece] += 1
            if key == (0, 0, u, m - 1):
                for i, (to, _) in enumerate(ends):
                    moving.append(_start_move(moves[i], src[i], dst[i], m_send.at[i], m_recv.at[i], to, me))
                own = [pltpu.make_async_copy(ins[i], outs[i].at[slot_of(me // PAIR, at.core, kinds[i])], own_sem.at[i]) for i in range(n_arr)]
                for copy in own:
                    copy.start()
        for piece in range(m):
            if pieces[piece][3] != 'chip':
                for kc in range(CHIPS):
                    _landed(part(kc, 1 - at.core, piece), p_recv.at[piece, kc])
        for i, (to, _) in enumerate(ends):
            _end_move(moves[i], moving[i], dst[i], m_recv.at[i], to, me)
        for copy in own:
            copy.wait()
        for copy in started:
            copy.wait_send()

    kinds = {p[0]: p[3] for p in pieces}
    for u in (0, 1):
        pl.when(at.u == u)(functools.partial(run, u))


def gather_all(blocks, pieces, orders, seq, moved, moves, n_dev, collective_id):
    n, m, n_arr = len(moves), len(pieces), len(blocks)
    dma = pltpu.SemaphoreType.DMA
    vmem, hbm = pl.BlockSpec(memory_space=pltpu.VMEM), pl.BlockSpec(memory_space=pl.ANY)
    nbytes = sum(v.size * v.dtype.itemsize for v in blocks)
    kinds = {p[0]: p[3] for p in pieces}
    res = pl.pallas_call(
        functools.partial(_gather_kernel, tuple(pieces), orders, seq, moves, n_arr),
        out_shape=[jax.ShapeDtypeStruct((n_dev // PAIR if kinds[i] == 'chip' else n_dev,) + v.shape, v.dtype) for i, v in enumerate(blocks)] + [
            jax.ShapeDtypeStruct(v.shape, v.dtype) for v in moved],
        in_specs=[vmem] * n_arr + [hbm] * n,
        out_specs=[hbm] * (n_arr + n),
        scratch_shapes=[dma((n_arr,)), dma((24 * m,)), dma((m, CHIPS)), dma((m, CHIPS)), dma((m, CHIPS)), dma((max(n, 1),)), dma((max(n, 1),))],
        compiler_params=pltpu.CompilerParams(collective_id=collective_id, has_side_effects=True, vmem_limit_bytes=nbytes + (SUB * MIB)),
        cost_estimate=cost(200_000_000, nbytes * HEAD),
        name='gather_all',
    )(*blocks, *moved)
    return res[:n_arr], res[n_arr:]


def _slots(pieces, orders, seq):
    table, most = {}, [1] * len(pieces)
    for u in (0, 1):
        used = [0] * len(pieces)
        for key in [_unpack(c) for c in reversed(seq[u])] + [(0, 0, u, i) for i in range(len(pieces))]:
            for side in _onward(u, key, orders):
                table[u, key, side] = used[key[3]]
                used[key[3]] += 1
        most = [max(a, b) for a, b in zip(most, used)]
    return table, most


def _order(u, seq, orders, n, n_late, lead, after):
    keys = [_unpack(c) for c in reversed(seq[u])]
    roots = [(0, 0, u, i) for i in range(n)]
    if not n_late:
        return keys + roots, [], []
    late = [key for key in keys if key[3] >= n - n_late]
    rest = [key for key in keys if key not in late]
    first = [key for key in rest if not _onward(u, key, orders)][:lead]
    rest = [key for key in rest if key not in first]
    sums = [key for key in rest if _onward(u, key, orders)]
    parts = [[sums.pop(0)] if some else [] for some in after]
    rest = [key for key in rest if [key] not in parts]
    out, share = [], 0
    rate = len(late) / (len(rest) * 0.85)
    for key in rest:
        out.append(key)
        share += rate
        while share >= 1 and late:
            out.append(late.pop(0))
            share -= 1
    return first, parts, out + late + roots


def _scatter_kernel(pieces, orders, seq, n_arr, work, *refs):
    table, _ = _slots(pieces, orders, seq)
    n = len(pieces)
    paired = [p[3] != 'chip' for p in pieces]
    n_late, n_in, n_out, n_scr = (work.arrays, work.inputs, work.outputs, work.scratches) if work else (0, 0, 0, 0)
    cut = lambda count: [refs_left.pop(0) for _ in range(count)]
    refs_left = list(refs)
    ins, work_in, outs, made, work_out = cut(n_arr - n_late), cut(n_in), cut(n_arr), cut(n_late), cut(n_out)
    ins += made
    land, stage, pair = cut(n), cut(n), cut(sum(paired))
    load_sem, send_sem, recv_sem, d_send, d_recv, out_sem = cut(6)
    got = [pair.pop(0) if p else None for p in paired]
    me = lax.axis_index(AXIS_NAME)
    at, partner_at = _Place(me), _Place(me, swapped=True)
    early = [i for i in range(n) if pieces[i][0] < n_arr - n_late]
    late = [i for i in range(n) if i not in early]

    def rows_of(ref, piece):
        _, r0, rows, _ = pieces[piece]
        return ref if rows == ref.shape[0] else ref.at[pl.ds(r0, rows)]

    def term(piece, kc, core):
        arr, _, rows, kind = pieces[piece]
        if kind == 'rows':
            return ins[arr].at[pl.ds(pl.multiple_of(ins[arr].shape[0] // CHIPS * kc + 24 * core, SUB), rows)]
        return rows_of(ins[arr].at[PAIR * kc + core if kind == 'device' else kc], piece)

    class Node:
        def __init__(self, u):
            self.u = u
            self.first, self.parts, self.rest = _order(u, seq, orders, n, len(late), 15, work.after if work else ())
            self.keys = self.first + sum(self.parts, []) + self.rest
            self.adds = [[key for key in self.keys if key[3] == i and (paired[i] or _onward(u, key, orders))] for i in range(n)]
            self.sent, self.given, self.done = [], [0] * n, [0] * n

        def meet(self):
            _meet([at.side(s) for s in ['a', 'b', 'z+'] + (['z-'] if self.u else [])] + [at.partner])

        def load(self, piece, j):
            return pltpu.make_async_copy(term(piece, at.chip(self.adds[piece][j]), at.core), stage[piece].at[j % PAIR], load_sem.at[piece, j % PAIR])

        def ready(self, some):
            for key in self.keys:
                piece = key[3]
                if paired[piece] and piece in some:
                    kc = partner_at.chip(key)
                    copy = _remote(term(piece, kc, 1 - at.core), got[piece].at[kc], d_send.at[piece, self.given[piece]], d_recv.at[piece, kc], at.partner)
                    self.given[piece] += 1
                    copy.start()
            for piece in some:
                for j in range(PAIR):
                    self.load(piece, j).start()

        def step(self, key):
            u, piece = self.u, key[3]
            arr, _, rows, _ = pieces[piece]
            kc = at.chip(key)
            root = key[:3] == (0, 0, u)
            children = _onward(u, key, orders)
            if not children and not paired[piece]:
                src = term(piece, kc, at.core)
            else:
                j = self.done[piece]
                self.done[piece] += 1
                parts = []
                if paired[piece]:
                    _landed(got[piece].at[kc], d_recv.at[piece, kc])
                    parts.append(got[piece].at[kc])
                for side in children:
                    slot = table[u, key, side]
                    _landed(land[piece].at[slot], recv_sem.at[piece, slot])
                    parts.append(land[piece].at[slot])
                self.load(piece, j).wait()
                parts.append(stage[piece].at[j % PAIR])
                src = parts[0]
                dtype = ins[arr].dtype
                size = SUB if dtype == F32 else CHIPS

                def add(r):
                    some = pl.ds(pl.multiple_of(r * size, size), size)
                    total = parts[0][some, :].astype(F32)
                    for ref in parts[1:]:
                        total = total + ref[some, :].astype(F32)
                    src[some, :] = total.astype(dtype)
                loop(rows // size, add)
                if j + PAIR < len(self.adds[piece]):
                    self.load(piece, j + PAIR).start()
            if root:
                copy = pltpu.make_async_copy(src, rows_of(outs[arr], piece), out_sem.at[piece])
            else:
                slot = table[_seen_by_parent(u, key, orders)]
                copy = _remote(src, land[piece].at[slot], send_sem.at[len(self.sent)], recv_sem.at[piece, slot], at.side(_via(u, key, orders)))
                self.sent.append(piece)
            copy.start()

        def finish(self):
            def sent(ref, sem):
                _remote(ref, ref, sem, sem, at.partner).wait_send()
            for i, piece in enumerate(self.sent):
                sent(land[piece].at[0], send_sem.at[i])
            for piece in range(n):
                for i in range(self.given[piece]):
                    sent(got[piece].at[0], d_send.at[piece, i])
                out = rows_of(outs[pieces[piece][0]], piece)
                _landed(out, out_sem.at[piece])

    nodes = [Node(u) for u in (0, 1)]

    def each(do):
        for node in nodes:
            pl.when(at.u == node.u)(functools.partial(do, node))

    def begin(node):
        node.meet()
        node.ready(early)
        for key in node.first:
            node.step(key)

    def end(node):
        node.ready(late)
        for key in node.rest:
            node.step(key)
        node.finish()
    each(begin)
    if work:
        def between(part, when=None):
            def steps(node):
                for key in node.parts[part]:
                    node.step(key)
            if when is None:
                each(steps)
            else:
                pl.when(when)(lambda: each(steps))
        work.run(work_in, made, work_out, refs_left, between)
    each(end)


def scatter_sum(arrays, pieces, orders, seq, collective_id, work=None):
    late = list(work.makes) if work else []
    n_arr, n = len(arrays) + len(late), len(pieces)
    dma, hbm, vmem = pltpu.SemaphoreType.DMA, pl.BlockSpec(memory_space=pl.ANY), pl.BlockSpec(memory_space=pltpu.VMEM)
    _, most = _slots(pieces, orders, seq)
    every = list(arrays) + late
    shapes = [(rows, every[arr].shape[-1], every[arr].dtype) for arr, _, rows, _ in pieces]
    scratch = [pltpu.VMEM((m, r, c), d) for m, (r, c, d) in zip(most, shapes)]
    scratch += [pltpu.VMEM((PAIR, r, c), d) for r, c, d in shapes]
    scratch += [pltpu.VMEM((CHIPS, r, c), d) for (r, c, d), p in zip(shapes, pieces) if p[3] != 'chip']
    outs = [jax.ShapeDtypeStruct((sum(p[PAIR] for p in pieces if p[0] == i), v.shape[-1]), v.dtype) for i, v in enumerate(every)]
    nbytes = sum((m + PAIR + CHIPS * int(p[3] != 'chip')) * (-(-r // CHIPS) * CHIPS) * c * d.itemsize for m, (r, c, d), p in zip(most, shapes, pieces))
    scratch += [dma((n, PAIR)), dma((CHIPS * n,)), dma((n, max(most))), dma((n, CHIPS)), dma((n, CHIPS)), dma((n,))]
    work_in = work.operands if work else []
    work_out = work.results if work else []
    limit = min(nbytes + (6 * MIB) + (work.nbytes if work else 0), 67043328)
    return pl.pallas_call(
        functools.partial(_scatter_kernel, tuple(pieces), orders, seq, n_arr, work),
        out_shape=outs + late + work_out,
        in_specs=[hbm] * len(arrays) + [vmem if near else hbm for _, near in work_in],
        out_specs=[hbm] * (n_arr + len(late)) + [vmem] * len(work_out),
        scratch_shapes=scratch + (work.scratch if work else []),
        compiler_params=pltpu.CompilerParams(collective_id=collective_id, has_side_effects=True, vmem_limit_bytes=limit),
        cost_estimate=cost(200_000_000, nbytes * QUAD),
        name='scatter_sum',
    )(*arrays, *[v for v, _ in work_in])


def _lookup_kernel(counts, codes, table_ref, out_ref, rows, block, sem):
    b = pl.program_id(0)
    n_col = out_ref.shape[PAIR] // LANES
    n_rows = rows.shape[0] // n_col

    @pl.when(b == 0)
    def _():
        def widen(i):
            for j in range(n_col):
                part = table_ref[pl.ds(pl.multiple_of(i * CHIPS, CHIPS), CHIPS), j * LANES:(j + 1) * LANES].astype(F32)
                line = pl.multiple_of(i * CHIPS * n_col, SUB)
                rows[pl.ds(line + j * SUB, SUB), :] = part[:SUB]
                rows[pl.ds(line + (n_col + j) * SUB, SUB), :] = part[SUB:]
        loop(n_rows // CHIPS, widen)

    seq = out_ref.shape[1]

    def clear(i):
        block[pl.ds(pl.multiple_of(i * SUB * n_col, SUB), SUB * n_col), :] = jnp.zeros((SUB * n_col, LANES), F32)
    loop(seq // SUB, clear)

    def pick(i):
        for t in range(SUB):
            code = codes[b * seq + i * SUB + t]
            block[pl.ds(code >> CHIPS, n_col, stride=SUB), :] = rows[pl.ds(code & 65535, n_col, stride=SUB), :]
    loop((counts[b] + 7) // SUB, pick)

    def narrow(i):
        line = pl.multiple_of(i * CHIPS * n_col, SUB)
        for j in range(n_col):
            part = jnp.concatenate([block[pl.ds(line + j * SUB, SUB), :], block[pl.ds(line + (n_col + j) * SUB, SUB), :]], axis=0)
            out_ref[0, pl.ds(pl.multiple_of(i * CHIPS, CHIPS), CHIPS), j * LANES:(j + 1) * LANES] = part.astype(BF16)
    loop(seq // CHIPS, narrow)


def lookup(table, counts, codes, seq):
    n_rows, dim = table.shape
    n_src = counts.shape[0]
    lines = dim // LANES
    return pl.pallas_call(
        _lookup_kernel,
        grid_spec=pltpu.PrefetchScalarGridSpec(
            num_scalar_prefetch=PAIR,
            grid=(n_src,),
            in_specs=[pl.BlockSpec(memory_space=pltpu.VMEM)],
            out_specs=pl.BlockSpec((1, seq, dim), lambda b, *_: (b, 0, 0)),
            scratch_shapes=[pltpu.VMEM((n_rows * lines, LANES), F32), pltpu.VMEM(((seq + SUB) * lines, LANES), F32), pltpu.SemaphoreType.DMA],
        ),
        out_shape=jax.ShapeDtypeStruct((n_src, seq, dim), table.dtype),
        compiler_params=pltpu.CompilerParams(vmem_limit_bytes=40 * MIB, dimension_semantics=('arbitrary',)),
        cost_estimate=cost(50_000_000, 40 * MIB),
        name='lookup',
    )(counts, codes, table)


def _add_rows_kernel(counts, codes, dx_ref, out_ref, buf, sem):
    n_src, lines, _ = dx_ref.shape
    n_col = 7
    seq = codes.shape[0] // n_src
    cut = lines // 5
    depth = buf.shape[0]

    def fetch(b):
        for i in range(5):
            some = pl.ds(i * cut, cut)
            pltpu.make_async_copy(dx_ref.at[b, some], buf.at[lax.rem(b, depth), some], sem.at[lax.rem(b, depth)]).start()

    for b in range(depth - 1):
        fetch(b)

    def clear(i):
        out_ref[pl.ds(pl.multiple_of(i * CHIPS * n_col, SUB), CHIPS * n_col), :] = jnp.zeros((CHIPS * n_col, LANES), F32)
    loop(out_ref.shape[0] // (CHIPS * n_col), clear)

    def source(b):
        at = lax.rem(b, depth)

        @pl.when(b + depth - 1 < n_src)
        def _():
            fetch(b + depth - 1)
        pltpu.make_async_copy(dx_ref.at[b], buf.at[at], sem.at[at]).wait()

        def add(first, i):
            code = codes[b * seq + first + i]
            line = pl.ds(code & 65535, n_col, stride=SUB)
            out_ref[line, :] = out_ref[line, :] + buf[at, pl.ds(code >> CHIPS, n_col, stride=SUB), :]

        def add_four(i):
            code = [codes[b * seq + i * QUAD + t] for t in range(QUAD)]
            line = [c & 65535 for c in code]
            news = [buf[at, pl.ds(c >> CHIPS, n_col, stride=SUB), :] for c in code]
            sums = []
            for t in range(QUAD):
                old = out_ref[pl.ds(line[t], n_col, stride=SUB), :]
                for before in range(t):
                    old = jnp.where(line[t] == line[before], sums[before], old)
                sums.append(old + news[t])
            for t in range(QUAD):
                out_ref[pl.ds(line[t], n_col, stride=SUB), :] = sums[t]
        n = counts[b]
        loop(n // QUAD, add_four)

        rest = n // QUAD * QUAD
        loop(n - rest, functools.partial(add, rest))
    loop(n_src, source)


def add_rows(dx, counts, codes, n_rows):
    n_src, lines, _ = dx.shape
    return pl.pallas_call(
        _add_rows_kernel,
        grid_spec=pltpu.PrefetchScalarGridSpec(
            num_scalar_prefetch=PAIR,
            grid=(),
            in_specs=[pl.BlockSpec(memory_space=pl.ANY)],
            out_specs=pl.BlockSpec(memory_space=pltpu.VMEM),
            scratch_shapes=[pltpu.VMEM((QUAD, lines, LANES), F32), pltpu.SemaphoreType.DMA((QUAD,))],
        ),
        out_shape=jax.ShapeDtypeStruct((n_rows * 7, LANES), F32),
        compiler_params=pltpu.CompilerParams(vmem_limit_bytes=48 * MIB),
        cost_estimate=cost(50_000_000, 80 * MIB),
        name='add_rows',
    )(counts, codes, dx)


def to_lines(v):
    rows, dim = v.shape
    return v.reshape(rows // SUB, SUB, dim // LANES, LANES).transpose(0, PAIR, 1, 3).reshape(rows * dim // LANES, LANES)


def from_lines(v, dim):
    rows = v.shape[0] * LANES // dim
    return v.reshape(rows // SUB, dim // LANES, SUB, LANES).transpose(0, PAIR, 1, 3).reshape(rows, dim)


def _rms(v):
    return lax.rsqrt(jnp.mean(v * v, axis=-1, keepdims=True) + NORM_EPS)


def _head_mean(v, low):
    first = jnp.sum(jnp.where(low, v, 0.0), axis=-1, keepdims=True)
    second = jnp.sum(jnp.where(low, 0.0, v), axis=-1, keepdims=True)
    return jnp.where(low, first, second) * (1.0 / 64.0)


def _turn(v, cos_t, sin_t, lead):
    return v * cos_t + jnp.where(lead, -pltpu.roll(v, 96, 1), pltpu.roll(v, 32, 1)) * sin_t


def _spread(tile, low, ref):
    first = jnp.where(low, tile, 0.0)
    second = jnp.where(low, 0.0, tile)
    ref[0] = first.astype(BF16)
    ref[1] = pltpu.roll(first, HEAD, 1).astype(BF16)
    ref[PAIR] = pltpu.roll(second, HEAD, 1).astype(BF16)
    ref[3] = second.astype(BF16)


def _probs(q, k, block):
    scores = mm_nt(q, k) * 0.125
    n = scores.shape[1]
    row = lax.broadcasted_iota(jnp.int32, scores.shape, 0) + block
    col = lax.broadcasted_iota(jnp.int32, scores.shape, 1)
    scores = jnp.where(row >= col, scores, -1e30)
    e = jnp.exp(scores - jnp.max(scores, axis=-1, keepdims=True))
    return e * (1.0 / jnp.sum(e, axis=-1, keepdims=True))


def _lanes(rows):
    lane = lax.broadcasted_iota(jnp.int32, (rows, LANES), 1)
    return lane < HEAD, lane % HEAD < 32


def _attn_fwd_kernel(x_ref, w_ref, gain_ref, cos_ref, sin_ref, qk_gain_ref, in_ref, raw_ref, q_ref, k_ref, flat_ref, hid_ref, mlp_ref, kk, vv):
    seq, dim = x_ref.shape
    n_q = dim // LANES
    step = LANES
    n_in = raw_ref.shape[1]

    def project(r):
        at = pl.ds(pl.multiple_of(r * step, step), step)
        low, lead = _lanes(step)
        x = x_ref[at, :].astype(F32)
        m1 = (x * _rms(x) * gain_ref[0:1, :]).astype(BF16)
        in_ref[at, :] = m1
        raw = mm(m1, w_ref[0]).astype(BF16)
        raw_ref[at, :] = raw
        cos_t, sin_t = cos_ref[at, :], sin_ref[at, :]
        for t in range(n_q + 1):
            v = raw[:, t * LANES:(t + 1) * LANES].astype(F32)
            v = v * lax.rsqrt(_head_mean(v * v, low) + NORM_EPS)
            which = int(t == n_q)
            v = _turn(v * qk_gain_ref[SUB * which:SUB * which + 1, :], cos_t, sin_t, lead).astype(BF16)
            if which:
                k_ref[at, :] = v
            else:
                q_ref[at, t * LANES:(t + 1) * LANES] = v
    loop(seq // step, project)
    low, _ = _lanes(seq)
    _spread(k_ref[...].astype(F32), low, kk)
    _spread(raw_ref[:, n_in - LANES:].astype(F32), low, vv)

    def heads(t):
        tile = pl.ds(pl.multiple_of(t * LANES, LANES), LANES)
        for b in range(seq // step):
            n = (b + 1) * step
            q = q_ref[b * step:n, tile]
            total = None
            for side in range(PAIR):
                i = PAIR * ((PAIR * t + side) // 7) + side
                p = _probs(q, kk[i, :n, :], b * step).astype(BF16)
                o = mm(p, vv[i, :n, :])
                total = o if total is None else total + o
            flat_ref[b * step:n, tile] = total.astype(BF16)
    loop(n_q, heads)

    def finish(r):
        at = pl.ds(pl.multiple_of(r * step, step), step)
        h = (x_ref[at, :].astype(F32) + mm(flat_ref[at, :], w_ref[1, :, :dim])).astype(BF16)
        hid_ref[at, :] = h
        h = h.astype(F32)
        mlp_ref[at, :] = (h * _rms(h) * gain_ref[SUB:9, :]).astype(BF16)
    loop(seq // step, finish)


def attn_forward(x, w, gains, cos_t, sin_t, qk_gain):
    seq, dim = x.shape
    n_in = w.shape[PAIR]
    vmem = pl.BlockSpec(memory_space=pltpu.VMEM)
    sds = lambda n: jax.ShapeDtypeStruct((seq, n), BF16)
    return pl.pallas_call(
        _attn_fwd_kernel,
        out_shape=[sds(dim), sds(n_in), sds(dim), sds(LANES), sds(dim), sds(dim), sds(dim)],
        in_specs=[vmem] * 6,
        out_specs=[vmem] * 7,
        scratch_shapes=[pltpu.VMEM((QUAD, seq, LANES), BF16), pltpu.VMEM((QUAD, seq, LANES), BF16)],
        compiler_params=pltpu.CompilerParams(vmem_limit_bytes=40 * MIB),
        cost_estimate=cost(4_000_000_000, 12 * MIB, 4_000_000),
        name='attn_forward',
    )(x, w, gains, cos_t, sin_t, qk_gain)


def _norm_back(grad, normed, inv, gain):
    grad = grad * gain
    return inv * (grad - normed * jnp.mean(grad * normed, axis=-1, keepdims=True))


def _hidden_bwd_kernel(w_ref, gain_ref, hid_ref, dy_ref, part_ref, recv_ref, gh_ref, hb_ref, do_ref, mlp_gain_ref):
    step = LANES
    mlp_gain_ref[...] = jnp.zeros_like(mlp_gain_ref)

    def hidden(r):
        at = pl.ds(pl.multiple_of(r * step, step), step)
        grad = part_ref[at, :] + recv_ref[at, :]
        h = hid_ref[at, :].astype(F32)
        inv = _rms(h)
        normed = h * inv
        g = dy_ref[at, :].astype(F32) + _norm_back(grad, normed, inv, gain_ref[SUB:9, :])
        gh_ref[at, :] = g
        g = g.astype(BF16)
        hb_ref[at, :] = g
        do_ref[at, :] = mm_nt(g, w_ref[1, :, :g.shape[1]]).astype(BF16)
        mlp_gain_ref[...] = mlp_gain_ref[...] + jnp.sum(grad * normed, axis=0, keepdims=True)
    loop(hid_ref.shape[0] // step, hidden)


def hidden_backward(w, gains, hidden, dy, part, recv):
    vmem = pl.BlockSpec(memory_space=pltpu.VMEM)
    sds = jax.ShapeDtypeStruct
    return pl.pallas_call(
        _hidden_bwd_kernel,
        out_shape=[sds(part.shape, F32), sds(part.shape, BF16), sds(part.shape, BF16), sds((SUB, part.shape[1]), F32)],
        in_specs=[vmem] * 6,
        out_specs=[vmem] * QUAD,
        compiler_params=pltpu.CompilerParams(vmem_limit_bytes=24 * MIB),
        cost_estimate=cost(1_000_000_000, CHIPS * MIB),
        name='hidden_backward',
    )(w, gains, hidden, dy, part, recv)


class AttnBackward:
    arrays, inputs, outputs, scratches = PAIR, 15, 1, 11
    after = (False, False, False, True, True, True, True, True)
    nbytes = 22 * MIB

    def __init__(self, x, w, gains, mlp_gain, cos_t, sin_t, qk_gain, saved, gh, hb, do):
        seq, dim = x.shape
        n_in = w.shape[PAIR]
        far = (w, gh)
        self.operands = [(v, all(v is not f for f in far)) for v in (gains, mlp_gain, cos_t, sin_t, qk_gain, x, *far, *saved[:5], hb, do)]
        self.makes = [jax.ShapeDtypeStruct((dim, n), F32) for n in (n_in, dim)]
        self.results = [jax.ShapeDtypeStruct((seq + SUB, dim), F32)]
        scr = lambda *s: pltpu.VMEM(s[:-1], s[-1])
        self.scratch = [scr(dim, n_in, BF16), scr(QUAD, seq, LANES, BF16), scr(QUAD, seq, LANES, BF16), scr(QUAD, seq, LANES, F32), scr(QUAD, seq, LANES, F32),
                        scr(seq, n_in, BF16), scr(PAIR, SUB, LANES, F32), scr(PAIR, LANES, n_in, F32), scr(PAIR, LANES, dim, F32),
                        pltpu.SemaphoreType.DMA((PAIR,)), pltpu.SemaphoreType.DMA((PAIR, PAIR))]

    def run(self, operands, made, results, scratch, between):
        (gain_ref, mlp_gain_ref, cos_ref, sin_ref, qk_gain_ref, x_ref, w_hbm, gh_hbm, in_ref, raw_ref, q_ref, k_ref, flat_ref, hb, do) = operands
        w_ref, kk, vv, dk, dv, dqkv, qk_sum, in_out, out_out, in_sem, store_sem = scratch
        dx_ref, = results
        seq, dim = x_ref.shape
        n_q = dim // LANES
        step = LANES
        n_blk = seq // step
        n_in = raw_ref.shape[1]
        fetch = [pltpu.make_async_copy(gh_hbm, dx_ref.at[pl.ds(0, seq)], in_sem.at[0]), pltpu.make_async_copy(w_hbm.at[0], w_ref, in_sem.at[1])]
        for copy in fetch:
            copy.start()
        low_all, _ = _lanes(seq)
        _spread(k_ref[...].astype(F32), low_all, kk)
        _spread(raw_ref[:, n_in - LANES:].astype(F32), low_all, vv)
        for ref in (dk, dv, qk_sum):
            ref[...] = jnp.zeros_like(ref)

        def raw_back(grad, tile, at, which, low, lead):
            v = raw_ref[at, tile].astype(F32)
            inv = lax.rsqrt(_head_mean(v * v, low) + NORM_EPS)
            normed = v * inv
            grad = _turn(grad, cos_ref[at, :], -sin_ref[at, :], lead)
            qk_sum[which] = qk_sum[which] + jnp.sum(grad * normed, axis=0, keepdims=True)
            grad = grad * qk_gain_ref[SUB * which:SUB * which + 1, :]
            return inv * (grad - normed * _head_mean(grad * normed, low))

        def heads(t):
            tile = pl.ds(pl.multiple_of(t * LANES, LANES), LANES)
            low, lead = _lanes(step)
            for b in range(n_blk):
                n = (b + 1) * step
                at = pl.ds(b * step, step)
                q = q_ref[at, tile]
                g = do[at, tile]
                grad_q = None
                for side in range(PAIR):
                    i = PAIR * ((PAIR * t + side) // 7) + side
                    k = kk[i, :n, :]
                    p = _probs(q, k, b * step)
                    dp = mm_nt(g, vv[i, :n, :])
                    ds = (p * (dp - jnp.sum(dp * p, axis=-1, keepdims=True)) * 0.125).astype(BF16)
                    dv[i, :n, :] = dv[i, :n, :] + mm_tn(p.astype(BF16), g)
                    dk[i, :n, :] = dk[i, :n, :] + mm_tn(ds, q)
                    part = mm(ds, k)
                    grad_q = part if grad_q is None else grad_q + part
                dqkv[at, tile] = raw_back(grad_q, tile, at, 0, low, lead).astype(BF16)
            for part in range(n_q):
                between(part, t == part)
        loop(n_q, heads)

        def keys(r):
            at = pl.ds(pl.multiple_of(r * step, step), step)
            low, lead = _lanes(step)

            def join(ref):
                return jnp.where(low, ref[0, at, :] + pltpu.roll(ref[1, at, :], HEAD, 1), ref[3, at, :] + pltpu.roll(ref[PAIR, at, :], HEAD, 1))
            dqkv[at, dim:dim + LANES] = raw_back(join(dk), pl.ds(dim, LANES), at, 1, low, lead).astype(BF16)
            dqkv[at, dim + LANES:] = join(dv).astype(BF16)
        loop(n_blk, keys)
        for copy in fetch:
            copy.wait()

        def inputs(r, total):
            at = pl.ds(pl.multiple_of(r * step, step), step)
            grad = mm_nt(dqkv[at, :], w_ref[...])
            x = x_ref[at, :].astype(F32)
            inv = _rms(x)
            normed = x * inv
            dx_ref[at, :] = dx_ref[at, :] + _norm_back(grad, normed, inv, gain_ref[0:1, :])
            return total + jnp.sum(grad * normed, axis=0, keepdims=True)
        attn_gain = lax.fori_loop(0, n_blk, inputs, jnp.zeros((1, dim), F32))
        between(n_q)

        low, _ = _lanes(SUB)
        row = lax.broadcasted_iota(jnp.int32, (SUB, dim), 0)
        fold = lambda v: v + pltpu.roll(v, HEAD, 1)
        dx_ref[seq:, :] = jnp.where(row == 1, jnp.broadcast_to(attn_gain, (SUB, dim)), jnp.where(row == PAIR, mlp_gain_ref[...], 0.0))
        dx_ref[seq:, :LANES] = jnp.where(row[:, :LANES] == 0, jnp.where(low, fold(qk_sum[0]), fold(qk_sum[1])), dx_ref[seq:, :LANES])

        def stores(t):
            return [pltpu.make_async_copy(buf.at[t % PAIR], ref.at[pl.ds(pl.multiple_of(t * LANES, LANES), LANES)], store_sem.at[i, t % PAIR])
                    for i, (buf, ref) in enumerate(((in_out, made[0]), (out_out, made[1])))]

        def weights(t):
            @pl.when(t >= PAIR)
            def _():
                for copy in stores(t - PAIR):
                    copy.wait()
            tile = pl.ds(pl.multiple_of(t * LANES, LANES), LANES)
            in_out[t % PAIR] = mm_tn(in_ref[:, tile], dqkv[...])
            out_out[t % PAIR] = mm_tn(flat_ref[:, tile], hb[...])
            for copy in stores(t):
                copy.start()
        loop(n_q, weights)
        for t in (n_q - PAIR, n_q - 1):
            for copy in stores(t):
                copy.wait()


def _mlp_kernel(x_ref, dy_ref, wgu_ref, wd_ref, y_mine, y_other, din_mine, din_other, dwg_ref, dwu_ref, dwd_ref, xt, wg, wu, wd, act, dg, du, og, ou, od, load_sem, store_sem):
    half, tile = dwd_ref.shape[0], act.shape[1]
    n_tile = -(-half // tile)
    shared = n_tile * tile - half
    seq = y_mine.shape[0]
    step = seq // PAIR

    def start_of(j):
        first = (j == 0).astype(jnp.int32)
        return pl.multiple_of(first * (half - tile) + (1 - first) * (j - 1) * tile, LANES)

    def loads(j):
        at, slot = start_of(j), j % PAIR
        return [pltpu.make_async_copy(wgu_ref.at[:, pl.ds(at, tile)], wg.at[slot], load_sem.at[0, slot]),
                pltpu.make_async_copy(wgu_ref.at[:, pl.ds(pl.multiple_of(half + at, LANES), tile)], wu.at[slot], load_sem.at[1, slot]),
                pltpu.make_async_copy(wd_ref.at[pl.ds(at, tile)], wd.at[slot], load_sem.at[PAIR, slot])]

    def stores(j):
        at, slot = start_of(j), j % PAIR
        return [pltpu.make_async_copy(og.at[slot], dwg_ref.at[:, pl.ds(at, tile)], store_sem.at[0, slot]),
                pltpu.make_async_copy(ou.at[slot], dwu_ref.at[:, pl.ds(at, tile)], store_sem.at[1, slot]),
                pltpu.make_async_copy(od.at[slot], dwd_ref.at[pl.ds(at, tile)], store_sem.at[PAIR, slot])]

    for copy in loads(jnp.int32(0)):
        copy.start()
    for ref in (y_mine, y_other, din_mine, din_other):
        ref[...] = jnp.zeros_like(ref)
    xt[...] = x_ref[...].T

    def columns(j):
        slot = j % PAIR

        @pl.when(j + 1 < n_tile)
        def _():
            for copy in loads(j + 1):
                copy.start()
        for copy in loads(j):
            copy.wait()

        def rows(y_ref, din_ref, first, r):
            at, inner = pl.ds(pl.multiple_of(first + r * step, step), step), pl.ds(pl.multiple_of(r * step, step), step)
            x = x_ref[at, :]
            gate, up, back = mm(x, wg[slot]), mm(x, wu[slot]), mm_nt(dy_ref[at, :], wd[slot])
            counts = lax.broadcasted_iota(jnp.int32, (step, tile), 1) >= (j == 0).astype(jnp.int32) * shared
            up, back = jnp.where(counts, up, 0.0), jnp.where(counts, back, 0.0)
            sig = lax.logistic(gate)
            silu = gate * sig
            a = (silu * up).astype(BF16)
            g = (back * up * sig * (1.0 + gate * (1.0 - sig))).astype(BF16)
            u = (back * silu).astype(BF16)
            act[at, :], dg[at, :], du[at, :] = a, g, u
            y_ref[inner, :] = y_ref[inner, :] + mm(a, wd[slot])
            din_ref[inner, :] = din_ref[inner, :] + mm_nt(g, wg[slot]) + mm_nt(u, wu[slot])
        loop(PAIR, functools.partial(rows, y_mine, din_mine, 0))
        loop(PAIR, functools.partial(rows, y_other, din_other, seq))

        @pl.when(j >= PAIR)
        def _():
            for copy in stores(j - PAIR):
                copy.wait()
        og[slot] = mm(xt[...], dg[...])
        ou[slot] = mm(xt[...], du[...])
        od[slot] = mm_tn(act[...], dy_ref[...])
        for copy in stores(j):
            copy.start()
    loop(n_tile, columns)
    for j in (n_tile - PAIR, n_tile - 1):
        for copy in stores(jnp.int32(j)):
            copy.wait()


def mlp(x, dy, wgu, wd):
    rows, dim = x.shape
    half = wd.shape[0]
    tile = 512
    vmem, hbm = pl.BlockSpec(memory_space=pltpu.VMEM), pl.BlockSpec(memory_space=pl.ANY)
    sds = lambda *s: jax.ShapeDtypeStruct(s, F32)
    dma = pltpu.SemaphoreType.DMA
    bf = lambda *s: pltpu.VMEM(s, BF16)
    f = lambda *s: pltpu.VMEM(s, F32)
    return pl.pallas_call(
        _mlp_kernel,
        out_shape=[sds(rows // PAIR, dim)] * QUAD + [sds(dim, half), sds(dim, half), sds(half, dim)],
        in_specs=[vmem, vmem, hbm, hbm],
        out_specs=[vmem] * QUAD + [hbm] * 3,
        scratch_shapes=[bf(dim, rows), bf(PAIR, dim, tile), bf(PAIR, dim, tile), bf(PAIR, tile, dim), bf(rows, tile), bf(rows, tile), bf(rows, tile),
                        f(PAIR, dim, tile), f(PAIR, dim, tile), f(PAIR, tile, dim), dma((3, PAIR)), dma((3, PAIR))],
        compiler_params=pltpu.CompilerParams(vmem_limit_bytes=44 * MIB),
        cost_estimate=cost(CHIPS * rows * dim * half, 50 * MIB, rows * half),
        name='mlp',
    )(x, dy, wgu, wd)


def _codes(numbers, count):
    return tuple(numbers[i // 10] // LANES ** (i % 10) % LANES for i in range(count))


ROWS_SEQ = (
    _codes((152348940317322383368, 678662145372396725288, 751232056588892674273, 827272104050806263145, 30857149562), 45),
    _codes((166206088102504171520, 236385149464955200810, 603605329936848293224, 1039985241786269873361, 32734212313), 45),
)
ATTN_SEQ = (
    _codes((370142165075936415752, 972012016723415295145, 1124725529257844811929), 30),
    _codes((961577811093152729088, 751808515438843144256, 1124738970787495025897), 30),
)
GRAD_SEQ = (
    _codes((106232080133048504328, 412786621588976116131, 918546169305131799568, 485409126374496736530, 238786845178607580779, 257151255934452689491, 843574817237186309276, 33002831324), 75),
    _codes((166206088102504171520, 704158088118449268010, 330331505424276671520, 463101567523338654259, 770399732085151419931, 1050366487184744456811, 848110399440616747490, 33002831324), 75),
)


def solution(mesh):
    n_dev = mesh.shape[AXIS_NAME]
    n_chip = n_dev // PAIR
    pair = [(i, i ^ 1) for i in range(n_dev)]
    groups = [[PAIR * k + c for k in range(n_chip)] for c in range(PAIR)]

    row_spec = P(AXIS_NAME, None)
    vec_spec = P(AXIS_NAME)
    full_spec = P(None)
    batch_spec = P(AXIS_NAME, None, None)
    weight_specs = (vec_spec, row_spec, row_spec, row_spec, full_spec, full_spec, row_spec, vec_spec, row_spec, row_spec, row_spec)

    def swap(v):
        return lax.ppermute(v, AXIS_NAME, pair)

    def gather_group(v):
        return lax.all_gather(v, AXIS_NAME, axis_index_groups=groups, tiled=True)

    def device_step(tokens, positions, table_shard, attn_norm, w_query, w_key, w_value, q_norm, k_norm, w_out, mlp_norm, w_gate, w_up, w_down, dy_out):
        me = lax.axis_index(AXIS_NAME)
        core = lax.rem(me, PAIR)
        seq_len = tokens.shape[1]
        rows_local, model_dim = table_shard.shape
        rows_w, ff = w_gate.shape
        half = ff // PAIR
        nq, nk = w_query.shape[1], w_key.shape[1]
        head_dim = q_norm.shape[0]

        n_in = nq + PAIR * nk

        def gate_up(c):
            return jnp.concatenate([lax.dynamic_slice(w, (0, c * half), (rows_w, half)) for w in (w_gate, w_up)], axis=1)

        def both_cores(mine, other):
            return jnp.where(core == 0, jnp.concatenate([mine, other], axis=0), jnp.concatenate([other, mine], axis=0))
        attn_in = jnp.concatenate([w_query, w_key, w_value], axis=1)
        attn_out = jnp.concatenate([w_out, below(jnp.stack([attn_norm, mlp_norm]), n_in - nq - PAIR).T], axis=1)
        mine_attn, other_attn = jnp.where(core == 0, attn_in, attn_out), jnp.where(core == 0, attn_out, attn_in)
        dy = dy_out.reshape(seq_len, model_dim)
        all_tokens, (down_block, recv_gu, recv_attn, dy_other) = all_rows(
            below(tokens.reshape(-1, LANES), QUAD), n_dev, [w_down, gate_up(1 - core), other_attn, dy], ('use', 'pair', 'pair', 'pair'), 0)
        wgu = gather_group(both_cores(gate_up(core), recv_gu))

        (attn_w, wd), _ = gather_all([both_cores(mine_attn, recv_attn), down_block], [(0, 0, PAIR * rows_w, 'core'), (1, 0, down_block.shape[0], 'chip')],
                                     ('bza', 'zba'), ATTN_SEQ, [], (), n_dev, 1)
        attn_w = attn_w.reshape(PAIR, model_dim, n_in)
        wd = wd.reshape(-1, model_dim)

        all_ids = all_tokens[:, :seq_len // LANES].reshape(-1)
        local_ids = all_ids - me * rows_local
        is_owner = (local_ids >= 0) & (local_ids < rows_local)
        own = is_owner.reshape(n_dev, seq_len)
        slot = jnp.arange(seq_len, dtype=jnp.int32)
        upto = (slot[:, None] <= slot[None, :]).astype(BF16)
        rank = jnp.where(own, mm(own.astype(BF16), upto).astype(jnp.int32) - 1, -1)
        counts = jnp.sum(own.astype(jnp.int32), axis=1)
        lines = model_dim // LANES
        line = lambda row: row // SUB * (SUB * lines) + row % SUB
        code = line(slot)[None] * 65536 + line(jnp.where(own, local_ids.reshape(n_dev, seq_len), 0))
        codes = jnp.sum(jnp.where(rank[:, :, None] == slot, code[:, :, None], 0), axis=1)
        codes = jnp.where(slot[None] < counts[:, None], codes, seq_len * lines * 65536).reshape(-1)
        picked = lookup(table_shard, counts, codes, seq_len)
        x_emb = scatter_sum([picked], [(0, 0, 192, 'device'), (0, 192, 208, 'device'), (0, 400, 112, 'device')], ('zba', 'zba', 'baz'), ROWS_SEQ, PAIR)[0]

        dy2 = jnp.concatenate([dy, dy_other], axis=0)

        gains = below(jnp.repeat(attn_w[1, :, nq:nq + PAIR].astype(F32).T, SUB, axis=0), SUB)
        qk_gain = jnp.repeat(jnp.stack([jnp.tile(q_norm, PAIR), jnp.tile(k_norm, PAIR)]).astype(F32), SUB, axis=0)

        inv_freq = jnp.exp((jnp.arange(LANES) % (head_dim // PAIR)).astype(F32) * (-2.0 * math.log(ROPE_THETA) / head_dim))
        angles = positions.reshape(seq_len, 1).astype(F32) * inv_freq
        cos_t, sin_t = jnp.cos(angles), jnp.sin(angles)
        saved = attn_forward(x_emb, attn_w, gains, cos_t, sin_t, qk_gain)
        hidden, mlp_in = saved[5:]

        mlp2 = jnp.concatenate([mlp_in, swap(mlp_in)], axis=0)
        y_mine, y_other, grad_in, grad_other, grad_w_gate, grad_w_up, grad_w_down = mlp(mlp2, dy2, wgu, wd)
        grad_recv = swap(grad_other)
        layer_out = (hidden.astype(F32) + (y_mine + swap(y_other))).astype(BF16)

        gh, hb, grad_heads, mlp_gain = hidden_backward(attn_w, gains, hidden, dy, grad_in, grad_recv)
        by_chip = [u.reshape(n_chip, -1, u.shape[1]) for u in (grad_w_down, grad_w_gate, grad_w_up)]
        down_rows, gate_shard, up_shard, in_shard, out_shard, _, _, dx_block = scatter_sum(
            by_chip, [(i, 0, u.shape[1], 'chip') for i, u in enumerate(by_chip)] + [(i, 0, 32, 'rows') for i in (3, QUAD)], ('bza', 'zba', 'bza', 'zba', 'zba'), GRAD_SEQ, 3,
            AttnBackward(x_emb, attn_w, gains, mlp_gain, cos_t, sin_t, qk_gain, saved, gh, hb, grad_heads))

        chip_rows = jnp.concatenate([gate_shard, up_shard], axis=1)
        mine = lax.dynamic_slice(chip_rows, (core * rows_w, 0), (rows_w, chip_rows.shape[1]))
        give = lax.dynamic_slice(chip_rows, ((1 - core) * rows_w, 0), (rows_w, chip_rows.shape[1]))
        (all_dx,), (down_shard, recv) = gather_all(
            [to_lines(dx_block)], [(0, 0, 200 * lines, 'device'), (0, 200 * lines, 200 * lines, 'device'), (0, 400 * lines, 120 * lines, 'device')],
            ('zba', 'zba', 'baz'), ROWS_SEQ, [down_rows, give], ('store', 'pair'), n_dev, QUAD)
        d_table = from_lines(add_rows(all_dx, counts, codes, rows_local), model_dim)
        gains_grad = from_lines(jnp.sum(all_dx[:, seq_len * lines:], axis=0), model_dim)
        qk = gains_grad[0]
        d_attn_norm, d_mlp_norm = (lax.dynamic_slice(gains_grad[i], (me * rows_w,), (rows_w,)) for i in (1, PAIR))
        low = jnp.where(core == 0, mine, recv)
        high = jnp.where(core == 0, recv, mine)
        d_gate = jnp.concatenate([low[:, :half], high[:, :half]], axis=1)
        d_up = jnp.concatenate([low[:, half:ff], high[:, half:ff]], axis=1)
        in_rows = lax.dynamic_slice(in_shard, (core * (rows_w - 24), 0), (rows_w, n_in))
        d_query, d_key, d_value = in_rows[:, :nq], in_rows[:, nq:nq + nk], in_rows[:, nq + nk:]
        d_out = lax.dynamic_slice(out_shard, (core * (rows_w - 24), 0), (rows_w, nq))
        return (layer_out.reshape(1, seq_len, model_dim), d_table, d_attn_norm, d_query, d_key, d_value, qk[:head_dim], qk[head_dim:PAIR * head_dim], d_out, d_mlp_norm, d_gate, d_up, down_shard)

    return jax.shard_map(device_step, mesh=mesh, in_specs=(row_spec, row_spec, row_spec) + weight_specs + (batch_spec,), out_specs=(batch_spec, row_spec) + weight_specs, check_vma=False)
```

```python
import functools
import math
import jax
import jax.numpy as jnp
from jax import lax
from jax.experimental import pallas as pl
from jax.experimental.pallas import tpu as pltpu
from jax.sharding import PartitionSpec as P

NORM_EPS = 1e-6
ROPE_THETA = 1.0e6
AXIS_NAME = 'fsdp'
F32 = jnp.float32
BF16 = jnp.bfloat16
MESH = pl.DeviceIdType.MESH
LANES, HEAD, CHIPS, SUB, QUAD, PAIR, MIB = 128, 64, 16, 8, 4, 2, 1 << 20
KIND = PIECE = 3


def mm(a, b):
    return lax.dot_general(a, b, (((1,), (0,)), ((), ())), preferred_element_type=F32)


def mm_nt(a, b):
    return lax.dot_general(a, b, (((1,), (1,)), ((), ())), preferred_element_type=F32)


def mm_tn(a, b):
    return lax.dot_general(a, b, (((0,), (0,)), ((), ())), preferred_element_type=F32)


def cost(flops, nbytes, transcendentals=0):
    return pl.CostEstimate(flops=flops, bytes_accessed=nbytes, transcendentals=transcendentals)


def below(v, rows):
    return jnp.pad(v, ((0, rows), (0, 0)))


def loop(count, body):
    def step(i, carry):
        body(i)
        return carry
    lax.fori_loop(0, count, step, 0)


def _unpack(code):
    return code // HEAD, code // 32 % PAIR, code // SUB % QUAD, code % SUB


def _via(u, key, orders):
    da, db, p, piece = key
    last = None
    for axis in orders[piece]:
        if axis == 'a' and da or axis == 'b' and db:
            last = axis
        if axis == 'z' and p != u:
            last = 'z+' if p > u else 'z-'
    return last


def _onward(u, key, orders):
    order = orders[key[PIECE]]
    via = _via(u, key, orders)
    left = order if via is None else order[order.index(via[0]) + 1:]
    out = []
    if u < 3 and (via == 'z-' or 'z' in left):
        out.append('z+')
    if u > 0 and (via == 'z+' or 'z' in left):
        out.append('z-')
    return out + [axis for axis in 'ba' if axis in left]


def _seen_by_parent(u, key, orders):
    da, db, p, piece = key
    via = _via(u, key, orders)
    if via == 'a':
        return u, (0, db, p, piece), 'a'
    if via == 'b':
        return u, (da, 0, p, piece), 'b'
    if via == 'z-':
        return u - 1, key, 'z+'
    if u == 0:
        return 1, key, 'z-'
    return 1, (da, db, 3 - p, piece), 'z+'


class _Place:
    def __init__(self, me, swapped=False):
        self.me = me
        self.core = me % PAIR
        x, y, self.z = (me // PAIR) % PAIR, (me // QUAD) % PAIR, me // SUB
        other = 1 - self.core if swapped else self.core
        self.a = y * (1 - other) + x * other
        self.b = x * (1 - other) + y * other
        self.a_str, self.b_str = QUAD - PAIR * other, PAIR + PAIR * other
        self.far = self.z // PAIR
        self.u = 3 * self.far + (1 - PAIR * self.far) * self.z
        self.partner = me + 1 - PAIR * self.core

    def chip(self, key):
        da, db, p = key[:3]
        a = self.a + da * (1 - PAIR * self.a)
        b = self.b + db * (1 - PAIR * self.b)
        z = 3 * self.far + (1 - PAIR * self.far) * p
        return (SUB * z + a * self.a_str + b * self.b_str) // PAIR

    def side(self, name):
        if name == 'a':
            return self.me + (1 - PAIR * self.a) * self.a_str
        if name == 'b':
            return self.me + (1 - PAIR * self.b) * self.b_str
        return self.me + SUB * (1 - PAIR * self.far) * (1 if name == 'z+' else -1)


def _remote(src, dst, send_sem, recv_sem, dev):
    return pltpu.make_async_remote_copy(src_ref=src, dst_ref=dst, send_sem=send_sem, recv_sem=recv_sem, device_id=(dev,), device_id_type=MESH)


def _meet(peers, me=None, ends=()):
    sem = pltpu.get_barrier_semaphore()

    def meet(everyone):
        for peer in everyone:
            pl.semaphore_signal(sem, inc=1, device_id=(peer,), device_id_type=MESH)
        pl.semaphore_wait(sem, len(everyone))

    if not ends:
        meet(peers)
        return
    to, frm = ends
    pl.when(to != me)(lambda: meet(peers + [to, frm]))
    pl.when(to == me)(lambda: meet(peers))


def _landed(ref, sem):
    pltpu.make_async_copy(ref, ref, sem).wait()


def _passes(moves, me):
    for kind in moves:
        if kind == 'pair':
            other = me + 1 - PAIR * (me % PAIR)
            yield other, other
        elif kind == 'use':
            yield PAIR * (me % CHIPS) + me // CHIPS, CHIPS * (me % PAIR) + me // PAIR
        else:
            yield CHIPS * (me % PAIR) + me // PAIR, PAIR * (me % CHIPS) + me // CHIPS


def _start_move(kind, src, dst, send_sem, recv_sem, to, me):
    copy = _remote(src, dst, send_sem, recv_sem, to)
    if kind == 'pair':
        copy.start()
    else:
        pl.when(to != me)(copy.start)
        pl.when(to == me)(pltpu.make_async_copy(src, dst, recv_sem).start)
    return copy


def _end_move(kind, copy, dst, recv_sem, to, me):
    _landed(dst, recv_sem)
    if kind == 'pair':
        copy.wait_send()
    else:
        pl.when(to != me)(copy.wait_send)


def _all_rows_kernel(n_dev, moves, *refs):
    n = len(moves)
    in_ref, src, out_ref, dst = refs[0], refs[1:1 + n], refs[1 + n], refs[PAIR + n:PAIR + PAIR * n]
    send_sem, recv_sem, m_send, m_recv = refs[PAIR + PAIR * n:]
    me = lax.axis_index(AXIS_NAME)
    peers = [(me + d) % n_dev for d in range(1, n_dev)]
    _meet(peers)
    copies = [_remote(in_ref, out_ref.at[me], send_sem.at[i], recv_sem.at[i], peer) for i, peer in enumerate(peers)]
    for copy in copies:
        copy.start()
    ends = [to for to, _ in _passes(moves, me)]
    moving = [_start_move(moves[i], src[i], dst[i], m_send.at[i], m_recv.at[i], to, me) for i, to in enumerate(ends)]
    out_ref[me] = in_ref[...]
    for copy in copies:
        copy.wait()
    for i, copy in enumerate(moving):
        _end_move(moves[i], copy, dst[i], m_recv.at[i], ends[i], me)


def all_rows(block, n_dev, moved, moves, collective_id):
    n = len(moves)
    dma = pltpu.SemaphoreType.DMA
    vmem, hbm = pl.BlockSpec(memory_space=pltpu.VMEM), pl.BlockSpec(memory_space=pl.ANY)
    res = pl.pallas_call(
        functools.partial(_all_rows_kernel, n_dev, moves),
        out_shape=[jax.ShapeDtypeStruct((n_dev,) + block.shape, block.dtype)] + [jax.ShapeDtypeStruct(v.shape, v.dtype) for v in moved],
        in_specs=[vmem] + [hbm] * n,
        out_specs=[vmem] + [hbm] * n,
        scratch_shapes=[dma((n_dev - 1,)), dma((n_dev - 1,)), dma((n,)), dma((n,))],
        compiler_params=pltpu.CompilerParams(collective_id=collective_id, has_side_effects=True),
        cost_estimate=cost(10_000_000, 1 * MIB),
        name='all_rows',
    )(block, *moved)
    return res[0], res[1:]


def _gather_kernel(pieces, orders, seq, moves, n_arr, work, *refs):
    n, m = len(moves), len(pieces)
    refs_left = list(refs)
    cut = lambda count: [refs_left.pop(0) for _ in range(count)]
    ins, src, work_in = cut(n_arr), cut(n), cut(PAIR if work else 0)
    outs, dst, work_out = cut(n_arr), cut(n), cut(1 if work else 0)
    own_sem, send_sem, recv_sem, p_send, p_recv, m_send, m_recv = cut(7)
    me = lax.axis_index(AXIS_NAME)
    at = _Place(me)
    ends = list(_passes(moves, me))
    kinds = {p[0]: p[KIND] for p in pieces}

    def slot_of(kc, core, kind):
        return {'device': PAIR * kc + core, 'core': CHIPS * core + kc, 'chip': kc}[kind]

    def part(kc, core, piece):
        arr, r0, rows, kind = pieces[piece]
        slot = slot_of(kc, core, kind)
        return outs[arr].at[slot] if rows == outs[arr].shape[1] else outs[arr].at[slot, pl.ds(r0, rows)]

    def own(i):
        return pltpu.make_async_copy(ins[i], outs[i].at[slot_of(me // PAIR, at.core, kinds[i])], own_sem.at[i])

    class Node:
        def __init__(self, u):
            self.u, self.sent, self.handed = u, [], [0] * m
            self.keys = [_unpack(c) for c in seq[u]]

        def step(self, key):
            piece = key[PIECE]
            arr, r0, rows, kind = pieces[piece]
            kc = at.chip(key)
            place = part(kc, at.core, piece)
            if _via(self.u, key, orders) is None:
                ref = ins[arr] if rows == ins[arr].shape[0] else ins[arr].at[pl.ds(r0, rows)]
            else:
                ref = place
                _landed(ref, recv_sem.at[piece, kc])
            for side in _onward(self.u, key, orders):
                _remote(ref, place, send_sem.at[len(self.sent)], recv_sem.at[piece, kc], at.side(side)).start()
                self.sent.append(piece)
            if kind != 'chip':
                _remote(ref, place, p_send.at[piece, self.handed[piece]], p_recv.at[piece, kc], at.partner).start()
                self.handed[piece] += 1

    nodes = [Node(u) for u in (0, 1)]

    def each(do):
        for node in nodes:
            pl.when(at.u == node.u)(functools.partial(do, node))

    def begin(node):
        far = [end for kind, end in zip(moves, ends) if kind != 'pair']
        _meet([at.side(s) for s in ['a', 'b', 'z+'] + (['z-'] if node.u else [])] + [at.partner], me, far[0] if far else ())
        for piece in range(m):
            node.step((0, 0, node.u, piece))

    def between(part, parts, when=None):
        def steps(node):
            count = len(node.keys)
            for key in node.keys[part * count // parts:(part + 1) * count // parts]:
                node.step(key)
        if when is None:
            each(steps)
        else:
            pl.when(when)(lambda: each(steps))

    def end(node):
        def sent(piece, sem):
            ref = part(0, 0, piece)
            _remote(ref, ref, sem, sem, at.partner).wait_send()
        for piece in range(m):
            if pieces[piece][KIND] != 'chip':
                for kc in range(CHIPS):
                    _landed(part(kc, 1 - at.core, piece), p_recv.at[piece, kc])
            for i in range(node.handed[piece]):
                sent(piece, p_send.at[piece, i])
        for i, piece in enumerate(node.sent):
            sent(piece, send_sem.at[i])
    each(begin)
    for i, (to, _) in enumerate(ends):
        _start_move(moves[i], src[i], dst[i], m_send.at[i], m_recv.at[i], to, me)
    for i in range(n_arr):
        own(i).start()
    if work:
        work(work_in, work_out, refs_left, between)
    else:
        between(0, 1)
    each(end)
    for i, (to, _) in enumerate(ends):
        _end_move(moves[i], _remote(src[i], dst[i], m_send.at[i], m_recv.at[i], to), dst[i], m_recv.at[i], to, me)
    for i in range(n_arr):
        own(i).wait()


def gather_all(blocks, pieces, orders, seq, moved, moves, n_dev, collective_id, found=None):
    n, m, n_arr = len(moves), len(pieces), len(blocks)
    dma = pltpu.SemaphoreType.DMA
    vmem, hbm = pl.BlockSpec(memory_space=pltpu.VMEM), pl.BlockSpec(memory_space=pl.ANY)
    nbytes = sum(v.size * v.dtype.itemsize for v in blocks)
    kinds = {p[0]: p[KIND] for p in pieces}
    scratch = [dma((n_arr,)), dma((24 * m,)), dma((m, CHIPS)), dma((m, CHIPS)), dma((m, CHIPS)), dma((max(n, 1),)), dma((max(n, 1),))]
    outs = [jax.ShapeDtypeStruct((n_dev // PAIR if kinds[i] == 'chip' else n_dev,) + v.shape, v.dtype) for i, v in enumerate(blocks)]
    outs += [jax.ShapeDtypeStruct(v.shape, v.dtype) for v in moved]
    extra, near = [], []
    if found is not None:
        codes, table, seq_len = found
        n_rows, dim = table.shape
        extra, near = [codes, table], [pl.BlockSpec(memory_space=pltpu.SMEM), hbm]
        outs.append(jax.ShapeDtypeStruct((codes.size // seq_len, seq_len, dim), table.dtype))
        scratch += [pltpu.VMEM((PAIR, _chunk(n_rows), dim), BF16), pltpu.VMEM(((n_rows + SUB) * dim // LANES, LANES), F32), pltpu.VMEM((seq_len * dim // LANES, LANES), F32),
                    pltpu.VMEM((PAIR, seq_len, dim), BF16), dma((PAIR,)), dma((PAIR,))]
        nbytes += 26 * MIB
    res = pl.pallas_call(
        functools.partial(_gather_kernel, tuple(pieces), orders, seq, moves, n_arr, _pick if found is not None else None),
        out_shape=outs,
        in_specs=[vmem] * n_arr + [hbm] * n + near,
        out_specs=[hbm] * len(outs),
        scratch_shapes=scratch,
        compiler_params=pltpu.CompilerParams(collective_id=collective_id, has_side_effects=True, vmem_limit_bytes=nbytes + (SUB * MIB)),
        cost_estimate=cost(200_000_000, nbytes * HEAD),
        name='gather_all',
    )(*blocks, *moved, *extra)
    return res[:n_arr], res[n_arr:]


def _chunk(n_rows):
    return n_rows // 9 if n_rows % 144 == 0 else n_rows


def _pick(operands, results, scratch, between):
    codes, table = operands
    picked, = results
    chunk, rows, block, out, load_sem, store_sem = scratch
    n_src, seq, dim = picked.shape
    n_col = dim // LANES
    size = chunk.shape[1]
    n_chunk = table.shape[0] // size

    def load(i):
        return pltpu.make_async_copy(table.at[pl.ds(pl.multiple_of(i * size, SUB), size)], chunk.at[i % PAIR], load_sem.at[i % PAIR])
    load(jnp.int32(0)).start()

    def widen(c):
        pl.when(c + 1 < n_chunk)(lambda: load(c + 1).start())
        load(c).wait()

        def part(i):
            line = (c * size + i * CHIPS) * n_col
            for j in range(n_col):
                v = chunk[c % PAIR, pl.ds(pl.multiple_of(i * CHIPS, CHIPS), CHIPS), j * LANES:(j + 1) * LANES].astype(F32)
                rows[pl.ds(pl.multiple_of(line + j * SUB, SUB), SUB), :] = v[:SUB]
                rows[pl.ds(pl.multiple_of(line + (n_col + j) * SUB, SUB), SUB), :] = v[SUB:]
        loop(size // CHIPS, part)
    loop(n_chunk, widen)
    rows[table.shape[0] * n_col:, :] = jnp.zeros((SUB * n_col, LANES), F32)

    def store(b):
        return pltpu.make_async_copy(out.at[b % PAIR], picked.at[b], store_sem.at[b % PAIR])

    def source(b):
        def eight(i):
            for t in range(SUB):
                block[pl.ds(i * (SUB * n_col) + t, n_col, stride=SUB), :] = rows[pl.ds(codes[b * seq + i * SUB + t], n_col, stride=SUB), :]
        loop(seq // SUB, eight)
        pl.when(b >= PAIR)(lambda: store(b - PAIR).wait())

        def narrow(i):
            line = pl.multiple_of(i * (CHIPS * n_col), SUB)
            for j in range(n_col):
                v = jnp.concatenate([block[pl.ds(line + j * SUB, SUB), :], block[pl.ds(line + (n_col + j) * SUB, SUB), :]], axis=0)
                out[b % PAIR, pl.ds(pl.multiple_of(i * CHIPS, CHIPS), CHIPS), j * LANES:(j + 1) * LANES] = v.astype(BF16)
        loop(seq // CHIPS, narrow)
        store(b).start()

    parts = n_src // PAIR

    def some(t):
        loop(PAIR, lambda i: source(PAIR * t + i))
        for part in range(parts):
            between(part, parts, t == part)
    loop(parts, some)
    for b in (n_src - PAIR, n_src - 1):
        store(jnp.int32(b)).wait()


def _slots(pieces, orders, seq):
    table, most = {}, [1] * len(pieces)
    for u in (0, 1):
        used = [0] * len(pieces)
        for key in [_unpack(c) for c in reversed(seq[u])] + [(0, 0, u, i) for i in range(len(pieces))]:
            for side in _onward(u, key, orders):
                table[u, key, side] = used[key[PIECE]]
                used[key[PIECE]] += 1
        most = [max(a, b) for a, b in zip(most, used)]
    return table, most


def _order(u, seq, orders, n, n_late, lead, after):
    keys = [_unpack(c) for c in reversed(seq[u])]
    roots = [(0, 0, u, i) for i in range(n)]
    if not n_late:
        return keys + roots, [], []
    late = [key for key in keys if key[PIECE] >= n - n_late]
    rest = [key for key in keys if key not in late]
    first = [key for key in rest if not _onward(u, key, orders)][:lead]
    rest = [key for key in rest if key not in first]
    sums = [key for key in rest if _onward(u, key, orders)]
    parts = [[sums.pop(0)] if some else [] for some in after]
    rest = [key for key in rest if [key] not in parts]
    out, share = [], 0
    rate = len(late) / (len(rest) * 0.85)
    for key in rest:
        out.append(key)
        share += rate
        while share >= 1 and late:
            out.append(late.pop(0))
            share -= 1
    return first, parts, out + late + roots


def _scatter_kernel(pieces, orders, seq, n_arr, work, *refs):
    table, _ = _slots(pieces, orders, seq)
    n = len(pieces)
    paired = [p[KIND] != 'chip' for p in pieces]
    n_late, n_in, n_out, n_scr = (work.arrays, work.inputs, work.outputs, work.scratches) if work else (0, 0, 0, 0)
    cut = lambda count: [refs_left.pop(0) for _ in range(count)]
    refs_left = list(refs)
    ins, work_in, outs, made, work_out = cut(n_arr - n_late), cut(n_in), cut(n_arr), cut(n_late), cut(n_out)
    ins += made
    land, stage, pair = cut(n), cut(n), cut(sum(paired))
    load_sem, send_sem, recv_sem, d_send, d_recv, out_sem = cut(6)
    got = [pair.pop(0) if p else None for p in paired]
    me = lax.axis_index(AXIS_NAME)
    at, partner_at = _Place(me), _Place(me, swapped=True)
    early = [i for i in range(n) if pieces[i][0] < n_arr - n_late]
    late = [i for i in range(n) if i not in early]

    def rows_of(ref, piece):
        _, r0, rows, _ = pieces[piece]
        return ref if rows == ref.shape[0] else ref.at[pl.ds(r0, rows)]

    def term(piece, kc, core):
        arr, _, rows, kind = pieces[piece]
        if kind == 'rows':
            return ins[arr].at[pl.ds(pl.multiple_of(ins[arr].shape[0] // CHIPS * kc + 24 * core, SUB), rows)]
        return rows_of(ins[arr].at[PAIR * kc + core if kind == 'device' else kc], piece)

    class Node:
        def __init__(self, u):
            self.u = u
            self.first, self.parts, self.rest = _order(u, seq, orders, n, len(late), 15, work.after if work else ())
            self.keys = self.first + sum(self.parts, []) + self.rest
            self.adds = [[key for key in self.keys if key[PIECE] == i and (paired[i] or _onward(u, key, orders))] for i in range(n)]
            self.sent, self.given, self.done = [], [0] * n, [0] * n

        def meet(self):
            _meet([at.side(s) for s in ['a', 'b', 'z+'] + (['z-'] if self.u else [])] + [at.partner])

        def load(self, piece, j):
            return pltpu.make_async_copy(term(piece, at.chip(self.adds[piece][j]), at.core), stage[piece].at[j % PAIR], load_sem.at[piece, j % PAIR])

        def ready(self, some):
            for key in self.keys:
                piece = key[PIECE]
                if paired[piece] and piece in some:
                    kc = partner_at.chip(key)
                    copy = _remote(term(piece, kc, 1 - at.core), got[piece].at[kc], d_send.at[piece, self.given[piece]], d_recv.at[piece, kc], at.partner)
                    self.given[piece] += 1
                    copy.start()
            for piece in some:
                for j in range(PAIR):
                    self.load(piece, j).start()

        def step(self, key):
            u, piece = self.u, key[PIECE]
            arr, _, rows, _ = pieces[piece]
            kc = at.chip(key)
            root = key[:3] == (0, 0, u)
            children = _onward(u, key, orders)
            if not children and not paired[piece]:
                src = term(piece, kc, at.core)
            else:
                j = self.done[piece]
                self.done[piece] += 1
                parts = []
                if paired[piece]:
                    _landed(got[piece].at[kc], d_recv.at[piece, kc])
                    parts.append(got[piece].at[kc])
                for side in children:
                    slot = table[u, key, side]
                    _landed(land[piece].at[slot], recv_sem.at[piece, slot])
                    parts.append(land[piece].at[slot])
                self.load(piece, j).wait()
                parts.append(stage[piece].at[j % PAIR])
                src = parts[0]
                dtype = ins[arr].dtype
                size = SUB if dtype == F32 else CHIPS

                def add(r):
                    some = pl.ds(pl.multiple_of(r * size, size), size)
                    total = parts[0][some, :].astype(F32)
                    for ref in parts[1:]:
                        total = total + ref[some, :].astype(F32)
                    src[some, :] = total.astype(dtype)
                loop(rows // size, add)
                if j + PAIR < len(self.adds[piece]):
                    self.load(piece, j + PAIR).start()
            if root:
                copy = pltpu.make_async_copy(src, rows_of(outs[arr], piece), out_sem.at[piece])
            else:
                slot = table[_seen_by_parent(u, key, orders)]
                copy = _remote(src, land[piece].at[slot], send_sem.at[len(self.sent)], recv_sem.at[piece, slot], at.side(_via(u, key, orders)))
                self.sent.append(piece)
            copy.start()

        def finish(self):
            def sent(ref, sem):
                _remote(ref, ref, sem, sem, at.partner).wait_send()
            for i, piece in enumerate(self.sent):
                sent(land[piece].at[0], send_sem.at[i])
            for piece in range(n):
                for i in range(self.given[piece]):
                    sent(got[piece].at[0], d_send.at[piece, i])
                out = rows_of(outs[pieces[piece][0]], piece)
                _landed(out, out_sem.at[piece])

    nodes = [Node(u) for u in (0, 1)]

    def each(do):
        for node in nodes:
            pl.when(at.u == node.u)(functools.partial(do, node))

    def begin(node):
        node.meet()
        node.ready(early)
        for key in node.first:
            node.step(key)

    def end(node):
        node.ready(late)
        for key in node.rest:
            node.step(key)
        node.finish()
    each(begin)
    if work:
        def between(part, when=None):
            def steps(node):
                for key in node.parts[part]:
                    node.step(key)
            if when is None:
                each(steps)
            else:
                pl.when(when)(lambda: each(steps))
        work.run(work_in, made, work_out, refs_left, between)
    each(end)


def scatter_sum(arrays, pieces, orders, seq, collective_id, work=None):
    late = list(work.makes) if work else []
    n_arr, n = len(arrays) + len(late), len(pieces)
    dma, hbm, vmem = pltpu.SemaphoreType.DMA, pl.BlockSpec(memory_space=pl.ANY), pl.BlockSpec(memory_space=pltpu.VMEM)
    _, most = _slots(pieces, orders, seq)
    every = list(arrays) + late
    shapes = [(rows, every[arr].shape[-1], every[arr].dtype) for arr, _, rows, _ in pieces]
    scratch = [pltpu.VMEM((m, r, c), d) for m, (r, c, d) in zip(most, shapes)]
    scratch += [pltpu.VMEM((PAIR, r, c), d) for r, c, d in shapes]
    scratch += [pltpu.VMEM((CHIPS, r, c), d) for (r, c, d), p in zip(shapes, pieces) if p[KIND] != 'chip']
    outs = [jax.ShapeDtypeStruct((sum(p[PAIR] for p in pieces if p[0] == i), v.shape[-1]), v.dtype) for i, v in enumerate(every)]
    nbytes = sum((m + PAIR + CHIPS * int(p[KIND] != 'chip')) * (-(-r // CHIPS) * CHIPS) * c * d.itemsize for m, (r, c, d), p in zip(most, shapes, pieces))
    scratch += [dma((n, PAIR)), dma((CHIPS * n,)), dma((n, max(most))), dma((n, CHIPS)), dma((n, CHIPS)), dma((n,))]
    work_in = work.operands if work else []
    work_out = work.results if work else []
    limit = min(nbytes + (6 * MIB) + (work.nbytes if work else 0), 67043328)
    return pl.pallas_call(
        functools.partial(_scatter_kernel, tuple(pieces), orders, seq, n_arr, work),
        out_shape=outs + late + work_out,
        in_specs=[hbm] * len(arrays) + [vmem if near else hbm for _, near in work_in],
        out_specs=[hbm] * (n_arr + len(late)) + [vmem] * len(work_out),
        scratch_shapes=scratch + (work.scratch if work else []),
        compiler_params=pltpu.CompilerParams(collective_id=collective_id, has_side_effects=True, vmem_limit_bytes=limit),
        cost_estimate=cost(200_000_000, nbytes * QUAD),
        name='scatter_sum',
    )(*arrays, *[v for v, _ in work_in])


def _add_rows_kernel(counts, codes, dx_ref, out_ref, buf, sem):
    n_src, lines, _ = dx_ref.shape
    n_col = 7
    seq = codes.shape[0] // n_src
    cut = lines // 5
    depth = buf.shape[0]

    def fetch(b):
        for i in range(5):
            some = pl.ds(i * cut, cut)
            pltpu.make_async_copy(dx_ref.at[b, some], buf.at[lax.rem(b, depth), some], sem.at[lax.rem(b, depth)]).start()

    for b in range(depth - 1):
        fetch(b)

    def clear(i):
        out_ref[pl.ds(pl.multiple_of(i * CHIPS * n_col, SUB), CHIPS * n_col), :] = jnp.zeros((CHIPS * n_col, LANES), F32)
    loop(out_ref.shape[0] // (CHIPS * n_col), clear)

    def source(b):
        at = lax.rem(b, depth)

        @pl.when(b + depth - 1 < n_src)
        def _():
            fetch(b + depth - 1)
        pltpu.make_async_copy(dx_ref.at[b], buf.at[at], sem.at[at]).wait()

        def add(first, i):
            code = codes[b * seq + first + i]
            line = pl.ds(code & 65535, n_col, stride=SUB)
            out_ref[line, :] = out_ref[line, :] + buf[at, pl.ds(code >> CHIPS, n_col, stride=SUB), :]

        def add_four(i):
            code = [codes[b * seq + i * QUAD + t] for t in range(QUAD)]
            line = [c & 65535 for c in code]
            news = [buf[at, pl.ds(c >> CHIPS, n_col, stride=SUB), :] for c in code]
            sums = []
            for t in range(QUAD):
                old = out_ref[pl.ds(line[t], n_col, stride=SUB), :]
                for before in range(t):
                    old = jnp.where(line[t] == line[before], sums[before], old)
                sums.append(old + news[t])
            for t in range(QUAD):
                out_ref[pl.ds(line[t], n_col, stride=SUB), :] = sums[t]
        n = counts[b]
        loop(n // QUAD, add_four)

        rest = n // QUAD * QUAD
        loop(n - rest, functools.partial(add, rest))
    loop(n_src, source)


def add_rows(dx, counts, codes, n_rows):
    n_src, lines, _ = dx.shape
    return pl.pallas_call(
        _add_rows_kernel,
        grid_spec=pltpu.PrefetchScalarGridSpec(
            num_scalar_prefetch=PAIR,
            grid=(),
            in_specs=[pl.BlockSpec(memory_space=pl.ANY)],
            out_specs=pl.BlockSpec(memory_space=pltpu.VMEM),
            scratch_shapes=[pltpu.VMEM((QUAD, lines, LANES), F32), pltpu.SemaphoreType.DMA((QUAD,))],
        ),
        out_shape=jax.ShapeDtypeStruct((n_rows * 7, LANES), F32),
        compiler_params=pltpu.CompilerParams(vmem_limit_bytes=48 * MIB),
        cost_estimate=cost(50_000_000, 80 * MIB),
        name='add_rows',
    )(counts, codes, dx)


def to_lines(v):
    rows, dim = v.shape
    return v.reshape(rows // SUB, SUB, dim // LANES, LANES).transpose(0, PAIR, 1, 3).reshape(rows * dim // LANES, LANES)


def from_lines(v, dim):
    rows = v.shape[0] * LANES // dim
    return v.reshape(rows // SUB, dim // LANES, SUB, LANES).transpose(0, PAIR, 1, 3).reshape(rows, dim)


def _rms(v):
    return lax.rsqrt(jnp.mean(v * v, axis=-1, keepdims=True) + NORM_EPS)


def _head_mean(v, low):
    first = jnp.sum(jnp.where(low, v, 0.0), axis=-1, keepdims=True)
    second = jnp.sum(jnp.where(low, 0.0, v), axis=-1, keepdims=True)
    return jnp.where(low, first, second) * (1.0 / 64.0)


def _turn(v, cos_t, sin_t, lead):
    return v * cos_t + jnp.where(lead, -pltpu.roll(v, 96, 1), pltpu.roll(v, 32, 1)) * sin_t


def _spread(tile, low, ref):
    first = jnp.where(low, tile, 0.0)
    second = jnp.where(low, 0.0, tile)
    ref[0] = first.astype(BF16)
    ref[1] = pltpu.roll(first, HEAD, 1).astype(BF16)
    ref[PAIR] = pltpu.roll(second, HEAD, 1).astype(BF16)
    ref[3] = second.astype(BF16)


def _probs(q, k, block):
    scores = mm_nt(q, k) * 0.125
    n = scores.shape[1]
    row = lax.broadcasted_iota(jnp.int32, scores.shape, 0) + block
    col = lax.broadcasted_iota(jnp.int32, scores.shape, 1)
    scores = jnp.where(row >= col, scores, -1e30)
    e = jnp.exp(scores - jnp.max(scores, axis=-1, keepdims=True))
    return e * (1.0 / jnp.sum(e, axis=-1, keepdims=True))


def _lanes(rows):
    lane = lax.broadcasted_iota(jnp.int32, (rows, LANES), 1)
    return lane < HEAD, lane % HEAD < 32


def _attn_fwd_kernel(x_ref, w_ref, gain_ref, cos_ref, sin_ref, qk_gain_ref, in_ref, raw_ref, q_ref, k_ref, flat_ref, hid_ref, mlp_ref, kk, vv):
    seq, dim = x_ref.shape
    n_q = dim // LANES
    step = LANES
    n_in = raw_ref.shape[1]

    def project(r):
        at = pl.ds(pl.multiple_of(r * step, step), step)
        low, lead = _lanes(step)
        x = x_ref[at, :].astype(F32)
        m1 = (x * _rms(x) * gain_ref[0:1, :]).astype(BF16)
        in_ref[at, :] = m1
        raw = mm(m1, w_ref[0]).astype(BF16)
        raw_ref[at, :] = raw
        cos_t, sin_t = cos_ref[at, :], sin_ref[at, :]
        for t in range(n_q + 1):
            v = raw[:, t * LANES:(t + 1) * LANES].astype(F32)
            v = v * lax.rsqrt(_head_mean(v * v, low) + NORM_EPS)
            which = int(t == n_q)
            v = _turn(v * qk_gain_ref[SUB * which:SUB * which + 1, :], cos_t, sin_t, lead).astype(BF16)
            if which:
                k_ref[at, :] = v
            else:
                q_ref[at, t * LANES:(t + 1) * LANES] = v
    loop(seq // step, project)
    low, _ = _lanes(seq)
    _spread(k_ref[...].astype(F32), low, kk)
    _spread(raw_ref[:, n_in - LANES:].astype(F32), low, vv)

    def heads(t):
        tile = pl.ds(pl.multiple_of(t * LANES, LANES), LANES)
        for b in range(seq // step):
            n = (b + 1) * step
            q = q_ref[b * step:n, tile]
            total = None
            for side in range(PAIR):
                i = PAIR * ((PAIR * t + side) // 7) + side
                p = _probs(q, kk[i, :n, :], b * step).astype(BF16)
                o = mm(p, vv[i, :n, :])
                total = o if total is None else total + o
            flat_ref[b * step:n, tile] = total.astype(BF16)
    loop(n_q, heads)

    def finish(r):
        at = pl.ds(pl.multiple_of(r * step, step), step)
        h = (x_ref[at, :].astype(F32) + mm(flat_ref[at, :], w_ref[1, :, :dim])).astype(BF16)
        hid_ref[at, :] = h
        h = h.astype(F32)
        mlp_ref[at, :] = (h * _rms(h) * gain_ref[SUB:9, :]).astype(BF16)
    loop(seq // step, finish)


def attn_forward(x, w, gains, cos_t, sin_t, qk_gain):
    seq, dim = x.shape
    n_in = w.shape[PAIR]
    vmem = pl.BlockSpec(memory_space=pltpu.VMEM)
    sds = lambda n: jax.ShapeDtypeStruct((seq, n), BF16)
    return pl.pallas_call(
        _attn_fwd_kernel,
        out_shape=[sds(dim), sds(n_in), sds(dim), sds(LANES), sds(dim), sds(dim), sds(dim)],
        in_specs=[vmem] * 6,
        out_specs=[vmem] * 7,
        scratch_shapes=[pltpu.VMEM((QUAD, seq, LANES), BF16), pltpu.VMEM((QUAD, seq, LANES), BF16)],
        compiler_params=pltpu.CompilerParams(vmem_limit_bytes=40 * MIB),
        cost_estimate=cost(4_000_000_000, 12 * MIB, 4_000_000),
        name='attn_forward',
    )(x, w, gains, cos_t, sin_t, qk_gain)


def _norm_back(grad, normed, inv, gain):
    grad = grad * gain
    return inv * (grad - normed * jnp.mean(grad * normed, axis=-1, keepdims=True))


def _hidden_bwd_kernel(w_ref, gain_ref, hid_ref, dy_ref, part_ref, recv_ref, gh_ref, hb_ref, do_ref, mlp_gain_ref):
    step = LANES
    mlp_gain_ref[...] = jnp.zeros_like(mlp_gain_ref)

    def hidden(r):
        at = pl.ds(pl.multiple_of(r * step, step), step)
        grad = part_ref[at, :] + recv_ref[at, :]
        h = hid_ref[at, :].astype(F32)
        inv = _rms(h)
        normed = h * inv
        g = dy_ref[at, :].astype(F32) + _norm_back(grad, normed, inv, gain_ref[SUB:9, :])
        gh_ref[at, :] = g
        g = g.astype(BF16)
        hb_ref[at, :] = g
        do_ref[at, :] = mm_nt(g, w_ref[1, :, :g.shape[1]]).astype(BF16)
        mlp_gain_ref[...] = mlp_gain_ref[...] + jnp.sum(grad * normed, axis=0, keepdims=True)
    loop(hid_ref.shape[0] // step, hidden)


def hidden_backward(w, gains, hidden, dy, part, recv):
    vmem = pl.BlockSpec(memory_space=pltpu.VMEM)
    sds = jax.ShapeDtypeStruct
    return pl.pallas_call(
        _hidden_bwd_kernel,
        out_shape=[sds(part.shape, F32), sds(part.shape, BF16), sds(part.shape, BF16), sds((SUB, part.shape[1]), F32)],
        in_specs=[vmem] * 6,
        out_specs=[vmem] * QUAD,
        compiler_params=pltpu.CompilerParams(vmem_limit_bytes=24 * MIB),
        cost_estimate=cost(1_000_000_000, CHIPS * MIB),
        name='hidden_backward',
    )(w, gains, hidden, dy, part, recv)


class AttnBackward:
    arrays, inputs, outputs, scratches = PAIR, 15, 1, 11
    after = (False, False, False, True, True, True, True, True)
    nbytes = 22 * MIB

    def __init__(self, x, w, gains, mlp_gain, cos_t, sin_t, qk_gain, saved, gh, hb, do):
        seq, dim = x.shape
        n_in = w.shape[PAIR]
        far = (w, gh)
        self.operands = [(v, all(v is not f for f in far)) for v in (gains, mlp_gain, cos_t, sin_t, qk_gain, x, *far, *saved[:5], hb, do)]
        self.makes = [jax.ShapeDtypeStruct((dim, n), F32) for n in (n_in, dim)]
        self.results = [jax.ShapeDtypeStruct((seq + SUB, dim), F32)]
        scr = lambda *s: pltpu.VMEM(s[:-1], s[-1])
        self.scratch = [scr(dim, n_in, BF16), scr(QUAD, seq, LANES, BF16), scr(QUAD, seq, LANES, BF16), scr(QUAD, seq, LANES, F32), scr(QUAD, seq, LANES, F32),
                        scr(seq, n_in, BF16), scr(PAIR, SUB, LANES, F32), scr(PAIR, LANES, n_in, F32), scr(PAIR, LANES, dim, F32),
                        pltpu.SemaphoreType.DMA((PAIR,)), pltpu.SemaphoreType.DMA((PAIR, PAIR))]

    def run(self, operands, made, results, scratch, between):
        (gain_ref, mlp_gain_ref, cos_ref, sin_ref, qk_gain_ref, x_ref, w_hbm, gh_hbm, in_ref, raw_ref, q_ref, k_ref, flat_ref, hb, do) = operands
        w_ref, kk, vv, dk, dv, dqkv, qk_sum, in_out, out_out, in_sem, store_sem = scratch
        dx_ref, = results
        seq, dim = x_ref.shape
        n_q = dim // LANES
        step = LANES
        n_blk = seq // step
        n_in = raw_ref.shape[1]
        fetch = [pltpu.make_async_copy(gh_hbm, dx_ref.at[pl.ds(0, seq)], in_sem.at[0]), pltpu.make_async_copy(w_hbm.at[0], w_ref, in_sem.at[1])]
        for copy in fetch:
            copy.start()
        low_all, _ = _lanes(seq)
        _spread(k_ref[...].astype(F32), low_all, kk)
        _spread(raw_ref[:, n_in - LANES:].astype(F32), low_all, vv)
        for ref in (dk, dv, qk_sum):
            ref[...] = jnp.zeros_like(ref)

        def raw_back(grad, tile, at, which, low, lead):
            v = raw_ref[at, tile].astype(F32)
            inv = lax.rsqrt(_head_mean(v * v, low) + NORM_EPS)
            normed = v * inv
            grad = _turn(grad, cos_ref[at, :], -sin_ref[at, :], lead)
            qk_sum[which] = qk_sum[which] + jnp.sum(grad * normed, axis=0, keepdims=True)
            grad = grad * qk_gain_ref[SUB * which:SUB * which + 1, :]
            return inv * (grad - normed * _head_mean(grad * normed, low))

        def heads(t):
            tile = pl.ds(pl.multiple_of(t * LANES, LANES), LANES)
            low, lead = _lanes(step)
            for b in range(n_blk):
                n = (b + 1) * step
                at = pl.ds(b * step, step)
                q = q_ref[at, tile]
                g = do[at, tile]
                grad_q = None
                for side in range(PAIR):
                    i = PAIR * ((PAIR * t + side) // 7) + side
                    k = kk[i, :n, :]
                    p = _probs(q, k, b * step)
                    dp = mm_nt(g, vv[i, :n, :])
                    ds = (p * (dp - jnp.sum(dp * p, axis=-1, keepdims=True)) * 0.125).astype(BF16)
                    dv[i, :n, :] = dv[i, :n, :] + mm_tn(p.astype(BF16), g)
                    dk[i, :n, :] = dk[i, :n, :] + mm_tn(ds, q)
                    part = mm(ds, k)
                    grad_q = part if grad_q is None else grad_q + part
                dqkv[at, tile] = raw_back(grad_q, tile, at, 0, low, lead).astype(BF16)
            for part in range(n_q):
                between(part, t == part)
        loop(n_q, heads)

        def keys(r):
            at = pl.ds(pl.multiple_of(r * step, step), step)
            low, lead = _lanes(step)

            def join(ref):
                return jnp.where(low, ref[0, at, :] + pltpu.roll(ref[1, at, :], HEAD, 1), ref[3, at, :] + pltpu.roll(ref[PAIR, at, :], HEAD, 1))
            dqkv[at, dim:dim + LANES] = raw_back(join(dk), pl.ds(dim, LANES), at, 1, low, lead).astype(BF16)
            dqkv[at, dim + LANES:] = join(dv).astype(BF16)
        loop(n_blk, keys)
        for copy in fetch:
            copy.wait()

        def inputs(r, total):
            at = pl.ds(pl.multiple_of(r * step, step), step)
            grad = mm_nt(dqkv[at, :], w_ref[...])
            x = x_ref[at, :].astype(F32)
            inv = _rms(x)
            normed = x * inv
            dx_ref[at, :] = dx_ref[at, :] + _norm_back(grad, normed, inv, gain_ref[0:1, :])
            return total + jnp.sum(grad * normed, axis=0, keepdims=True)
        attn_gain = lax.fori_loop(0, n_blk, inputs, jnp.zeros((1, dim), F32))
        between(n_q)

        low, _ = _lanes(SUB)
        row = lax.broadcasted_iota(jnp.int32, (SUB, dim), 0)
        fold = lambda v: v + pltpu.roll(v, HEAD, 1)
        dx_ref[seq:, :] = jnp.where(row == 1, jnp.broadcast_to(attn_gain, (SUB, dim)), jnp.where(row == PAIR, mlp_gain_ref[...], 0.0))
        dx_ref[seq:, :LANES] = jnp.where(row[:, :LANES] == 0, jnp.where(low, fold(qk_sum[0]), fold(qk_sum[1])), dx_ref[seq:, :LANES])

        def stores(t):
            return [pltpu.make_async_copy(buf.at[t % PAIR], ref.at[pl.ds(pl.multiple_of(t * LANES, LANES), LANES)], store_sem.at[i, t % PAIR])
                    for i, (buf, ref) in enumerate(((in_out, made[0]), (out_out, made[1])))]

        def weights(t):
            @pl.when(t >= PAIR)
            def _():
                for copy in stores(t - PAIR):
                    copy.wait()
            tile = pl.ds(pl.multiple_of(t * LANES, LANES), LANES)
            in_out[t % PAIR] = mm_tn(in_ref[:, tile], dqkv[...])
            out_out[t % PAIR] = mm_tn(flat_ref[:, tile], hb[...])
            for copy in stores(t):
                copy.start()
        loop(n_q, weights)
        for t in (n_q - PAIR, n_q - 1):
            for copy in stores(t):
                copy.wait()


def _mlp_kernel(x_ref, dy_ref, wgu_ref, wd_ref, y_mine, y_other, din_mine, din_other, dwg_ref, dwu_ref, dwd_ref, xt, wg, wu, wd, act, dg, du, og, ou, od, load_sem, store_sem):
    half, tile = dwd_ref.shape[0], act.shape[1]
    n_tile = -(-half // tile)
    shared = n_tile * tile - half
    seq = y_mine.shape[0]
    step = seq // PAIR

    def start_of(j):
        first = (j == 0).astype(jnp.int32)
        return pl.multiple_of(first * (half - tile) + (1 - first) * (j - 1) * tile, LANES)

    def loads(j):
        at, slot = start_of(j), j % PAIR
        return [pltpu.make_async_copy(wgu_ref.at[:, pl.ds(at, tile)], wg.at[slot], load_sem.at[0, slot]),
                pltpu.make_async_copy(wgu_ref.at[:, pl.ds(pl.multiple_of(half + at, LANES), tile)], wu.at[slot], load_sem.at[1, slot]),
                pltpu.make_async_copy(wd_ref.at[pl.ds(at, tile)], wd.at[slot], load_sem.at[PAIR, slot])]

    def stores(j):
        at, slot = start_of(j), j % PAIR
        return [pltpu.make_async_copy(og.at[slot], dwg_ref.at[:, pl.ds(at, tile)], store_sem.at[0, slot]),
                pltpu.make_async_copy(ou.at[slot], dwu_ref.at[:, pl.ds(at, tile)], store_sem.at[1, slot]),
                pltpu.make_async_copy(od.at[slot], dwd_ref.at[pl.ds(at, tile)], store_sem.at[PAIR, slot])]

    for copy in loads(jnp.int32(0)):
        copy.start()
    for ref in (y_mine, y_other, din_mine, din_other):
        ref[...] = jnp.zeros_like(ref)
    xt[...] = x_ref[...].T

    def columns(j):
        slot = j % PAIR

        @pl.when(j + 1 < n_tile)
        def _():
            for copy in loads(j + 1):
                copy.start()
        for copy in loads(j):
            copy.wait()

        def rows(y_ref, din_ref, first, r):
            at, inner = pl.ds(pl.multiple_of(first + r * step, step), step), pl.ds(pl.multiple_of(r * step, step), step)
            x = x_ref[at, :]
            gate, up, back = mm(x, wg[slot]), mm(x, wu[slot]), mm_nt(dy_ref[at, :], wd[slot])
            counts = lax.broadcasted_iota(jnp.int32, (step, tile), 1) >= (j == 0).astype(jnp.int32) * shared
            up, back = jnp.where(counts, up, 0.0), jnp.where(counts, back, 0.0)
            sig = lax.logistic(gate)
            silu = gate * sig
            a = (silu * up).astype(BF16)
            g = (back * up * sig * (1.0 + gate * (1.0 - sig))).astype(BF16)
            u = (back * silu).astype(BF16)
            act[at, :], dg[at, :], du[at, :] = a, g, u
            y_ref[inner, :] = y_ref[inner, :] + mm(a, wd[slot])
            din_ref[inner, :] = din_ref[inner, :] + mm_nt(g, wg[slot]) + mm_nt(u, wu[slot])
        loop(PAIR, functools.partial(rows, y_mine, din_mine, 0))
        loop(PAIR, functools.partial(rows, y_other, din_other, seq))

        @pl.when(j >= PAIR)
        def _():
            for copy in stores(j - PAIR):
                copy.wait()
        og[slot] = mm(xt[...], dg[...])
        ou[slot] = mm(xt[...], du[...])
        od[slot] = mm_tn(act[...], dy_ref[...])
        for copy in stores(j):
            copy.start()
    loop(n_tile, columns)
    for j in (n_tile - PAIR, n_tile - 1):
        for copy in stores(jnp.int32(j)):
            copy.wait()


def mlp(x, dy, wgu, wd):
    rows, dim = x.shape
    half = wd.shape[0]
    tile = 512
    vmem, hbm = pl.BlockSpec(memory_space=pltpu.VMEM), pl.BlockSpec(memory_space=pl.ANY)
    sds = lambda *s: jax.ShapeDtypeStruct(s, F32)
    dma = pltpu.SemaphoreType.DMA
    bf = lambda *s: pltpu.VMEM(s, BF16)
    f = lambda *s: pltpu.VMEM(s, F32)
    return pl.pallas_call(
        _mlp_kernel,
        out_shape=[sds(rows // PAIR, dim)] * QUAD + [sds(dim, half), sds(dim, half), sds(half, dim)],
        in_specs=[vmem, vmem, hbm, hbm],
        out_specs=[vmem] * QUAD + [hbm] * 3,
        scratch_shapes=[bf(dim, rows), bf(PAIR, dim, tile), bf(PAIR, dim, tile), bf(PAIR, tile, dim), bf(rows, tile), bf(rows, tile), bf(rows, tile),
                        f(PAIR, dim, tile), f(PAIR, dim, tile), f(PAIR, tile, dim), dma((3, PAIR)), dma((3, PAIR))],
        compiler_params=pltpu.CompilerParams(vmem_limit_bytes=44 * MIB),
        cost_estimate=cost(CHIPS * rows * dim * half, 50 * MIB, rows * half),
        name='mlp',
    )(x, dy, wgu, wd)


def _codes(numbers, count):
    return tuple(numbers[i // 10] // LANES ** (i % 10) % LANES for i in range(count))


ROWS_SEQ = (
    _codes((152348940317322383368, 678662145372396725288, 751232056588892674273, 827272104050806263145, 30857149562), 45),
    _codes((166206088102504171520, 236385149464955200810, 603605329936848293224, 1039985241786269873361, 32734212313), 45),
)
ATTN_SEQ = (
    _codes((370142165075936415752, 972012016723415295145, 1124725529257844811929), 30),
    _codes((961577811093152729088, 751808515438843144256, 1124738970787495025897), 30),
)
GRAD_SEQ = (
    _codes((106232080133048504328, 412786621588976116131, 918546169305131799568, 485409126374496736530, 238786845178607580779, 257151255934452689491, 843574817237186309276, 33002831324), 75),
    _codes((166206088102504171520, 704158088118449268010, 330331505424276671520, 463101567523338654259, 770399732085151419931, 1050366487184744456811, 848110399440616747490, 33002831324), 75),
)


def solution(mesh):
    n_dev = mesh.shape[AXIS_NAME]
    n_chip = n_dev // PAIR
    pair = [(i, i ^ 1) for i in range(n_dev)]
    groups = [[PAIR * k + c for k in range(n_chip)] for c in range(PAIR)]

    row_spec = P(AXIS_NAME, None)
    vec_spec = P(AXIS_NAME)
    full_spec = P(None)
    batch_spec = P(AXIS_NAME, None, None)
    weight_specs = (vec_spec, row_spec, row_spec, row_spec, full_spec, full_spec, row_spec, vec_spec, row_spec, row_spec, row_spec)

    def swap(v):
        return lax.ppermute(v, AXIS_NAME, pair)

    def gather_group(v):
        return lax.all_gather(v, AXIS_NAME, axis_index_groups=groups, tiled=True)

    def device_step(tokens, positions, table_shard, attn_norm, w_query, w_key, w_value, q_norm, k_norm, w_out, mlp_norm, w_gate, w_up, w_down, dy_out):
        me = lax.axis_index(AXIS_NAME)
        core = lax.rem(me, PAIR)
        seq_len = tokens.shape[1]
        rows_local, model_dim = table_shard.shape
        rows_w, ff = w_gate.shape
        half = ff // PAIR
        nq, nk = w_query.shape[1], w_key.shape[1]
        head_dim = q_norm.shape[0]

        n_in = nq + PAIR * nk

        def gate_up(c):
            return jnp.concatenate([lax.dynamic_slice(w, (0, c * half), (rows_w, half)) for w in (w_gate, w_up)], axis=1)

        def both_cores(mine, other):
            return jnp.where(core == 0, jnp.concatenate([mine, other], axis=0), jnp.concatenate([other, mine], axis=0))
        attn_in = jnp.concatenate([w_query, w_key, w_value], axis=1)
        attn_out = jnp.concatenate([w_out, below(jnp.stack([attn_norm, mlp_norm]), n_in - nq - PAIR).T], axis=1)
        mine_attn, other_attn = jnp.where(core == 0, attn_in, attn_out), jnp.where(core == 0, attn_out, attn_in)
        dy = dy_out.reshape(seq_len, model_dim)
        all_tokens, (down_block, recv_gu, recv_attn, dy_other) = all_rows(
            below(tokens.reshape(-1, LANES), QUAD), n_dev, [w_down, gate_up(1 - core), other_attn, dy], ('use', 'pair', 'pair', 'pair'), 0)
        wgu = gather_group(both_cores(gate_up(core), recv_gu))

        all_ids = all_tokens[:, :seq_len // LANES].reshape(-1)
        local_ids = all_ids - me * rows_local
        is_owner = (local_ids >= 0) & (local_ids < rows_local)
        lines = model_dim // LANES
        line = lambda row: row // SUB * (SUB * lines) + row % SUB
        found = (jnp.where(is_owner, line(local_ids), rows_local * lines), table_shard, seq_len)
        (attn_w, wd), (picked,) = gather_all([both_cores(mine_attn, recv_attn), down_block], [(0, 0, PAIR * rows_w, 'core'), (1, 0, down_block.shape[0], 'chip')],
                                     ('bza', 'zba'), ATTN_SEQ, [], (), n_dev, 1, found)
        attn_w = attn_w.reshape(PAIR, model_dim, n_in)
        wd = wd.reshape(-1, model_dim)

        x_emb = scatter_sum([picked], [(0, 0, 192, 'device'), (0, 192, 208, 'device'), (0, 400, 112, 'device')], ('zba', 'zba', 'baz'), ROWS_SEQ, PAIR)[0]

        dy2 = jnp.concatenate([dy, dy_other], axis=0)

        gains = below(jnp.repeat(attn_w[1, :, nq:nq + PAIR].astype(F32).T, SUB, axis=0), SUB)
        qk_gain = jnp.repeat(jnp.stack([jnp.tile(q_norm, PAIR), jnp.tile(k_norm, PAIR)]).astype(F32), SUB, axis=0)

        inv_freq = jnp.exp((jnp.arange(LANES) % (head_dim // PAIR)).astype(F32) * (-2.0 * math.log(ROPE_THETA) / head_dim))
        angles = positions.reshape(seq_len, 1).astype(F32) * inv_freq
        cos_t, sin_t = jnp.cos(angles), jnp.sin(angles)
        saved = attn_forward(x_emb, attn_w, gains, cos_t, sin_t, qk_gain)
        hidden, mlp_in = saved[5:]

        mlp2 = jnp.concatenate([mlp_in, swap(mlp_in)], axis=0)
        y_mine, y_other, grad_in, grad_other, grad_w_gate, grad_w_up, grad_w_down = mlp(mlp2, dy2, wgu, wd)
        grad_recv = swap(grad_other)
        layer_out = (hidden.astype(F32) + (y_mine + swap(y_other))).astype(BF16)

        gh, hb, grad_heads, mlp_gain = hidden_backward(attn_w, gains, hidden, dy, grad_in, grad_recv)
        by_chip = [u.reshape(n_chip, -1, u.shape[1]) for u in (grad_w_down, grad_w_gate, grad_w_up)]
        down_rows, gate_shard, up_shard, in_shard, out_shard, _, _, dx_block = scatter_sum(
            by_chip, [(i, 0, u.shape[1], 'chip') for i, u in enumerate(by_chip)] + [(i, 0, 32, 'rows') for i in (3, QUAD)], ('bza', 'zba', 'bza', 'zba', 'zba'), GRAD_SEQ, 3,
            AttnBackward(x_emb, attn_w, gains, mlp_gain, cos_t, sin_t, qk_gain, saved, gh, hb, grad_heads))

        chip_rows = jnp.concatenate([gate_shard, up_shard], axis=1)
        mine = lax.dynamic_slice(chip_rows, (core * rows_w, 0), (rows_w, chip_rows.shape[1]))
        give = lax.dynamic_slice(chip_rows, ((1 - core) * rows_w, 0), (rows_w, chip_rows.shape[1]))
        (all_dx,), (down_shard, recv) = gather_all(
            [to_lines(dx_block)], [(0, 0, 200 * lines, 'device'), (0, 200 * lines, 200 * lines, 'device'), (0, 400 * lines, 120 * lines, 'device')],
            ('zba', 'zba', 'baz'), ROWS_SEQ, [down_rows, give], ('store', 'pair'), n_dev, QUAD)
        own = is_owner.reshape(n_dev, seq_len)
        slot = jnp.arange(seq_len, dtype=jnp.int32)
        upto = (slot[:, None] <= slot[None, :]).astype(BF16)
        rank = jnp.where(own, mm(own.astype(BF16), upto).astype(jnp.int32) - 1, -1)
        counts = jnp.sum(own.astype(jnp.int32), axis=1)
        code = line(slot)[None] * 65536 + line(jnp.where(own, local_ids.reshape(n_dev, seq_len), 0))
        codes = jnp.sum(jnp.where(rank[:, :, None] == slot, code[:, :, None], 0), axis=1)
        codes = jnp.where(slot[None] < counts[:, None], codes, seq_len * lines * 65536).reshape(-1)
        d_table = from_lines(add_rows(all_dx, counts, codes, rows_local), model_dim)
        gains_grad = from_lines(jnp.sum(all_dx[:, seq_len * lines:], axis=0), model_dim)
        qk = gains_grad[0]
        d_attn_norm, d_mlp_norm = (lax.dynamic_slice(gains_grad[i], (me * rows_w,), (rows_w,)) for i in (1, PAIR))
        low = jnp.where(core == 0, mine, recv)
        high = jnp.where(core == 0, recv, mine)
        d_gate = jnp.concatenate([low[:, :half], high[:, :half]], axis=1)
        d_up = jnp.concatenate([low[:, half:ff], high[:, half:ff]], axis=1)
        in_rows = lax.dynamic_slice(in_shard, (core * (rows_w - 24), 0), (rows_w, n_in))
        d_query, d_key, d_value = in_rows[:, :nq], in_rows[:, nq:nq + nk], in_rows[:, nq + nk:]
        d_out = lax.dynamic_slice(out_shard, (core * (rows_w - 24), 0), (rows_w, nq))
        return (layer_out.reshape(1, seq_len, model_dim), d_table, d_attn_norm, d_query, d_key, d_value, qk[:head_dim], qk[head_dim:PAIR * head_dim], d_out, d_mlp_norm, d_gate, d_up, down_shard)

    return jax.shard_map(device_step, mesh=mesh, in_specs=(row_spec, row_spec, row_spec) + weight_specs + (batch_spec,), out_specs=(batch_spec, row_spec) + weight_specs, check_vma=False)
```
